32 devices in a mesh: dp: 8 (over z, x), mp: 4 (over y, core).
Axes of the slice: x: 2, y: 2, z: 4, core: 2. Of those that a mesh axis runs over, the one named last changes fastest.
Arguments:
- patches: bfloat16 [16384, 768], P(('dp', 'mp')), may hold values from -6 to 6
- segment_ids: int32 [16, 1024], P('dp'), may hold values from 0 to 7, never falling along the last dimension, each value on 1 to 256 neighbouring positions
- fill_counts: int32 [16], P('dp'), may hold values from 512 to 1024, as said below
- attn_gain: float32 [768], replicated, may hold values from 0.1 to 1.9
- attn_shift: float32 [768], replicated, may hold values from -3 to 3
- qkv_weight: bfloat16 [3, 768, 768], P(None, None, 'mp'), may hold values from -0.21875 to 0.21875
- qv_bias: bfloat16 [2, 768], P(None, 'mp'), may hold values from -3 to 3
- rel_table: bfloat16 [12, 1024, 1024], P('mp'), may hold values from -4 to 4
- proj_weight: bfloat16 [768, 768], P('mp'), may hold values from -1.5 to 1.5
- proj_bias: bfloat16 [768], replicated, may hold values from -3 to 3
- attn_scale: float32 [768], replicated, may hold values from 0.5 to 2
- mlp_gain: float32 [768], replicated, may hold values from 0.1 to 1.9
- mlp_shift: float32 [768], replicated, may hold values from -3 to 3
- up_weight: bfloat16 [768, 3072], P(None, 'mp'), may hold values from -0.21875 to 0.21875
- up_bias: bfloat16 [3072], P('mp'), may hold values from -3 to 3
- down_weight: bfloat16 [3072, 768], P('mp'), may hold values from -0.109375 to 0.109375
- down_bias: bfloat16 [768], replicated, may hold values from -3 to 3
- mlp_scale: float32 [768], replicated, may hold values from 0.5 to 2
- cotangent: bfloat16 [16384, 768], P(('dp', 'mp')), may hold values from -6 to 6
Outputs:
- layer_out: bfloat16 [16384, 768], P(('dp', 'mp'))
- patch_grad: float32 [16384, 768], P(('dp', 'mp'))
- attn_gain_grad: float32 [768], replicated
- attn_shift_grad: float32 [768], replicated
- qkv_grad: float32 [3, 768, 768], P(None, 'dp', 'mp')
- qv_bias_grad: float32 [2, 768], P(None, 'mp')
- table_grad: float32 [12, 1024, 1024], P('mp', 'dp')
- proj_grad: float32 [768, 768], P('mp', 'dp')
- proj_bias_grad: float32 [768], replicated
- attn_scale_grad: float32 [768], replicated
- mlp_gain_grad: float32 [768], replicated
- mlp_shift_grad: float32 [768], replicated
- up_grad: float32 [768, 3072], P('dp', 'mp')
- up_bias_grad: float32 [3072], P('mp')
- down_grad: float32 [3072, 768], P('mp', 'dp')
- down_bias_grad: float32 [768], replicated
- mlp_scale_grad: float32 [768], replicated
The draws below stay inside these ranges and needn't reach their ends.
Inputs may be any that keep to these rules, and one draw needn't show every extreme that they name: `segment_ids`: within each sequence the page numbers never fall, and each page holds 1 to 256 patches. `fill_counts`: positions at or past a sequence's count are padding; some sequence is full and some is half full.
All inputs are finite; a program needn't handle non-finite values.
Results may differ from the reference program's by a relative error of at most 0.012.
Values may be sent and summed in bfloat16 or wider, within the bound.
A program may use at most 192 MiB of HBM per device.

```python
import math
import jax
import jax.numpy as jnp
import numpy as np
from jax import lax

D = 768
HEADS = 12
HEAD_DIM = 64
FF = 3072
L = 1024
PAGES = 8
SEQS = 2
PAGE_MOST = 256
SEQUENCES = 16
TOKENS = 16384
N_DP = 8


def draw_fill_counts(key, part):
    counts = jax.random.randint(key, (SEQUENCES,), L // 2, L + 1)
    counts = counts.at[0].set(L)
    counts = counts.at[1].set(L // 2)
    return counts.astype(jnp.int32)


def strengthened(entries, stream_key, source, target, blocks, factor):
    owner, partner = [(jnp.arange(entries.shape[axis_at]) // (entries.shape[axis_at] // blocks)).reshape([-1 if axis == axis_at else 1 for axis in range(entries.ndim)]) for axis_at in (source, target)]
    chosen = jax.random.permutation(stream_key, blocks)[partner]
    strong = (owner == chosen) | (owner == (partner + blocks // 2) % blocks)
    return jnp.where(strong, factor * entries, entries)


def block_levels(stream_key, shape, pieces, low, high):
    level, own = 1.0, jax.random.fold_in(stream_key, 6)
    for axis_at, blocks in pieces:
        heights = jnp.exp(jax.random.uniform(jax.random.fold_in(own, axis_at), (blocks,), jnp.float32, low / len(pieces), high / len(pieces)))
        level = level * jnp.repeat(heights, shape[axis_at] // blocks).reshape([-1 if axis == axis_at else 1 for axis in range(len(shape))])
    return level


def length_profile(number_of, total, limit, skew):
    portions = [(1 << 20) // math.isqrt(standing ** skew) + 1 for standing in range(2, number_of + 1)]
    surplus, given = total - limit - (number_of - 1), [1] * (number_of - 1)
    while surplus > 0:
        movable = [i for i in range(number_of - 1) if given[i] < limit]
        whole, left = sum([portions[i] for i in movable]), surplus
        for i in movable:
            addition = min(limit - given[i], max(1, left * portions[i] // whole), surplus)
            given[i] = given[i] + addition
            surplus = surplus - addition
    return np.array([limit] + given)


def ragged_sizes(own_key, amount, total, reach, skew):
    if amount == 2:
        one = jax.random.randint(own_key, (), max(1, total - reach), min(reach, total - 1) + 1)
        return jnp.stack([one, total - one])
    sizes = jnp.asarray(length_profile(amount, total, reach, skew), jnp.int32)
    twos = (amount - 1) // 2
    donor, taker = sizes[1:1 + 2 * twos:2], sizes[2:2 + 2 * twos:2]
    room = jnp.minimum(donor - 1, reach - taker)
    shifted = jax.random.randint(jax.random.fold_in(own_key, 1), (twos,), 0, 1 << 20) % (room + 1)
    sizes = sizes.at[1:1 + 2 * twos:2].set(donor - shifted).at[2:2 + 2 * twos:2].set(taker + shifted)
    return sizes[jax.random.permutation(jax.random.fold_in(own_key, 2), amount)]


def bell_draw(rng, shape, spread, most, cuts=(), dtype=jnp.bfloat16):
    factor_of = block_levels(rng, shape, cuts, -0.22, 0.18) if cuts else 1.0
    drawn = jax.random.normal(rng, shape, jnp.float32) * spread * factor_of
    return jnp.minimum(jnp.maximum(drawn, -most), most).astype(dtype)


def bell_draw_with(key, shape, width, reach, split, heavy, held_as=jnp.bfloat16):
    array = width * jax.random.normal(key, shape, jnp.float32)
    if split:
        array = array * block_levels(key, shape, split, -0.22, 0.18)
    return jnp.clip(strengthened(array, jax.random.fold_in(key, 3), *heavy), -reach, reach).astype(held_as)


def setup_inputs(seed: int = 0) -> dict:
    splits = jax.random.split(jax.random.key(seed), 20)
    patches = bell_draw(splits[0], (TOKENS, D), 1.0, 6.0, ((0, 32),))
    segment_ids = jax.vmap(lambda own: jnp.searchsorted(jnp.cumsum(ragged_sizes(own, PAGES, L, PAGE_MOST, 0)), jnp.arange(L), side="right"))(jax.random.split(splits[1], SEQUENCES)).reshape((SEQUENCES, L)).astype(jnp.int32)
    fill_counts = draw_fill_counts(jax.random.fold_in(splits[19], 71), 0)
    attn_gain = jnp.clip(1.0 + 0.18 * jax.random.normal(splits[3], (D,), jnp.float32), 0.1, 1.9)
    attn_shift = bell_draw(splits[4], (D,), 0.3, 3.0, (), jnp.float32)
    qkv_weight = bell_draw(splits[5], (3, D, D), D ** -0.5, 0.21875, ((2, 4),))
    qv_bias = bell_draw(splits[6], (2, D), 0.5, 3.0, ((1, 4),))
    rel_table = bell_draw(splits[7], (HEADS, L, L), 1.0, 4.0, ((0, 4),))
    proj_weight = bell_draw(splits[8], (D, D), (HEAD_DIM // 4) ** -0.5, 1.5, ((0, 4),))
    proj_bias = bell_draw(splits[9], (D,), 0.3, 3.0)
    attn_scale = jnp.clip(jnp.exp(jax.random.uniform(splits[10], (D,), jnp.float32, math.log(0.5), math.log(2.0))), 0.5, 2.0)
    mlp_gain = jnp.clip(1.0 + 0.18 * jax.random.normal(splits[11], (D,), jnp.float32), 0.1, 1.9)
    mlp_shift = bell_draw(splits[12], (D,), 0.3, 3.0, (), jnp.float32)
    up_weight = bell_draw(splits[13], (D, FF), D ** -0.5, 0.21875, ((1, 4),))
    up_bias = bell_draw(splits[14], (FF,), 0.5, 3.0, ((0, 4),))
    down_weight = bell_draw(splits[15], (FF, D), FF ** -0.5, 0.109375, ((0, 4),))
    down_bias = bell_draw(splits[16], (D,), 0.3, 3.0)
    mlp_scale = jnp.clip(jnp.exp(jax.random.uniform(splits[17], (D,), jnp.float32, math.log(0.5), math.log(2.0))), 0.5, 2.0)
    cotangent = bell_draw_with(splits[18], (TOKENS, D), 1.0, 6.0, ((0, 32),), (0, 1, 32, 2.75))
    return dict(patches=patches, segment_ids=segment_ids, fill_counts=fill_counts, attn_gain=attn_gain, attn_shift=attn_shift, qkv_weight=qkv_weight, qv_bias=qv_bias, rel_table=rel_table, proj_weight=proj_weight, proj_bias=proj_bias, attn_scale=attn_scale, mlp_gain=mlp_gain, mlp_shift=mlp_shift, up_weight=up_weight, up_bias=up_bias, down_weight=down_weight, down_bias=down_bias, mlp_scale=mlp_scale, cotangent=cotangent)


@jax.custom_vjp
def low(v):
    return lax.optimization_barrier(v.astype(jnp.bfloat16)).astype(jnp.float32)

@jax.custom_vjp
def low_back(v):
    return v

def low_keep(v):
    return (low(v), None)

def low_pass(kept, grad):
    return (grad,)

def back_keep(v):
    return (v, None)

def back_low(kept, grad):
    return (low(grad),)
low.defvjp(low_keep, low_pass)
low_back.defvjp(back_keep, back_low)

def matmul(left, right):
    return jnp.dot(left, right, precision=lax.Precision.HIGHEST)

def norm_rows(rows, gain, shift):
    centre = rows - lax.optimization_barrier(jnp.mean(rows, axis=-1, keepdims=True))
    normed = centre * lax.rsqrt(lax.optimization_barrier(jnp.mean(centre * centre, axis=-1, keepdims=True)) + 1e-06)
    return normed * gain + shift

def attend(table, query_seq, keys_seq, values_seq, seg_row, fill_one):
    scores = jnp.einsum('qhd,khd->hqk', query_seq, keys_seq, precision=lax.Precision.HIGHEST) * 0.125 + table
    scores = low_back(scores)
    places = jnp.arange(L).astype(jnp.int32)
    valid = places < fill_one
    allowed = (seg_row[:, None] == seg_row[None, :]) & valid[:, None] & valid[None, :] | (places[:, None] == places[None, :])
    probs = low(jax.nn.softmax(jnp.where(allowed[None], scores, -1e+30), axis=-1))
    return jnp.einsum('hqk,khd->qhd', probs, values_seq, precision=lax.Precision.HIGHEST)

def group_forward(params, rows, seg_group, fill_group):
    attn_gain, attn_shift, qkv_weight, qv_bias, rel_table, proj_weight, proj_bias, attn_scale, mlp_gain, mlp_shift, up_weight, up_bias, down_weight, down_bias, mlp_scale = params
    normed_one = low(norm_rows(rows, attn_gain, attn_shift))
    queries = low_back(low(matmul(normed_one, qkv_weight[0]) + qv_bias[0]))
    keys_all = low_back(low(matmul(normed_one, qkv_weight[1])))
    values_all = low_back(low(matmul(normed_one, qkv_weight[2]) + qv_bias[1]))
    shaped = (SEQS, L, HEADS, HEAD_DIM)

    def attend_one(items):
        return attend(rel_table, items[0], items[1], items[2], items[3], items[4])
    context = lax.map(jax.checkpoint(attend_one), (queries.reshape(shaped), keys_all.reshape(shaped), values_all.reshape(shaped), seg_group, fill_group))
    context = low_back(low(context.reshape(SEQS * L, D)))
    attn_out = low_back(matmul(context, proj_weight) + proj_bias)
    middle = rows + attn_scale * attn_out
    normed_two = low(norm_rows(middle, mlp_gain, mlp_shift))
    pre_act = low_back(matmul(normed_two, up_weight) + up_bias)
    hidden = low(jax.nn.gelu(pre_act, approximate=True))
    mlp_out = low_back(matmul(hidden, down_weight) + down_bias)
    return middle + mlp_scale * mlp_out

def reference(patches, segment_ids, fill_counts, attn_gain, attn_shift, qkv_weight, qv_bias, rel_table, proj_weight, proj_bias, attn_scale, mlp_gain, mlp_shift, up_weight, up_bias, down_weight, down_bias, mlp_scale, cotangent):
    params = (attn_gain.astype(jnp.float32), attn_shift.astype(jnp.float32), qkv_weight.astype(jnp.float32), qv_bias.astype(jnp.float32), rel_table.astype(jnp.float32), proj_weight.astype(jnp.float32), proj_bias.astype(jnp.float32), attn_scale.astype(jnp.float32), mlp_gain.astype(jnp.float32), mlp_shift.astype(jnp.float32), up_weight.astype(jnp.float32), up_bias.astype(jnp.float32), down_weight.astype(jnp.float32), down_bias.astype(jnp.float32), mlp_scale.astype(jnp.float32))
    rows_all = patches.astype(jnp.float32).reshape(N_DP, SEQS * L, D)
    cot_all = cotangent.astype(jnp.float32).reshape(N_DP, SEQS * L, D)
    seg_all = segment_ids.reshape(N_DP, SEQS, L)
    fill_all = fill_counts.reshape(N_DP, SEQS)

    def step(totals, items):
        rows, segs, fills, cots = items

        def forward(weights, inputs):
            return group_forward(weights, inputs, segs, fills)
        output, pullback = jax.vjp(forward, params, rows)
        grad_params, grad_rows = pullback(cots)
        totals = jax.tree.map(jnp.add, totals, grad_params)
        return (totals, (output.astype(jnp.bfloat16), grad_rows))
    zeros = jax.tree.map(jnp.zeros_like, params)
    totals, (outputs, grads) = lax.scan(step, zeros, (rows_all, seg_all, fill_all, cot_all))
    return (outputs.reshape(TOKENS, D), grads.reshape(TOKENS, D), totals[0], totals[1], totals[2], totals[3], totals[4], totals[5], totals[6], totals[7], totals[8], totals[9], totals[10], totals[11], totals[12], totals[13], totals[14])
```

```python
from functools import partial

import jax
import jax.numpy as jnp
from jax import lax
from jax.experimental import pallas as pl
from jax.experimental.pallas import tpu as pltpu
from jax.sharding import PartitionSpec as P

HEAD_DIM = 64
BLOCK = 256
GROUP = 128
PAGE_MOST = 256
BF = jnp.bfloat16
F32 = jnp.float32
MESH = pl.DeviceIdType.MESH
VMEM_MOST = 60 * 1024 * 1024
NT = (((1,), (1,)), ((), ()))
TN = (((0,), (0,)), ((), ()))


def vmem():
    return pl.BlockSpec(memory_space=pltpu.VMEM)


def dot(a, b):
    return jnp.dot(a, b, preferred_element_type=F32)


def dot_nt(a, b):
    return lax.dot_general(a, b, NT, preferred_element_type=F32)


def dot_tn(a, b):
    return lax.dot_general(a, b, TN, preferred_element_type=F32)


def norm_rows(rows, gain, shift):
    centre = rows - jnp.mean(rows, axis=-1, keepdims=True)
    inv_std = lax.rsqrt(jnp.mean(centre * centre, axis=-1, keepdims=True) + 1e-06)
    normed = centre * inv_std
    return (normed * gain + shift, normed, inv_std)


def norm_back(grad_out, normed, inv_std, gain):
    scaled = grad_out * gain
    inner = (
        scaled
        - jnp.mean(scaled, axis=-1, keepdims=True)
        - normed * jnp.mean(scaled * normed, axis=-1, keepdims=True)
    )
    return (inv_std * inner, jnp.sum(grad_out * normed, axis=0), jnp.sum(grad_out, axis=0))


def gelu_back(pre_act, grad):
    _, pullback = jax.vjp(partial(jax.nn.gelu, approximate=True), pre_act)
    return pullback(grad)[0]


def window(index, length):
    width = min(length, BLOCK + 2 * PAGE_MOST)
    start = jnp.clip(index * BLOCK - PAGE_MOST, 0, length - width)
    return pl.multiple_of(start, 128), width


def band_window(group, length):
    wide = min(length, GROUP + 2 * PAGE_MOST)
    start = jnp.clip(group * GROUP - PAGE_MOST, 0, length - wide)
    return pl.multiple_of(start, 128), wide


def head_lanes(head, cols):
    return lax.broadcasted_iota(jnp.int32, (1, cols), 1) // HEAD_DIM == head


def id_columns(ids_ref, cols_ref, seqs, length):
    for s in range(seqs):
        wide = jnp.broadcast_to(ids_ref[s : s + 1, :], (128, length))
        cols_ref[s * length : (s + 1) * length, :] = wide.T


def attend_body(q_ref, k_ref, v_ref, table_ref, ids_ref, cols_ref, ctx_ref, lse_ref, length, step, heads):
    cols = q_ref.shape[1]
    blocks = length // BLOCK
    seq, index = step // blocks, step % blocks
    base = seq * length
    start, width = window(index, length)
    rows = pl.ds(pl.multiple_of(base + index * BLOCK, BLOCK), BLOCK)
    keys_at = pl.ds(pl.multiple_of(base + start, 128), width)
    query = q_ref[rows, :]
    keys = k_ref[keys_at, :]
    values = v_ref[keys_at, :]
    same = cols_ref[rows, 0:1] == ids_ref[pl.ds(seq, 1), pl.ds(start, width)]
    context = jnp.zeros((BLOCK, cols), F32)
    sums = jnp.zeros((BLOCK, 128), F32)
    lane = lax.broadcasted_iota(jnp.int32, (1, 128), 1)
    for head in range(heads):
        mine = head_lanes(head, cols)
        scores = dot_nt(jnp.where(mine, query, 0), keys)
        bias = table_ref[head, pl.ds(pl.multiple_of(index * BLOCK, BLOCK), BLOCK), pl.ds(start, width)]
        scores = jnp.where(same, scores + bias.astype(F32), -1e30)
        peak = jnp.max(scores, axis=-1, keepdims=True)
        expo = jnp.exp(scores - peak)
        total = jnp.sum(expo, axis=-1, keepdims=True)
        part = dot(expo.astype(BF), values) * (1.0 / total)
        context = jnp.where(mine, part, context)
        sums = jnp.where(lane == head, peak + jnp.log(total), sums)
    ctx_ref[rows, :] = context.astype(BF)
    lse_ref[rows, :] = sums


def attend_kernel(seqs, length, heads, q_ref, k_ref, v_ref, table_ref, ids_ref, ctx_ref, lse_ref, cols_ref):
    id_columns(ids_ref, cols_ref, seqs, length)

    def step(i, _):
        attend_body(q_ref, k_ref, v_ref, table_ref, ids_ref, cols_ref, ctx_ref, lse_ref, length, i, heads)
        return 0

    lax.fori_loop(0, seqs * (length // BLOCK), step, 0)


def attend(q, k, v, table, ids):
    seqs, length = ids.shape
    rows, cols = q.shape
    heads = cols // HEAD_DIM
    return pl.pallas_call(
        partial(attend_kernel, seqs, length, heads),
        out_shape=(jax.ShapeDtypeStruct((rows, cols), BF), jax.ShapeDtypeStruct((rows, 128), F32)),
        in_specs=[vmem()] * 5,
        out_specs=(vmem(), vmem()),
        scratch_shapes=[pltpu.VMEM((rows, 128), F32)],
        compiler_params=pltpu.CompilerParams(vmem_limit_bytes=VMEM_MOST),
        name="attend",
    )(q, k, v, table, ids)


def attend_back_kernel(
    seqs, length, heads,
    q_ref, k_ref, v_ref, g_ref, lse_ref, table_ref, ids_ref,
    dq_ref, dk_ref, dv_ref, band_ref,
    cols_ref, qt_ref, gt_ref, dkt_ref, dvt_ref, total_ref,
):
    cols = q_ref.shape[1]
    blocks = length // BLOCK
    id_columns(ids_ref, cols_ref, seqs, length)
    lane = lax.broadcasted_iota(jnp.int32, (1, 128), 1)

    def flip(i, _):
        at = pl.ds(pl.multiple_of(i * BLOCK, BLOCK), BLOCK)
        qt_ref[:, at] = q_ref[at, :].T
        gt_ref[:, at] = g_ref[at, :].T
        return 0

    lax.fori_loop(0, seqs * blocks, flip, 0)
    dkt_ref[...] = jnp.zeros_like(dkt_ref)
    dvt_ref[...] = jnp.zeros_like(dvt_ref)

    def step(i, _):
        head, index = i // blocks, i % blocks
        start, width = window(index, length)
        mine = head_lanes(head, cols)
        feats = pl.ds(pl.multiple_of(head * HEAD_DIM, HEAD_DIM), HEAD_DIM)
        bias = table_ref[head, pl.ds(pl.multiple_of(index * BLOCK, BLOCK), BLOCK), pl.ds(start, width)].astype(F32)
        for seq in range(seqs):
            base = seq * length
            rows = pl.ds(pl.multiple_of(base + index * BLOCK, BLOCK), BLOCK)
            keys_at = pl.ds(pl.multiple_of(base + start, 128), width)
            keys = k_ref[keys_at, :]
            same = cols_ref[rows, 0:1] == ids_ref[seq : seq + 1, pl.ds(start, width)]
            sums = jnp.sum(jnp.where(lane == head, lse_ref[rows, :], 0.0), axis=-1, keepdims=True)
            scores = dot_nt(jnp.where(mine, q_ref[rows, :], 0), keys) + bias
            probs = jnp.where(same, jnp.exp(scores - sums), 0.0)
            grad_probs = dot_nt(jnp.where(mine, g_ref[rows, :], 0), v_ref[keys_at, :])
            centre = jnp.sum(grad_probs * probs, axis=-1, keepdims=True)
            grad_scores = (probs * (grad_probs - centre)).astype(BF)
            dvt_ref[feats, keys_at] += dot(gt_ref[feats, rows], probs.astype(BF))
            dkt_ref[feats, keys_at] += dot(qt_ref[feats, rows], grad_scores)
            grad_q = (dot(grad_scores, keys) * 0.125).astype(BF)
            dq_ref[rows, :] = jnp.where(mine, grad_q, dq_ref[rows, :])
            if seq == 0:
                total_ref[:, 0:width] = grad_scores.astype(F32)
            else:
                total_ref[:, 0:width] += grad_scores.astype(F32)
        for part in range(BLOCK // GROUP):
            owner = index * (BLOCK // GROUP) + part
            first, wide = band_window(owner, length)
            offset = pl.multiple_of(first - start, 128)
            band_ref[owner, head, :, :] = total_ref[part * GROUP : (part + 1) * GROUP, pl.ds(offset, wide)].astype(BF)
        return 0

    dq_ref[...] = jnp.zeros_like(dq_ref)
    total_ref[...] = jnp.zeros_like(total_ref)
    lax.fori_loop(0, heads * blocks, step, 0)

    def finish(i, _):
        at = pl.ds(pl.multiple_of(i * BLOCK, BLOCK), BLOCK)
        dk_ref[at, :] = dkt_ref[:, at].T.astype(BF)
        dv_ref[at, :] = dvt_ref[:, at].T.astype(BF)
        return 0

    lax.fori_loop(0, seqs * blocks, finish, 0)


def attend_back(q, k, v, g, lse, table, ids):
    seqs, length = ids.shape
    rows, cols = q.shape
    heads = cols // HEAD_DIM
    wide = band_window(0, length)[1]
    width = min(length, BLOCK + 2 * PAGE_MOST)
    one = jax.ShapeDtypeStruct((rows, cols), BF)
    return pl.pallas_call(
        partial(attend_back_kernel, seqs, length, heads),
        out_shape=(one, one, one, jax.ShapeDtypeStruct((length // GROUP, heads, GROUP, wide), BF)),
        in_specs=[vmem()] * 7,
        out_specs=(vmem(),) * 4,
        scratch_shapes=[
            pltpu.VMEM((rows, 128), F32),
            pltpu.VMEM((cols, rows), BF),
            pltpu.VMEM((cols, rows), BF),
            pltpu.VMEM((cols, rows), F32),
            pltpu.VMEM((cols, rows), F32),
            pltpu.VMEM((BLOCK, width), F32),
        ],
        compiler_params=pltpu.CompilerParams(vmem_limit_bytes=VMEM_MOST),
        name="attend_back",
    )(q, k, v, g, lse, table, ids)


def scatter_dp(x):
    return lax.psum_scatter(x, "dp", scatter_dimension=0, tiled=True).astype(F32)


def scatter_mp(x):
    return lax.psum_scatter(x.astype(BF), "mp", scatter_dimension=0, tiled=True).astype(F32)


def reduce_table(band, length, n_dp):
    groups, heads, _, wide = band.shape
    shard = length // n_dp
    send = band.reshape(groups, heads, GROUP // shard, shard, wide).swapaxes(1, 2)
    part = scatter_dp(send.reshape(n_dp * heads * shard, wide)).reshape(heads, shard, wide)
    first = band_window(lax.axis_index("dp") * shard // GROUP, length)[0]
    return lax.dynamic_update_slice(jnp.zeros((heads, shard, length), F32), part, (0, 0, first))


def local(
    patches, segment_ids, fill_counts, attn_gain, attn_shift, qkv_weight, qv_bias, rel_table, proj_weight,
    proj_bias, attn_scale, mlp_gain, mlp_shift, up_weight, up_bias, down_weight, down_bias, mlp_scale, cotangent,
):
    n_dp = lax.axis_size("dp")
    seqs, length = segment_ids.shape
    cols = qkv_weight.shape[2]
    heads = cols // HEAD_DIM
    places = jnp.arange(length, dtype=jnp.int32)[None]
    ids = jnp.where(places < fill_counts[:, None], segment_ids, -1 - places).astype(F32)
    inputs = patches.astype(F32)
    grad_top = cotangent.astype(F32)
    normed_one, hat_one, inv_one = norm_rows(inputs, attn_gain, attn_shift)
    rows_one = lax.all_gather(normed_one.astype(BF), "mp", axis=0, tiled=True)
    grad_mlp = (grad_top * mlp_scale).astype(BF)
    grad_rows = lax.all_gather(grad_mlp, "mp", axis=0, tiled=True)
    queries = ((dot(rows_one, qkv_weight[0]) + qv_bias[0].astype(F32)).astype(BF) * 0.125).astype(BF)
    keys = dot(rows_one, qkv_weight[1]).astype(BF)
    values = (dot(rows_one, qkv_weight[2]) + qv_bias[1].astype(F32)).astype(BF)
    context, lse = attend(queries, keys, values, rel_table, ids)
    attn_out = scatter_mp(dot(context, proj_weight)) + proj_bias.astype(F32)
    middle = inputs + attn_scale * attn_out
    normed_two, hat_two, inv_two = norm_rows(middle, mlp_gain, mlp_shift)
    rows_two = lax.all_gather(normed_two.astype(BF), "mp", axis=0, tiled=True)
    pre_act = dot(rows_two, up_weight) + up_bias.astype(F32)
    hidden = jax.nn.gelu(pre_act, approximate=True).astype(BF)
    grad_hidden = dot_nt(grad_rows, down_weight)
    grad_pre = gelu_back(pre_act, grad_hidden).astype(BF)
    grad_norm_two = scatter_mp(dot_nt(grad_pre, up_weight))
    mlp_out = scatter_mp(dot(hidden, down_weight)) + down_bias.astype(F32)
    layer_out = (middle + mlp_scale * mlp_out).astype(BF)
    up_local = dot_tn(rows_two, grad_pre).astype(BF)
    down_local = dot_tn(grad_rows, hidden).astype(BF)
    up_grad = scatter_dp(up_local)
    down_grad = scatter_dp(down_local).T
    up_bias_local = jnp.sum(grad_pre.astype(F32), axis=0)
    scale_two_grad = jnp.sum(grad_top * mlp_out, axis=0)
    down_bias_grad = jnp.sum(grad_mlp.astype(F32), axis=0)
    back_two, gain_two_grad, shift_two_grad = norm_back(grad_norm_two, hat_two, inv_two, mlp_gain)
    grad_middle = grad_top + back_two
    grad_attn = (grad_middle * attn_scale).astype(BF)
    scale_one_grad = jnp.sum(grad_middle * attn_out, axis=0)
    proj_bias_grad = jnp.sum(grad_attn.astype(F32), axis=0)
    attn_grad_rows = lax.all_gather(grad_attn, "mp", axis=0, tiled=True)
    grad_context = dot_nt(attn_grad_rows, proj_weight).astype(BF)
    grad_q, grad_k, grad_v, band = attend_back(queries, keys, values, grad_context, lse, rel_table, ids)
    total = dot_nt(grad_q, qkv_weight[0]) + dot_nt(grad_k, qkv_weight[1]) + dot_nt(grad_v, qkv_weight[2])
    grad_norm_one = scatter_mp(total)
    table_grad = reduce_table(band, length, n_dp)
    mixed = jnp.concatenate(
        [dot_tn(rows_one, grad_q), dot_tn(rows_one, grad_k), dot_tn(rows_one, grad_v), dot_tn(attn_grad_rows, context)],
        axis=1,
    ).astype(BF)
    mixed = scatter_dp(mixed)
    qkv_grad = mixed[:, : 3 * cols].reshape(-1, 3, cols).swapaxes(0, 1)
    proj_grad = mixed[:, 3 * cols :].T
    qv_bias_local = jnp.stack([jnp.sum(grad_q.astype(F32), axis=0), jnp.sum(grad_v.astype(F32), axis=0)])
    back_one, gain_one_grad, shift_one_grad = norm_back(grad_norm_one, hat_one, inv_one, attn_gain)
    patch_grad = grad_middle + back_one
    small = lax.psum(
        jnp.stack(
            [
                gain_one_grad, shift_one_grad, proj_bias_grad, scale_one_grad,
                gain_two_grad, shift_two_grad, down_bias_grad, scale_two_grad,
            ]
        ),
        ("dp", "mp"),
    )
    qv_bias_grad, up_bias_grad = lax.psum((qv_bias_local, up_bias_local), "dp")
    return (
        layer_out, patch_grad, small[0], small[1], qkv_grad, qv_bias_grad, table_grad, proj_grad, small[2], small[3],
        small[4], small[5], up_grad, up_bias_grad, down_grad, small[6], small[7],
    )


def solution(mesh):
    rows, split = P(("dp", "mp"), None), P("mp", None)
    placed = (
        rows, P("dp", None), P("dp"), P(), P(), P(None, None, "mp"), P(None, "mp"), P("mp", None, None), split,
        P(), P(), P(), P(), P(None, "mp"), P("mp"), split, P(), P(), rows,
    )
    given = (
        rows, rows, P(), P(), P(None, "dp", "mp"), P(None, "mp"), P("mp", "dp", None), P("mp", "dp"), P(), P(),
        P(), P(), P("dp", "mp"), P("mp"), P("mp", "dp"), P(), P(),
    )
    return jax.shard_map(local, mesh=mesh, in_specs=placed, out_specs=given, check_vma=False)
```

```python
from functools import partial

import jax
import jax.numpy as jnp
from jax import lax
from jax.experimental import pallas as pl
from jax.experimental.pallas import tpu as pltpu
from jax.sharding import PartitionSpec as P

HEAD_DIM = 64
BLOCK = 256
GROUP = 128
PAGE_MOST = 256
BF = jnp.bfloat16
F32 = jnp.float32
MESH = pl.DeviceIdType.MESH
VMEM_MOST = 60 * 1024 * 1024
NT = (((1,), (1,)), ((), ()))
TN = (((0,), (0,)), ((), ()))


def vmem():
    return pl.BlockSpec(memory_space=pltpu.VMEM)


def dot(a, b):
    return jnp.dot(a, b, preferred_element_type=F32)


def dot_nt(a, b):
    return lax.dot_general(a, b, NT, preferred_element_type=F32)


def dot_tn(a, b):
    return lax.dot_general(a, b, TN, preferred_element_type=F32)


def norm_rows(rows, gain, shift):
    centre = rows - jnp.mean(rows, axis=-1, keepdims=True)
    inv_std = lax.rsqrt(jnp.mean(centre * centre, axis=-1, keepdims=True) + 1e-06)
    normed = centre * inv_std
    return (normed * gain + shift, normed, inv_std)


def norm_back(grad_out, normed, inv_std, gain):
    scaled = grad_out * gain
    inner = (
        scaled
        - jnp.mean(scaled, axis=-1, keepdims=True)
        - normed * jnp.mean(scaled * normed, axis=-1, keepdims=True)
    )
    return (inv_std * inner, jnp.sum(grad_out * normed, axis=0), jnp.sum(grad_out, axis=0))


def window(index, length):
    width = min(length, BLOCK + 2 * PAGE_MOST)
    start = jnp.clip(index * BLOCK - PAGE_MOST, 0, length - width)
    return pl.multiple_of(start, 128), width


def band_window(group, length):
    wide = min(length, GROUP + 2 * PAGE_MOST)
    start = jnp.clip(group * GROUP - PAGE_MOST, 0, length - wide)
    return pl.multiple_of(start, 128), wide


def head_lanes(head, cols):
    return lax.broadcasted_iota(jnp.int32, (1, cols), 1) // HEAD_DIM == head


def id_columns(ids_ref, cols_ref, seqs, length):
    for s in range(seqs):
        wide = jnp.broadcast_to(ids_ref[s : s + 1, :], (128, length))
        cols_ref[s * length : (s + 1) * length, :] = wide.T


def attend_body(q_ref, k_ref, v_ref, table_ref, ids_ref, cols_ref, ctx_ref, lse_ref, length, step, heads):
    cols = q_ref.shape[1]
    blocks = length // BLOCK
    seq, index = step // blocks, step % blocks
    base = seq * length
    start, width = window(index, length)
    rows = pl.ds(pl.multiple_of(base + index * BLOCK, BLOCK), BLOCK)
    keys_at = pl.ds(pl.multiple_of(base + start, 128), width)
    query = q_ref[rows, :]
    keys = k_ref[keys_at, :]
    values = v_ref[keys_at, :]
    same = cols_ref[rows, 0:1] == ids_ref[pl.ds(seq, 1), pl.ds(start, width)]
    context = jnp.zeros((BLOCK, cols), F32)
    sums = jnp.zeros((BLOCK, 128), F32)
    lane = lax.broadcasted_iota(jnp.int32, (1, 128), 1)
    for head in range(heads):
        mine = head_lanes(head, cols)
        scores = dot_nt(jnp.where(mine, query, 0), keys)
        bias = table_ref[head, pl.ds(pl.multiple_of(index * BLOCK, BLOCK), BLOCK), pl.ds(start, width)]
        scores = jnp.where(same, scores + bias.astype(F32), -1e30)
        peak = jnp.max(scores, axis=-1, keepdims=True)
        expo = jnp.exp(scores - peak)
        total = jnp.sum(expo, axis=-1, keepdims=True)
        part = dot(expo.astype(BF), values) * (1.0 / total)
        context = jnp.where(mine, part, context)
        sums = jnp.where(lane == head, peak + jnp.log(total), sums)
    ctx_ref[rows, :] = context.astype(BF)
    lse_ref[rows, :] = sums


def attend_kernel(seqs, length, heads, q_ref, k_ref, v_ref, table_ref, ids_ref, ctx_ref, lse_ref, cols_ref):
    id_columns(ids_ref, cols_ref, seqs, length)

    def step(i, _):
        attend_body(q_ref, k_ref, v_ref, table_ref, ids_ref, cols_ref, ctx_ref, lse_ref, length, i, heads)
        return 0

    lax.fori_loop(0, seqs * (length // BLOCK), step, 0)


def attend(q, k, v, table, ids):
    seqs, length = ids.shape
    rows, cols = q.shape
    heads = cols // HEAD_DIM
    return pl.pallas_call(
        partial(attend_kernel, seqs, length, heads),
        out_shape=(jax.ShapeDtypeStruct((rows, cols), BF), jax.ShapeDtypeStruct((rows, 128), F32)),
        in_specs=[vmem()] * 5,
        out_specs=(vmem(), vmem()),
        scratch_shapes=[pltpu.VMEM((rows, 128), F32)],
        compiler_params=pltpu.CompilerParams(vmem_limit_bytes=VMEM_MOST),
        name="attend",
    )(q, k, v, table, ids)


def attend_back_kernel(
    seqs, length, heads,
    q_ref, k_ref, v_ref, g_ref, lse_ref, table_ref, ids_ref,
    dq_ref, dk_ref, dv_ref, band_ref,
    cols_ref, qt_ref, gt_ref, dkt_ref, dvt_ref, total_ref,
):
    cols = q_ref.shape[1]
    blocks = length // BLOCK
    id_columns(ids_ref, cols_ref, seqs, length)
    lane = lax.broadcasted_iota(jnp.int32, (1, 128), 1)

    def flip(i, _):
        at = pl.ds(pl.multiple_of(i * BLOCK, BLOCK), BLOCK)
        qt_ref[:, at] = q_ref[at, :].T
        gt_ref[:, at] = g_ref[at, :].T
        return 0

    lax.fori_loop(0, seqs * blocks, flip, 0)
    dkt_ref[...] = jnp.zeros_like(dkt_ref)
    dvt_ref[...] = jnp.zeros_like(dvt_ref)

    def step(i, _):
        head, index = i // blocks, i % blocks
        start, width = window(index, length)
        mine = head_lanes(head, cols)
        feats = pl.ds(pl.multiple_of(head * HEAD_DIM, HEAD_DIM), HEAD_DIM)
        bias = table_ref[head, pl.ds(pl.multiple_of(index * BLOCK, BLOCK), BLOCK), pl.ds(start, width)].astype(F32)
        for seq in range(seqs):
            base = seq * length
            rows = pl.ds(pl.multiple_of(base + index * BLOCK, BLOCK), BLOCK)
            keys_at = pl.ds(pl.multiple_of(base + start, 128), width)
            keys = k_ref[keys_at, :]
            same = cols_ref[rows, 0:1] == ids_ref[seq : seq + 1, pl.ds(start, width)]
            sums = jnp.sum(jnp.where(lane == head, lse_ref[rows, :], 0.0), axis=-1, keepdims=True)
            scores = dot_nt(jnp.where(mine, q_ref[rows, :], 0), keys) + bias
            probs = jnp.where(same, jnp.exp(scores - sums), 0.0)
            grad_probs = dot_nt(jnp.where(mine, g_ref[rows, :], 0), v_ref[keys_at, :])
            centre = jnp.sum(grad_probs * probs, axis=-1, keepdims=True)
            grad_scores = (probs * (grad_probs - centre)).astype(BF)
            dvt_ref[feats, keys_at] += dot(gt_ref[feats, rows], probs.astype(BF))
            dkt_ref[feats, keys_at] += dot(qt_ref[feats, rows], grad_scores)
            grad_q = (dot(grad_scores, keys) * 0.125).astype(BF)
            dq_ref[rows, :] = jnp.where(mine, grad_q, dq_ref[rows, :])
            if seq == 0:
                total_ref[:, 0:width] = grad_scores.astype(F32)
            else:
                total_ref[:, 0:width] += grad_scores.astype(F32)
        for part in range(BLOCK // GROUP):
            owner = index * (BLOCK // GROUP) + part
            first, wide = band_window(owner, length)
            offset = pl.multiple_of(first - start, 128)
            band_ref[owner, head, :, :] = total_ref[part * GROUP : (part + 1) * GROUP, pl.ds(offset, wide)].astype(BF)
        return 0

    dq_ref[...] = jnp.zeros_like(dq_ref)
    total_ref[...] = jnp.zeros_like(total_ref)
    lax.fori_loop(0, heads * blocks, step, 0)

    def finish(i, _):
        at = pl.ds(pl.multiple_of(i * BLOCK, BLOCK), BLOCK)
        dk_ref[at, :] = dkt_ref[:, at].T.astype(BF)
        dv_ref[at, :] = dvt_ref[:, at].T.astype(BF)
        return 0

    lax.fori_loop(0, seqs * blocks, finish, 0)


def attend_back(q, k, v, g, lse, table, ids):
    seqs, length = ids.shape
    rows, cols = q.shape
    heads = cols // HEAD_DIM
    wide = band_window(0, length)[1]
    width = min(length, BLOCK + 2 * PAGE_MOST)
    one = jax.ShapeDtypeStruct((rows, cols), BF)
    return pl.pallas_call(
        partial(attend_back_kernel, seqs, length, heads),
        out_shape=(one, one, one, jax.ShapeDtypeStruct((length // GROUP, heads, GROUP, wide), BF)),
        in_specs=[vmem()] * 7,
        out_specs=(vmem(),) * 4,
        scratch_shapes=[
            pltpu.VMEM((rows, 128), F32),
            pltpu.VMEM((cols, rows), BF),
            pltpu.VMEM((cols, rows), BF),
            pltpu.VMEM((cols, rows), F32),
            pltpu.VMEM((cols, rows), F32),
            pltpu.VMEM((BLOCK, width), F32),
        ],
        compiler_params=pltpu.CompilerParams(vmem_limit_bytes=VMEM_MOST),
        name="attend_back",
    )(q, k, v, g, lse, table, ids)


CHUNKS = 4


def loop(count, body):
    lax.fori_loop(0, count, lambda i, _: (body(i), 0)[1], 0)


def neighbours():
    me = lax.axis_index("mp")
    partner = me + 1 - 2 * lax.rem(me, 2)
    return me, partner, lax.rem(me + 2, 4), lax.rem(partner + 2, 4)


def greet(peers):
    barrier = pltpu.get_barrier_semaphore()
    for peer in peers:
        pl.semaphore_signal(barrier, inc=1, device_id=peer, device_id_type=MESH)
    pl.semaphore_wait(barrier, len(peers))


def greet_mp():
    _, partner, cross, _ = neighbours()
    greet(({"mp": partner}, {"mp": cross}))


class Gather:
    def __init__(self, buffer, send, recv):
        self.buffer, self.send, self.recv = buffer, send, recv
        self.size = buffer.shape[0] // 4 // CHUNKS
        self.me, self.partner, self.cross, self.diag = neighbours()

    def rows(self, block, chunk):
        return pl.ds(pl.multiple_of((block * CHUNKS + chunk) * self.size, self.size), self.size)

    def copy(self, kind, block, chunk):
        part = self.buffer.at[self.rows(block, chunk), :]
        return pltpu.make_async_remote_copy(
            src_ref=part, dst_ref=part, send_sem=self.send.at[kind, chunk], recv_sem=self.recv.at[kind, chunk],
            device_id={"mp": self.cross if kind == 0 else self.partner}, device_id_type=MESH,
        )

    def send_own(self, chunk):
        self.copy(0, self.me, chunk).start()
        self.copy(1, self.me, chunk).start()

    def wait_partner(self, chunk):
        self.copy(1, self.partner, chunk).wait_recv()

    def relay(self, chunk):
        self.copy(0, self.cross, chunk).wait_recv()
        self.copy(2, self.cross, chunk).start()

    def wait_diag(self, chunk):
        self.copy(2, self.diag, chunk).wait_recv()

    def drain(self, chunk):
        self.copy(0, self.me, chunk).wait_send()
        self.copy(1, self.me, chunk).wait_send()
        self.copy(2, self.cross, chunk).wait_send()


class Scatter:
    def __init__(self, out, inn, send, recv):
        self.out, self.inn, self.send, self.recv = out, inn, send, recv
        self.size = out.shape[1] // CHUNKS
        self.me, self.partner, self.cross, self.diag = neighbours()

    def rows(self, chunk):
        return pl.ds(pl.multiple_of(chunk * self.size, self.size), self.size)

    def copy(self, kind, chunk):
        return pltpu.make_async_remote_copy(
            src_ref=self.out.at[kind, self.rows(chunk), :], dst_ref=self.inn.at[kind, self.rows(chunk), :],
            send_sem=self.send.at[kind, chunk], recv_sem=self.recv.at[kind, chunk],
            device_id={"mp": self.cross if kind == 1 else self.partner}, device_id_type=MESH,
        )

    def put(self, kind, chunk, value):
        self.out[kind, self.rows(chunk), :] = value.astype(BF)
        self.copy(kind, chunk).start()

    def take(self, kind, chunk):
        self.copy(kind, chunk).wait_recv()
        return self.inn[kind, self.rows(chunk), :].astype(F32)

    def drain(self, chunk):
        for kind in range(3):
            self.copy(kind, chunk).wait_send()


def moves():
    return [pltpu.SemaphoreType.DMA((3, CHUNKS)), pltpu.SemaphoreType.DMA((3, CHUNKS))]


def halves(rows, cols):
    return [pltpu.VMEM((3, rows, cols), BF), pltpu.VMEM((3, rows, cols), BF)] + moves()


def call(kernel, name, number, outs, scratch, *args):
    return pl.pallas_call(
        kernel,
        out_shape=tuple(jax.ShapeDtypeStruct(shape, dtype) for shape, dtype in outs),
        in_specs=[vmem()] * len(args),
        out_specs=tuple(vmem() for _ in outs),
        scratch_shapes=scratch,
        compiler_params=pltpu.CompilerParams(
            vmem_limit_bytes=VMEM_MOST, collective_id=number, has_side_effects=True
        ),
        name=name,
    )(*args)


def gather_qkv_kernel(x_ref, gain_ref, shift_ref, w_ref, bias_ref, rows_ref, q_ref, k_ref, v_ref, send, recv):
    net = Gather(rows_ref, send, recv)
    greet_mp()

    def own(chunk):
        part = x_ref[pl.ds(pl.multiple_of(chunk * net.size, net.size), net.size), :].astype(F32)
        rows_ref[net.rows(net.me, chunk), :] = norm_rows(part, gain_ref[...], shift_ref[...])[0].astype(BF)
        net.send_own(chunk)

    loop(CHUNKS, own)
    tall = 2 * net.size

    def project(block):
        def part(i):
            at = pl.ds(pl.multiple_of(block * CHUNKS * net.size + i * tall, tall), tall)
            rows = rows_ref[at, :]
            query = dot(rows, w_ref[0]) + bias_ref[0:1, :].astype(F32)
            q_ref[at, :] = (query.astype(BF).astype(F32) * 0.125).astype(BF)
            k_ref[at, :] = dot(rows, w_ref[1]).astype(BF)
            v_ref[at, :] = (dot(rows, w_ref[2]) + bias_ref[1:2, :].astype(F32)).astype(BF)

        loop(CHUNKS // 2, part)

    project(net.me)
    loop(CHUNKS, net.wait_partner)
    project(net.partner)
    loop(CHUNKS, net.relay)
    project(net.cross)
    loop(CHUNKS, net.wait_diag)
    project(net.diag)
    loop(CHUNKS, net.drain)


def gather_qkv(patches, gain, shift, weight, bias):
    rows, width = patches.shape
    cols = weight.shape[2]
    one = ((4 * rows, cols), BF)
    return call(
        gather_qkv_kernel, "gather_qkv", 1, [((4 * rows, width), BF), one, one, one], moves(),
        patches, gain[None], shift[None], weight, bias,
    )


def project_kernel(
    ctx_ref, w_ref, bias_ref, x_ref, scale_ref, gain_ref, shift_ref, attn_ref, mid_ref, norm_ref, out, inn, send, recv
):
    net = Scatter(out, inn, send, recv)
    greet_mp()

    def share(block, chunk):
        at = pl.ds(pl.multiple_of((block * CHUNKS + chunk) * net.size, net.size), net.size)
        return dot(ctx_ref[at, :], w_ref[...])

    loop(CHUNKS, lambda c: net.put(0, c, share(net.diag, c)))
    loop(CHUNKS, lambda c: net.put(1, c, share(net.cross, c) + net.take(0, c)))
    loop(CHUNKS, lambda c: net.put(2, c, share(net.partner, c)))

    def own(chunk):
        attn_ref[net.rows(chunk), :] = share(net.me, chunk) + net.take(2, chunk) + bias_ref[...].astype(F32)

    loop(CHUNKS, own)

    def last(chunk):
        at = net.rows(chunk)
        attn = attn_ref[at, :] + net.take(1, chunk)
        middle = x_ref[at, :].astype(F32) + scale_ref[...] * attn
        attn_ref[at, :] = attn
        mid_ref[at, :] = middle
        norm_ref[at, :] = norm_rows(middle, gain_ref[...], shift_ref[...])[0].astype(BF)

    loop(CHUNKS, last)
    loop(CHUNKS, net.drain)


def project(context, weight, bias, patches, scale, gain, shift):
    rows, width = patches.shape
    return call(
        project_kernel, "project", 2, [((rows, width), F32), ((rows, width), F32), ((rows, width), BF)],
        halves(rows, width), context, weight, bias[None], patches, scale[None], gain[None], shift[None],
    )


def gelu_both(u):
    inner = 0.7978845608028654 * (u + 0.044715 * (u * u * u))
    t = jnp.tanh(inner)
    half = 0.5 * (1.0 + t)
    slope = half + (0.5 * u) * (1.0 - t * t) * (0.7978845608028654 * (1.0 + 0.134145 * (u * u)))
    return u * half, slope


def mlp_kernel(
    norm_ref, grad_ref, up_ref, bias_ref, down_ref, mid_ref, attn_ref, cot_ref, gain_ref, scale_ref,
    gmid_ref, gattn_ref, share_ref, upg_ref, downg_ref, sums_ref,
    rows_ref, hid_ref, pre_ref, own_ref, far_ref, gsend, grecv, out, inn, send, recv,
):
    gat = Gather(rows_ref, gsend, grecv)
    net = Scatter(out, inn, send, recv)
    size = gat.size
    greet_mp()
    sums_ref[...] = jnp.zeros_like(sums_ref)

    def own(chunk):
        rows_ref[gat.rows(gat.me, chunk), :] = norm_ref[net.rows(chunk), :]
        gat.send_own(chunk)

    loop(CHUNKS, own)

    def two(first, second, chunk):
        at, by = gat.rows(first, chunk), gat.rows(second, chunk)
        both = lambda ref: jnp.concatenate([ref[at, :], ref[by, :]], axis=0)
        value, slope = gelu_both(dot(both(rows_ref), up_ref[...]) + bias_ref[...].astype(F32))
        hidden = value.astype(BF)
        hid_ref[at, :], hid_ref[by, :] = hidden[:size], hidden[size:]
        grad_pre = (dot_nt(both(grad_ref), down_ref[...]) * slope).astype(BF)
        pre_ref[at, :], pre_ref[by, :] = grad_pre[:size], grad_pre[size:]
        sums_ref[0:1, :] += jnp.sum(grad_pre.astype(F32), axis=0, keepdims=True)
        part = dot(hidden, down_ref[...]).astype(BF)
        share_ref[at, :], share_ref[by, :] = part[:size], part[size:]
        back = dot_nt(grad_pre, up_ref[...])
        return back[:size], back[size:]

    def near(chunk):
        gat.wait_partner(chunk)
        theirs, mine = two(gat.partner, gat.me, chunk)
        net.put(2, chunk, theirs)
        own_ref[net.rows(chunk), :] = mine

    loop(CHUNKS, near)

    def across(chunk):
        net.put(1, chunk, far_ref[net.rows(chunk), :] + net.take(0, chunk))

    def far(chunk):
        gat.relay(chunk)
        gat.wait_diag(chunk)
        theirs, mine = two(gat.diag, gat.cross, chunk)
        net.put(0, chunk, theirs)
        far_ref[net.rows(chunk), :] = mine

        @pl.when(chunk > 0)
        def _():
            across(chunk - 1)

    loop(CHUNKS, far)
    across(CHUNKS - 1)
    tile = 256

    def weights(i):
        at = pl.ds(pl.multiple_of(i * tile, tile), tile)
        upg_ref[at, :] = dot_tn(rows_ref[:, at], pre_ref[...]).astype(BF)
        downg_ref[at, :] = dot_tn(grad_ref[:, at], hid_ref[...]).astype(BF)

    loop(rows_ref.shape[1] // tile, weights)

    def last(chunk):
        at = net.rows(chunk)
        grad = own_ref[at, :] + net.take(2, chunk) + net.take(1, chunk)
        normed, inv = norm_rows(mid_ref[at, :], 1.0, 0.0)[1:]
        back, gain_sum, shift_sum = norm_back(grad, normed, inv, gain_ref[...])
        middle = cot_ref[at, :].astype(F32) + back
        gattn = (middle * scale_ref[...]).astype(BF)
        gmid_ref[at, :] = middle
        gattn_ref[at, :] = gattn
        sums_ref[1:2, :] += gain_sum[None]
        sums_ref[2:3, :] += shift_sum[None]
        sums_ref[3:4, :] += jnp.sum(middle * attn_ref[at, :], axis=0, keepdims=True)
        sums_ref[4:5, :] += jnp.sum(gattn.astype(F32), axis=0, keepdims=True)

    loop(CHUNKS, last)
    loop(CHUNKS, gat.drain)
    loop(CHUNKS, net.drain)


def mlp(normed, grad_rows, up, bias, down, middle, attn, cotangent, gain, scale):
    rows, width = normed.shape
    ff = up.shape[1]
    return call(
        mlp_kernel, "mlp", 3,
        [
            ((rows, width), F32), ((rows, width), BF), ((4 * rows, width), BF), ((width, ff), BF), ((width, ff), BF),
            ((8, width), F32),
        ],
        [
            pltpu.VMEM((4 * rows, width), BF), pltpu.VMEM((4 * rows, ff), BF), pltpu.VMEM((4 * rows, ff), BF),
            pltpu.VMEM((rows, width), F32), pltpu.VMEM((rows, width), F32),
        ] + moves() + halves(rows, width),
        normed, grad_rows, up, bias[None], down, middle, attn, cotangent, gain[None], scale[None],
    )


def gather_back_kernel(g_ref, w_ref, ctx_ref, back_ref, proj_ref, rows_ref, send, recv):
    net = Gather(rows_ref, send, recv)
    greet_mp()

    def own(chunk):
        at = pl.ds(pl.multiple_of(chunk * net.size, net.size), net.size)
        rows_ref[net.rows(net.me, chunk), :] = g_ref[at, :]
        net.send_own(chunk)

    loop(CHUNKS, own)

    def block(number):
        size = CHUNKS * net.size
        at = pl.ds(pl.multiple_of(number * size, size), size)
        back_ref[at, :] = dot_nt(rows_ref[at, :], w_ref[...]).astype(BF)

    block(net.me)
    loop(CHUNKS, net.wait_partner)
    block(net.partner)
    loop(CHUNKS, net.relay)
    block(net.cross)
    loop(CHUNKS, net.wait_diag)
    block(net.diag)
    tile = 256

    def weights(i):
        at = pl.ds(pl.multiple_of(i * tile, tile), tile)
        proj_ref[at, :] = dot_tn(rows_ref[:, at], ctx_ref[...]).astype(BF)

    loop(rows_ref.shape[1] // tile, weights)
    loop(CHUNKS, net.drain)


def gather_back(grad, weight, context):
    rows, width = grad.shape
    cols = weight.shape[0]
    return call(
        gather_back_kernel, "gather_back", 4, [((4 * rows, cols), BF), ((width, cols), BF)],
        [pltpu.VMEM((4 * rows, width), BF)] + moves(), grad, weight, context,
    )


def tail_kernel(
    dq_ref, dk_ref, dv_ref, w_ref, rows_ref, x_ref, gmid_ref, gain_ref,
    grad_ref, qkv_ref, sums_ref, bias_ref, own_ref, out, inn, send, recv,
):
    net = Scatter(out, inn, send, recv)
    cols = dq_ref.shape[1]
    greet_mp()

    def share(block, chunk):
        at = pl.ds(pl.multiple_of((block * CHUNKS + chunk) * net.size, net.size), net.size)
        return dot_nt(dq_ref[at, :], w_ref[0]) + dot_nt(dk_ref[at, :], w_ref[1]) + dot_nt(dv_ref[at, :], w_ref[2])

    loop(CHUNKS, lambda c: net.put(0, c, share(net.diag, c)))
    loop(CHUNKS, lambda c: net.put(1, c, share(net.cross, c) + net.take(0, c)))
    loop(CHUNKS, lambda c: net.put(2, c, share(net.partner, c)))
    tile = 256

    def weights(i):
        at = pl.ds(pl.multiple_of(i * tile, tile), tile)
        rows = rows_ref[:, at]
        for number, ref in enumerate((dq_ref, dk_ref, dv_ref)):
            qkv_ref[at, number * cols : (number + 1) * cols] = dot_tn(rows, ref[...]).astype(BF)

    loop(rows_ref.shape[1] // tile, weights)
    bias_ref[0:1, :] = jnp.sum(dq_ref[...].astype(F32), axis=0, keepdims=True)
    bias_ref[1:2, :] = jnp.sum(dv_ref[...].astype(F32), axis=0, keepdims=True)

    def own(chunk):
        own_ref[net.rows(chunk), :] = share(net.me, chunk) + net.take(2, chunk)

    loop(CHUNKS, own)
    sums_ref[...] = jnp.zeros_like(sums_ref)

    def last(chunk):
        at = net.rows(chunk)
        grad = own_ref[at, :] + net.take(1, chunk)
        normed, inv = norm_rows(x_ref[at, :].astype(F32), 1.0, 0.0)[1:]
        back, gain_sum, shift_sum = norm_back(grad, normed, inv, gain_ref[...])
        grad_ref[at, :] = gmid_ref[at, :] + back
        sums_ref[0:1, :] += gain_sum[None]
        sums_ref[1:2, :] += shift_sum[None]

    loop(CHUNKS, last)
    loop(CHUNKS, net.drain)


def tail(dq, dk, dv, weight, rows_one, patches, grad_middle, gain):
    rows, width = patches.shape
    cols = dq.shape[1]
    return call(
        tail_kernel, "tail", 5,
        [((rows, width), F32), ((width, 3 * cols), BF), ((8, width), F32), ((2, cols), F32)],
        [pltpu.VMEM((rows, width), F32)] + halves(rows, width),
        dq, dk, dv, weight, rows_one, patches, grad_middle, gain[None],
    )


def scatter_dp(x):
    return lax.psum_scatter(x, "dp", scatter_dimension=0, tiled=True).astype(F32)


def scatter_mp(x):
    return lax.psum_scatter(x.astype(BF), "mp", scatter_dimension=0, tiled=True).astype(F32)


def reduce_table(band, length, n_dp):
    groups, heads, _, wide = band.shape
    shard = length // n_dp
    send = band.reshape(groups, heads, GROUP // shard, shard, wide).swapaxes(1, 2)
    part = scatter_dp(send.reshape(n_dp * heads * shard, wide)).reshape(heads, shard, wide)
    first = band_window(lax.axis_index("dp") * shard // GROUP, length)[0]
    return lax.dynamic_update_slice(jnp.zeros((heads, shard, length), F32), part, (0, 0, first))


def local(
    patches, segment_ids, fill_counts, attn_gain, attn_shift, qkv_weight, qv_bias, rel_table, proj_weight,
    proj_bias, attn_scale, mlp_gain, mlp_shift, up_weight, up_bias, down_weight, down_bias, mlp_scale, cotangent,
):
    n_dp = lax.axis_size("dp")
    seqs, length = segment_ids.shape
    cols = qkv_weight.shape[2]
    heads = cols // HEAD_DIM
    places = jnp.arange(length, dtype=jnp.int32)[None]
    ids = jnp.where(places < fill_counts[:, None], segment_ids, -1 - places).astype(F32)
    grad_top = cotangent.astype(F32)
    grad_mlp = (grad_top * mlp_scale).astype(BF)
    grad_rows = lax.all_gather(grad_mlp, "mp", axis=0, tiled=True)
    rows_one, queries, keys, values = gather_qkv(patches, attn_gain, attn_shift, qkv_weight, qv_bias)
    context, lse = attend(queries, keys, values, rel_table, ids)
    attn_out, middle, normed_two = project(context, proj_weight, proj_bias, patches, attn_scale, mlp_gain, mlp_shift)
    grad_middle, grad_attn, mlp_share, up_local, down_local, sums_two = mlp(
        normed_two, grad_rows, up_weight, up_bias, down_weight, middle, attn_out, cotangent, mlp_gain, attn_scale
    )
    mlp_out = scatter_mp(mlp_share) + down_bias.astype(F32)
    layer_out = (middle + mlp_scale * mlp_out).astype(BF)
    scale_two_grad = jnp.sum(grad_top * mlp_out, axis=0)
    down_bias_grad = jnp.sum(grad_mlp.astype(F32), axis=0)
    up_grad = scatter_dp(up_local)
    down_grad = scatter_dp(down_local).T
    grad_context, proj_local = gather_back(grad_attn, proj_weight, context)
    grad_q, grad_k, grad_v, band = attend_back(queries, keys, values, grad_context, lse, rel_table, ids)
    patch_grad, qkv_local, sums_one, qv_bias_local = tail(
        grad_q, grad_k, grad_v, qkv_weight, rows_one, patches, grad_middle, attn_gain
    )
    table_grad = reduce_table(band, length, n_dp)
    mixed = scatter_dp(jnp.concatenate([qkv_local, proj_local], axis=1))
    qkv_grad = mixed[:, : 3 * cols].reshape(-1, 3, cols).swapaxes(0, 1)
    proj_grad = mixed[:, 3 * cols :].T
    small = lax.psum(
        jnp.stack(
            [
                sums_one[0], sums_one[1], sums_two[4], sums_two[3], sums_two[1], sums_two[2], down_bias_grad,
                scale_two_grad,
            ]
        ),
        ("dp", "mp"),
    )
    qv_bias_grad, up_bias_grad = lax.psum((qv_bias_local, sums_two[0]), "dp")
    return (
        layer_out, patch_grad, small[0], small[1], qkv_grad, qv_bias_grad, table_grad, proj_grad, small[2], small[3],
        small[4], small[5], up_grad, up_bias_grad, down_grad, small[6], small[7],
    )


def solution(mesh):
    rows, split = P(("dp", "mp"), None), P("mp", None)
    placed = (
        rows, P("dp", None), P("dp"), P(), P(), P(None, None, "mp"), P(None, "mp"), P("mp", None, None), split,
        P(), P(), P(), P(), P(None, "mp"), P("mp"), split, P(), P(), rows,
    )
    given = (
        rows, rows, P(), P(), P(None, "dp", "mp"), P(None, "mp"), P("mp", "dp", None), P("mp", "dp"), P(), P(),
        P(), P(), P("dp", "mp"), P("mp"), P("mp", "dp"), P(), P(),
    )
    return jax.shard_map(local, mesh=mesh, in_specs=placed, out_specs=given, check_vma=False)
```

```python
from functools import partial

import jax
import jax.numpy as jnp
from jax import lax
from jax.experimental import pallas as pl
from jax.experimental.pallas import tpu as pltpu
from jax.sharding import PartitionSpec as P

HEAD_DIM = 64
BLOCK = 256
GROUP = 128
CHUNKS = 4
SLOTS = 8
PARTS = 2
PAGE_MOST = 256
BF = jnp.bfloat16
F32 = jnp.float32
MESH = pl.DeviceIdType.MESH
VMEM_MOST = 61 * 1024 * 1024
NT = (((1,), (1,)), ((), ()))
TN = (((0,), (0,)), ((), ()))


def vmem():
    return pl.BlockSpec(memory_space=pltpu.VMEM)


def dot(a, b):
    return jnp.dot(a, b, preferred_element_type=F32)


def dot_nt(a, b):
    return lax.dot_general(a, b, NT, preferred_element_type=F32)


def dot_tn(a, b):
    return lax.dot_general(a, b, TN, preferred_element_type=F32)


def norm_rows(rows, gain, shift):
    centre = rows - jnp.mean(rows, axis=-1, keepdims=True)
    inv_std = lax.rsqrt(jnp.mean(centre * centre, axis=-1, keepdims=True) + 1e-06)
    normed = centre * inv_std
    return (normed * gain + shift, normed, inv_std)


def norm_back(grad_out, normed, inv_std, gain):
    scaled = grad_out * gain
    inner = (
        scaled
        - jnp.mean(scaled, axis=-1, keepdims=True)
        - normed * jnp.mean(scaled * normed, axis=-1, keepdims=True)
    )
    return (inv_std * inner, jnp.sum(grad_out * normed, axis=0), jnp.sum(grad_out, axis=0))


def window(index, length):
    width = min(length, BLOCK + 2 * PAGE_MOST)
    start = jnp.clip(index * BLOCK - PAGE_MOST, 0, length - width)
    return pl.multiple_of(start, 128), width


def band_window(group, length):
    wide = min(length, GROUP + 2 * PAGE_MOST)
    start = jnp.clip(group * GROUP - PAGE_MOST, 0, length - wide)
    return pl.multiple_of(start, 128), wide


def head_lanes(head, cols):
    return lax.broadcasted_iota(jnp.int32, (1, cols), 1) // HEAD_DIM == head


def id_columns(ids_ref, cols_ref, seqs, length):
    for s in range(seqs):
        wide = jnp.broadcast_to(ids_ref[s : s + 1, :], (128, length))
        cols_ref[s * length : (s + 1) * length, :] = wide.T


def loop(count, body):
    lax.fori_loop(0, count, lambda i, _: (body(i), 0)[1], 0)


def neighbours():
    me = lax.axis_index("mp")
    partner = me + 1 - 2 * lax.rem(me, 2)
    return me, partner, lax.rem(me + 2, 4), lax.rem(partner + 2, 4)


def greet(peers):
    barrier = pltpu.get_barrier_semaphore()
    for peer in peers:
        pl.semaphore_signal(barrier, inc=1, device_id=peer, device_id_type=MESH)
    pl.semaphore_wait(barrier, len(peers))


def greet_mp():
    _, partner, cross, _ = neighbours()
    greet(({"mp": partner}, {"mp": cross}))


class Gather:
    def __init__(self, buffer, send, recv):
        self.buffer, self.send, self.recv = buffer, send, recv
        self.size = buffer.shape[0] // 4 // CHUNKS
        self.me, self.partner, self.cross, self.diag = neighbours()

    def rows(self, block, chunk):
        return pl.ds(pl.multiple_of((block * CHUNKS + chunk) * self.size, self.size), self.size)

    def copy(self, kind, block, chunk):
        part = self.buffer.at[self.rows(block, chunk), :]
        return pltpu.make_async_remote_copy(
            src_ref=part, dst_ref=part, send_sem=self.send.at[kind, chunk], recv_sem=self.recv.at[kind, chunk],
            device_id={"mp": self.cross if kind == 0 else self.partner}, device_id_type=MESH,
        )

    def send_own(self, chunk):
        self.copy(0, self.me, chunk).start()
        self.copy(1, self.me, chunk).start()

    def wait_partner(self, chunk):
        self.copy(1, self.partner, chunk).wait_recv()

    def relay(self, chunk):
        self.copy(0, self.cross, chunk).wait_recv()
        self.copy(2, self.cross, chunk).start()

    def wait_diag(self, chunk):
        self.copy(2, self.diag, chunk).wait_recv()

    def drain(self, chunk):
        self.copy(0, self.me, chunk).wait_send()
        self.copy(1, self.me, chunk).wait_send()
        self.copy(2, self.cross, chunk).wait_send()


class Scatter:
    def __init__(self, out, inn, send, recv):
        self.out, self.inn, self.send, self.recv = out, inn, send, recv
        self.size = out.shape[1] // CHUNKS
        self.me, self.partner, self.cross, self.diag = neighbours()

    def rows(self, chunk):
        return pl.ds(pl.multiple_of(chunk * self.size, self.size), self.size)

    def copy(self, kind, chunk):
        return pltpu.make_async_remote_copy(
            src_ref=self.out.at[kind, self.rows(chunk), :], dst_ref=self.inn.at[kind, self.rows(chunk), :],
            send_sem=self.send.at[kind, chunk], recv_sem=self.recv.at[kind, chunk],
            device_id={"mp": self.cross if kind == 1 else self.partner}, device_id_type=MESH,
        )

    def put(self, kind, chunk, value):
        self.out[kind, self.rows(chunk), :] = value.astype(BF)
        self.copy(kind, chunk).start()

    def take(self, kind, chunk):
        self.copy(kind, chunk).wait_recv()
        return self.inn[kind, self.rows(chunk), :].astype(F32)

    def drain(self, chunk, kinds=(0, 1, 2)):
        for kind in kinds:
            self.copy(kind, chunk).wait_send()


def slot_of(place):
    return 4 * lax.rem(place, 2) + 2 * lax.rem(place // 2, 2) + place // 4


def half_of(ref, i):
    size = ref.shape[1] // 2
    return pl.ds(pl.multiple_of(i * size, size), size)


def pack(ref, half, value, at=0):
    size = ref.shape[1]
    for j in range(SLOTS // 2):
        ref[4 * (j % 2) + 2 * (j // 2) + half, :, at : at + value.shape[1]] = value[j * size : (j + 1) * size].astype(BF)


def moves():
    return [pltpu.SemaphoreType.DMA((3, CHUNKS)), pltpu.SemaphoreType.DMA((3, CHUNKS))]


def halves(rows, cols):
    return [pltpu.VMEM((3, rows, cols), BF), pltpu.VMEM((3, rows, cols), BF)] + moves()


def call(kernel, name, number, outs, scratch, *args, far=0):
    return pl.pallas_call(
        kernel,
        out_shape=tuple(jax.ShapeDtypeStruct(shape, dtype) for shape, dtype in outs),
        in_specs=[vmem()] * (len(args) - far) + [pl.BlockSpec(memory_space=pl.ANY)] * far,
        out_specs=tuple(vmem() for _ in outs),
        scratch_shapes=scratch,
        compiler_params=pltpu.CompilerParams(
            vmem_limit_bytes=VMEM_MOST, collective_id=number, has_side_effects=True
        ),
        name=name,
    )(*args)


def attend_block(q_ref, k_ref, v_ref, table_ref, ids_ref, cols_ref, ctx_ref, lse_ref, seq, index):
    cols = q_ref.shape[1]
    length = ids_ref.shape[1]
    base = seq * length
    start, width = window(index, length)
    here = pl.ds(pl.multiple_of(index * BLOCK, BLOCK), BLOCK)
    rows = pl.ds(pl.multiple_of(base + index * BLOCK, BLOCK), BLOCK)
    keys_at = pl.ds(pl.multiple_of(base + start, 128), width)
    query = q_ref[rows, :]
    keys = k_ref[keys_at, :]
    values = v_ref[keys_at, :]
    same = cols_ref[rows, 0:1] == ids_ref[pl.ds(seq, 1), pl.ds(start, width)]
    context = jnp.zeros((BLOCK, cols), F32)
    sums = jnp.zeros((BLOCK, 128), F32)
    lane = lax.broadcasted_iota(jnp.int32, (1, 128), 1)
    for head in range(cols // HEAD_DIM):
        mine = head_lanes(head, cols)
        scores = dot_nt(jnp.where(mine, query, 0), keys)
        scores = jnp.where(same, scores + table_ref[head, here, pl.ds(start, width)].astype(F32), -1e30)
        peak = jnp.max(scores, axis=-1, keepdims=True)
        expo = jnp.exp(scores - peak)
        total = jnp.sum(expo, axis=-1, keepdims=True)
        part = dot(expo.astype(BF), values) * (1.0 / total)
        context = jnp.where(mine, part, context)
        sums = jnp.where(lane == head, peak + jnp.log(total), sums)
    ctx_ref[rows, :] = context.astype(BF)
    lse_ref[rows, :] = sums


def front_kernel(
    x_ref, gain_ref, shift_ref, w_ref, bias_ref, cot_ref, scale_ref, ids_ref, table_hbm,
    rows_ref, grad_ref, q_ref, k_ref, v_ref, ctx_ref, lse_ref,
    table_ref, cols_ref, load, send, recv, gsend, grecv,
):
    net = Gather(rows_ref, send, recv)
    top = Gather(grad_ref, gsend, grecv)
    seqs, length = ids_ref.shape
    fetch = pltpu.make_async_copy(table_hbm, table_ref, load)
    fetch.start()
    greet_mp()

    def own(chunk):
        part = x_ref[pl.ds(pl.multiple_of(chunk * net.size, net.size), net.size), :].astype(F32)
        rows_ref[net.rows(net.me, chunk), :] = norm_rows(part, gain_ref[...], shift_ref[...])[0].astype(BF)
        net.send_own(chunk)

    loop(CHUNKS, own)

    def top_own(chunk):
        part = cot_ref[pl.ds(pl.multiple_of(chunk * net.size, net.size), net.size), :].astype(F32)
        grad_ref[net.rows(net.me, chunk), :] = (part * scale_ref[...]).astype(BF)

    loop(CHUNKS, top_own)
    id_columns(ids_ref, cols_ref, seqs, length)
    tall = 2 * net.size

    def project(block):
        def part(i):
            at = pl.ds(pl.multiple_of(block * CHUNKS * net.size + i * tall, tall), tall)
            rows = rows_ref[at, :]
            query = dot(rows, w_ref[0]) + bias_ref[0:1, :].astype(F32)
            q_ref[at, :] = (query.astype(BF).astype(F32) * 0.125).astype(BF)
            k_ref[at, :] = dot(rows, w_ref[1]).astype(BF)
            v_ref[at, :] = (dot(rows, w_ref[2]) + bias_ref[1:2, :].astype(F32)).astype(BF)

        loop(CHUNKS // 2, part)

    def attend(seq, index):
        attend_block(q_ref, k_ref, v_ref, table_ref, ids_ref, cols_ref, ctx_ref, lse_ref, seq, index)

    project(net.me)
    loop(CHUNKS, net.wait_partner)
    project(net.partner)
    fetch.wait()
    mine = net.me // 2
    steps = length // BLOCK

    def near(i):
        attend(mine, i)
        net.relay(i)
        top.send_own(i)

    loop(steps, near)
    project(net.cross)
    loop(CHUNKS, net.wait_diag)
    project(net.diag)

    def far(i):
        attend(1 - mine, i)
        top.relay(i)
        net.drain(i)

    loop(steps, far)
    for wait in (top.wait_partner, top.wait_diag, top.drain):
        loop(CHUNKS, wait)


def front(patches, gain, shift, weight, bias, cotangent, scale, ids, table):
    rows, width = patches.shape
    cols = weight.shape[2]
    one, wide = ((4 * rows, cols), BF), ((4 * rows, width), BF)
    return call(
        front_kernel, "front", 1, [wide, wide, one, one, one, one, ((4 * rows, 128), F32)],
        [pltpu.VMEM(table.shape, BF), pltpu.VMEM((4 * rows, 128), F32), pltpu.SemaphoreType.DMA] + moves() + moves(),
        patches, gain[None], shift[None], weight, bias, cotangent, scale[None], ids, table, far=1,
    )


def project_kernel(
    ctx_ref, w_ref, bias_ref, x_ref, scale_ref, gain_ref, shift_ref, attn_ref, mid_ref, norm_ref, out, inn, send, recv
):
    net = Scatter(out, inn, send, recv)
    greet_mp()

    def share(block, chunk):
        at = pl.ds(pl.multiple_of((block * CHUNKS + chunk) * net.size, net.size), net.size)
        return dot(ctx_ref[at, :], w_ref[...])

    loop(CHUNKS, lambda c: net.put(0, c, share(net.diag, c)))
    loop(CHUNKS, lambda c: net.put(1, c, share(net.cross, c) + net.take(0, c)))
    loop(CHUNKS, lambda c: net.put(2, c, share(net.partner, c)))

    def own(chunk):
        attn_ref[net.rows(chunk), :] = share(net.me, chunk) + net.take(2, chunk) + bias_ref[...].astype(F32)

    loop(CHUNKS, own)

    def last(chunk):
        at = net.rows(chunk)
        attn = attn_ref[at, :] + net.take(1, chunk)
        middle = x_ref[at, :].astype(F32) + scale_ref[...] * attn
        attn_ref[at, :] = attn
        mid_ref[at, :] = middle
        norm_ref[at, :] = norm_rows(middle, gain_ref[...], shift_ref[...])[0].astype(BF)

    loop(CHUNKS, last)
    loop(CHUNKS, net.drain)


def project(context, weight, bias, patches, scale, gain, shift):
    rows, width = patches.shape
    return call(
        project_kernel, "project", 2, [((rows, width), F32), ((rows, width), F32), ((rows, width), BF)],
        halves(rows, width), context, weight, bias[None], patches, scale[None], gain[None], shift[None],
    )


def gelu_both(u):
    inner = 0.7978845608028654 * (u + 0.044715 * (u * u * u))
    t = jnp.tanh(inner)
    half = 0.5 * (1.0 + t)
    slope = half + (0.5 * u) * (1.0 - t * t) * (0.7978845608028654 * (1.0 + 0.134145 * (u * u)))
    return u * half, slope


def mlp_kernel(
    norm_ref, grad_ref, up_ref, bias_ref, down_ref, mid_ref, attn_ref, cot_ref, gain_ref, scale_ref,
    gmid_ref, gattn_ref, cross_ref, here_ref, upg_ref, downg_ref, sums_ref,
    rows_ref, hid_ref, pre_ref, own_ref, far_ref, mfar_ref, gsend, grecv, out, inn, send, recv,
    mout, minn, msend, mrecv,
):
    gat = Gather(rows_ref, gsend, grecv)
    net = Scatter(out, inn, send, recv)
    top = Scatter(mout, minn, msend, mrecv)
    size = gat.size
    greet_mp()
    sums_ref[...] = jnp.zeros_like(sums_ref)

    def own(chunk):
        rows_ref[gat.rows(gat.me, chunk), :] = norm_ref[net.rows(chunk), :]
        gat.send_own(chunk)

    loop(CHUNKS, own)

    def two(first, second, chunk):
        at, by = gat.rows(first, chunk), gat.rows(second, chunk)
        both = lambda ref: jnp.concatenate([ref[at, :], ref[by, :]], axis=0)
        value, slope = gelu_both(dot(both(rows_ref), up_ref[...]) + bias_ref[...].astype(F32))
        hidden = value.astype(BF)
        hid_ref[at, :], hid_ref[by, :] = hidden[:size], hidden[size:]
        grad_pre = (dot_nt(both(grad_ref), down_ref[...]) * slope).astype(BF)
        pre_ref[at, :], pre_ref[by, :] = grad_pre[:size], grad_pre[size:]
        sums_ref[0:1, :] += jnp.sum(grad_pre.astype(F32), axis=0, keepdims=True)
        back = dot_nt(grad_pre, up_ref[...])
        part = dot(hidden, down_ref[...])
        return back[:size], back[size:], part[:size], part[size:]

    def near(chunk):
        gat.wait_partner(chunk)
        theirs, mine, share, kept = two(gat.partner, gat.me, chunk)
        net.put(2, chunk, theirs)
        top.put(2, chunk, share)
        own_ref[net.rows(chunk), :] = mine
        here_ref[net.rows(chunk), :] = kept

    loop(CHUNKS, near)

    def across(chunk):
        net.put(1, chunk, far_ref[net.rows(chunk), :] + net.take(0, chunk))

    def far(chunk):
        gat.relay(chunk)
        gat.wait_diag(chunk)
        theirs, mine, share, kept = two(gat.diag, gat.cross, chunk)
        net.put(0, chunk, theirs)
        top.put(0, chunk, share)
        far_ref[net.rows(chunk), :] = mine
        mfar_ref[net.rows(chunk), :] = kept

        @pl.when(chunk > 0)
        def _():
            across(chunk - 1)

    loop(CHUNKS, far)
    across(CHUNKS - 1)

    def weights(i):
        pack(upg_ref, i, dot_tn(rows_ref[:, half_of(rows_ref, i)], pre_ref[...]))
        pack(downg_ref, i, dot_tn(grad_ref[:, half_of(grad_ref, i)], hid_ref[...]))

    loop(2, weights)

    def outs(chunk):
        at = net.rows(chunk)
        here_ref[at, :] += top.take(2, chunk)
        cross_ref[at, :] = (mfar_ref[at, :] + top.take(0, chunk)).astype(BF)

    loop(CHUNKS, outs)

    def last(chunk):
        at = net.rows(chunk)
        grad = own_ref[at, :] + net.take(2, chunk) + net.take(1, chunk)
        normed, inv = norm_rows(mid_ref[at, :], 1.0, 0.0)[1:]
        back, gain_sum, shift_sum = norm_back(grad, normed, inv, gain_ref[...])
        middle = cot_ref[at, :].astype(F32) + back
        gattn = (middle * scale_ref[...]).astype(BF)
        gmid_ref[at, :] = middle
        gattn_ref[at, :] = gattn
        sums_ref[1:2, :] += gain_sum[None]
        sums_ref[2:3, :] += shift_sum[None]
        sums_ref[3:4, :] += jnp.sum(middle * attn_ref[at, :], axis=0, keepdims=True)
        sums_ref[4:5, :] += jnp.sum(gattn.astype(F32), axis=0, keepdims=True)

    loop(CHUNKS, last)
    loop(CHUNKS, gat.drain)
    loop(CHUNKS, net.drain)
    loop(CHUNKS, lambda chunk: top.drain(chunk, (0, 2)))


def mlp(normed, grad_rows, up, bias, down, middle, attn, cotangent, gain, scale):
    rows, width = normed.shape
    ff = up.shape[1]
    one = pltpu.VMEM((rows, width), F32)
    packed = ((SLOTS, width // SLOTS, ff), BF)
    return call(
        mlp_kernel, "mlp", 3,
        [((rows, width), F32), ((rows, width), BF), ((rows, width), BF), ((rows, width), F32), packed, packed, ((8, width), F32)],
        [pltpu.VMEM((4 * rows, width), BF), pltpu.VMEM((4 * rows, ff), BF), pltpu.VMEM((4 * rows, ff), BF), one, one, one]
        + moves() + halves(rows, width) + halves(rows, width),
        normed, grad_rows, up, bias[None], down, middle, attn, cotangent, gain[None], scale[None],
    )


class Fold:
    def __init__(self, src, inn, send, recv):
        self.src, self.inn, self.send, self.recv = src, inn, send, recv
        self.size = src.shape[1] // PARTS
        place = lax.axis_index("dp")
        x, lo, hi = lax.rem(place, 2), lax.rem(place // 2, 2), place // 4
        self.peers = (place + 1 - 2 * x, place + 2 - 4 * lo, place + 4 - 8 * hi)
        self.theirs = (4 * (1 - x), 2 * (1 - lo), 4 + 1 - hi)
        self.mine = (4 * x, 2 * lo, 4 + hi)

    def copy(self, stage, part):
        count, offset = (4, 2, 1)[stage], (0, 4, 6)[stage]
        rows = pl.ds(part * self.size, self.size)
        src = self.src if stage == 0 else self.inn
        return pltpu.make_async_remote_copy(
            src_ref=src.at[pl.ds(self.theirs[stage], count), rows, :],
            dst_ref=self.inn.at[pl.ds(offset, count), rows, :],
            send_sem=self.send.at[stage, part], recv_sem=self.recv.at[stage, part],
            device_id={"dp": self.peers[stage]}, device_id_type=MESH,
        )

    def start(self):
        for part in range(PARTS):
            self.copy(0, part).start()

    def advance(self, stage):
        count, offset = (4, 2)[stage], (0, 4)[stage]
        src = self.src if stage == 0 else self.inn
        for part in range(PARTS):
            rows = pl.ds(part * self.size, self.size)
            self.copy(stage, part).wait_recv()
            for i in range(count):
                self.inn[offset + i, rows, :] = self.inn[offset + i, rows, :] + src[self.mine[stage] + i, rows, :]
            self.copy(stage + 1, part).start()

    def finish(self, put):
        for part in range(PARTS):
            rows = pl.ds(part * self.size, self.size)
            self.copy(2, part).wait_recv()
            put(rows, self.inn[self.mine[2], rows, :].astype(F32) + self.inn[6, rows, :].astype(F32))

    def drain(self):
        for stage in range(3):
            for part in range(PARTS):
                self.copy(stage, part).wait_send()


class Total:
    def __init__(self, acc, inn, send, recv):
        self.acc, self.inn, self.send, self.recv = acc, inn, send, recv
        place = lax.axis_index("dp")
        x, lo, hi = lax.rem(place, 2), lax.rem(place // 2, 2), place // 4
        _, partner, cross, _ = neighbours()
        self.peers = (
            {"dp": place + 1 - 2 * x}, {"dp": place + 2 - 4 * lo}, {"dp": place + 4 - 8 * hi}, {"mp": partner}, {"mp": cross},
        )

    def copy(self, stage):
        return pltpu.make_async_remote_copy(
            src_ref=self.acc.at[stage], dst_ref=self.inn.at[stage], send_sem=self.send.at[stage],
            recv_sem=self.recv.at[stage], device_id=self.peers[stage], device_id_type=MESH,
        )

    def start(self, stage):
        self.copy(stage).start()

    def finish(self, stage):
        self.copy(stage).wait_recv()
        self.acc[stage + 1] = self.acc[stage] + self.inn[stage]

    def drain(self):
        for stage in range(5):
            self.copy(stage).wait_send()


def back_kernel(
    fold,
    pw_ref, ctx_ref, q_ref, k_ref, v_ref, lse_ref, ids_ref, w_ref, x_ref, gmid_ref, gain_ref,
    cot_ref, mid_ref, cross_ref, here_ref, dbias_ref, mscale_ref, upg_ref, downg_ref, two_ref, gattn_hbm, rows_hbm, table_hbm,
    *refs,
):
    if fold:
        layer_ref, grad_ref, tab_ref, upo_ref, downo_ref, mixo_ref, sums_ref, *refs = refs
        band_ref, mix_ref, acc_ref, *refs = refs
        winn, wsend, wrecv, tinn, tsend, trecv, ainn, asend, arecv, *refs = refs
    else:
        layer_ref, grad_ref, band_ref, mix_ref, sums_ref, *refs = refs
        acc_ref = None
    (
        table_ref, cols_ref, rowsg_ref, g_ref, qt_ref, gt_ref, dkt_ref, dvt_ref, total_ref, dq_ref, dv_ref,
        far_ref, load, fsend, frecv, gsend, grecv, out, inn, send, recv,
    ) = refs
    dk_ref = g_ref
    own_ref = grad_ref
    gat = Gather(rowsg_ref, gsend, grecv)
    net = Scatter(out, inn, send, recv)
    seqs, length = ids_ref.shape
    rows_all, cols = q_ref.shape
    blocks = length // BLOCK
    heads = cols // HEAD_DIM
    small_ref = acc_ref.at[0] if fold else sums_ref
    me, partner, cross, _ = neighbours()
    whole = CHUNKS * gat.size
    mine_at = pl.ds(pl.multiple_of(me * whole, whole), whole)
    first = pltpu.make_async_copy(gattn_hbm, rowsg_ref.at[mine_at, :], load.at[0])
    first.start()

    def fetch(head):
        at = pl.ds(pl.multiple_of(lax.rem(head, 2) * length, length), length)
        return pltpu.make_async_copy(table_hbm.at[head], table_ref.at[at, :], load.at[1 + head])

    fetch(0).start()
    fetch(1).start()
    far = pltpu.make_async_remote_copy(
        src_ref=cross_ref, dst_ref=far_ref, send_sem=fsend, recv_sem=frecv, device_id={"mp": cross}, device_id_type=MESH
    )
    if fold:
        up = Fold(upg_ref, winn.at[0], wsend.at[0], wrecv.at[0])
        down = Fold(downg_ref, winn.at[1], wsend.at[1], wrecv.at[1])
        mix = Fold(mix_ref, winn.at[2], wsend.at[2], wrecv.at[2])
        tab = lambda head: Fold(band_ref.at[head], tinn.at[head], tsend.at[head], trecv.at[head])
        small = Total(acc_ref, ainn, asend, arecv)
        greet(({"mp": partner}, {"mp": cross}) + tuple({"dp": peer} for peer in up.peers))
    else:
        greet_mp()

    first.wait()
    loop(CHUNKS, gat.send_own)
    if fold:
        up.start()
        down.start()
    id_columns(ids_ref, cols_ref, seqs, length)

    def block(number):
        at = pl.ds(pl.multiple_of(number * whole, whole), whole)
        g_ref[at, :] = dot_nt(rowsg_ref[at, :], pw_ref[...]).astype(BF)

    def tall(i):
        return pl.ds(pl.multiple_of(i * BLOCK, BLOCK), BLOCK)

    def flip_q(i):
        qt_ref[:, tall(i)] = q_ref[tall(i), :].T

    def flip_g(i):
        gt_ref[:, tall(i)] = g_ref[tall(i), :].T

    block(gat.me)
    loop(CHUNKS, gat.wait_partner)
    block(gat.partner)
    loop(rows_all // BLOCK, flip_q)
    dkt_ref[...] = jnp.zeros_like(dkt_ref)
    dvt_ref[...] = jnp.zeros_like(dvt_ref)
    dq_ref[...] = jnp.zeros_like(dq_ref)
    small_ref[...] = jnp.zeros_like(small_ref)
    if fold:
        tab_ref[...] = jnp.zeros_like(tab_ref)
    loop(CHUNKS, gat.relay)
    block(gat.cross)
    loop(CHUNKS, gat.wait_diag)
    block(gat.diag)
    far.start()
    loop(rows_all // BLOCK, flip_g)
    if fold:
        up.advance(0)
    lane = lax.broadcasted_iota(jnp.int32, (1, 128), 1)

    def step(head, index):
        start, width = window(index, length)
        mine = head_lanes(head, cols)
        feats = pl.ds(pl.multiple_of(head * HEAD_DIM, HEAD_DIM), HEAD_DIM)
        bias = table_ref[tall(lax.rem(head, 2) * blocks + index), pl.ds(start, width)].astype(F32)
        for seq in range(seqs):
            base = seq * length
            rows = pl.ds(pl.multiple_of(base + index * BLOCK, BLOCK), BLOCK)
            keys_at = pl.ds(pl.multiple_of(base + start, 128), width)
            keys = k_ref[keys_at, :]
            same = cols_ref[rows, 0:1] == ids_ref[seq : seq + 1, pl.ds(start, width)]
            sums = jnp.sum(jnp.where(lane == head, lse_ref[rows, :], 0.0), axis=-1, keepdims=True)
            scores = dot_nt(jnp.where(mine, q_ref[rows, :], 0), keys) + bias
            probs = jnp.where(same, jnp.exp(scores - sums), 0.0)
            grad_probs = dot_nt(jnp.where(mine, g_ref[rows, :], 0), v_ref[keys_at, :])
            centre = jnp.sum(grad_probs * probs, axis=-1, keepdims=True)
            grad_scores = (probs * (grad_probs - centre)).astype(BF)
            dvt_ref[feats, keys_at] += dot(gt_ref[feats, rows], probs.astype(BF))
            dkt_ref[feats, keys_at] += dot(qt_ref[feats, rows], grad_scores)
            grad_q = (dot(grad_scores, keys) * 0.125).astype(BF)
            dq_ref[rows, :] = jnp.where(mine, grad_q, dq_ref[rows, :])
            if seq == 0:
                total_ref[:, 0:width] = grad_scores.astype(F32)
            else:
                total_ref[:, 0:width] += grad_scores.astype(F32)
        for part in range(BLOCK // GROUP):
            group = index * (BLOCK // GROUP) + part
            first, wide = band_window(group, length)
            offset = pl.multiple_of(first - start, 128)
            value = total_ref[part * GROUP : (part + 1) * GROUP, pl.ds(offset, wide)]
            band_ref[head, slot_of(group), :, :] = value.astype(BF)

    def one_head(head):
        fetch(head).wait()
        loop(blocks, lambda index: step(head, index))

        @pl.when(head + 2 < heads)
        def _():
            fetch(head + 2).start()

        if fold:
            tab(head).start()

            @pl.when(head == 0)
            def _():
                down.advance(0)
                up.advance(1)

            @pl.when(head == 1)
            def _():
                down.advance(1)

            @pl.when(head == 2)
            def _():
                tab(0).advance(0)

    loop(heads, one_head)
    rows_ref = table_ref.at[:, 0 : rowsg_ref.shape[1]]
    again = pltpu.make_async_copy(rows_hbm, rows_ref, load.at[0])
    again.start()

    def unflip(i):
        dk_ref[tall(i), :] = dkt_ref[:, tall(i)].T.astype(BF)
        dv_ref[tall(i), :] = dvt_ref[:, tall(i)].T.astype(BF)

    loop(rows_all // BLOCK, unflip)

    again.wait()

    def weights(i):
        rows = table_ref[:, half_of(rowsg_ref, i)]
        for number, ref in enumerate((dq_ref, dk_ref, dv_ref)):
            pack(mix_ref, i, dot_tn(rows, ref[...]), number * cols)
        pack(mix_ref, i, dot_tn(rowsg_ref[:, half_of(rowsg_ref, i)], ctx_ref[...]), 3 * cols)

    loop(2, weights)

    def put_table(head):
        def put(rows, value):
            first = band_window(lax.axis_index("dp"), length)[0]
            tab_ref[head, rows, pl.ds(first, value.shape[1])] = value
        return put

    def put_to(ref):
        def put(rows, value):
            ref[rows, :] = value
        return put

    if fold:
        mix.start()

    def share(number, chunk):
        at = gat.rows(number, chunk)
        return dot_nt(dq_ref[at, :], w_ref[0]) + dot_nt(dk_ref[at, :], w_ref[1]) + dot_nt(dv_ref[at, :], w_ref[2])

    loop(CHUNKS, lambda c: net.put(0, c, share(net.diag, c)))
    loop(CHUNKS, lambda c: net.put(1, c, share(net.cross, c) + net.take(0, c)))
    if fold:
        up.finish(put_to(upo_ref))
        down.finish(put_to(downo_ref))
        tab(0).advance(1)
        tab(1).advance(0)
    loop(CHUNKS, lambda c: net.put(2, c, share(net.partner, c)))

    def keep(chunk):
        own_ref[net.rows(chunk), :] = share(net.me, chunk) + net.take(2, chunk)

    loop(CHUNKS, keep)
    far.wait_recv()

    def layer(chunk):
        at = net.rows(chunk)
        mlp_out = here_ref[at, :] + far_ref[at, :].astype(F32) + dbias_ref[...].astype(F32)
        layer_ref[at, :] = (mid_ref[at, :] + mscale_ref[...] * mlp_out).astype(BF)
        top = cot_ref[at, :].astype(F32)
        small_ref[7:8, :] += jnp.sum(top * mlp_out, axis=0, keepdims=True)
        low = (top * mscale_ref[...]).astype(BF).astype(F32)
        small_ref[6:7, :] += jnp.sum(low, axis=0, keepdims=True)

    loop(CHUNKS, layer)
    for row, source in ((2, 4), (3, 3), (4, 1), (5, 2), (8, 0)):
        small_ref[row : row + 1, :] = two_ref[source : source + 1, :]
    small_ref[9:10, 0:cols] = jnp.sum(dq_ref[...].astype(F32), axis=0, keepdims=True)
    small_ref[10:11, 0:cols] = jnp.sum(dv_ref[...].astype(F32), axis=0, keepdims=True)
    if fold:
        tab(2).advance(0)
        tab(1).advance(1)
        tab(0).finish(put_table(0))

    def last(chunk):
        at = net.rows(chunk)
        grad = own_ref[at, :] + net.take(1, chunk)
        normed, inv = norm_rows(x_ref[at, :].astype(F32), 1.0, 0.0)[1:]
        back, gain_sum, shift_sum = norm_back(grad, normed, inv, gain_ref[...])
        grad_ref[at, :] = gmid_ref[at, :] + back
        small_ref[0:1, :] += gain_sum[None]
        small_ref[1:2, :] += shift_sum[None]

    loop(CHUNKS, last)
    if fold:
        small.start(0)
        mix.advance(0)
        small.finish(0)
        small.start(1)
        tab(2).advance(1)
        tab(1).finish(put_table(1))
        small.finish(1)
        small.start(2)
        mix.advance(1)
        small.finish(2)
        small.start(3)
        tab(2).finish(put_table(2))
        small.finish(3)
        small.start(4)
        mix.finish(put_to(mixo_ref))
        small.finish(4)
        sums_ref[0:8, :] = acc_ref[5, 0:8, :]
        sums_ref[8:16, :] = acc_ref[3, 8:16, :]
        for piece in (up, down, mix, tab(0), tab(1), tab(2), small):
            piece.drain()
    far.wait_send()
    loop(CHUNKS, gat.drain)
    loop(CHUNKS, net.drain)


def back(fold, length, gattn, rows_one, table, proj, ctx, q, k, v, lse, ids, qkv, patches, gmid, gain, *rest):
    rows, width = patches.shape
    cols = q.shape[1]
    heads = cols // HEAD_DIM
    piece, wide = width // SLOTS, band_window(0, length)[1]
    strip = min(length, BLOCK + 2 * PAGE_MOST)
    band, mix = ((heads, SLOTS, GROUP, wide), BF), ((SLOTS, piece, width), BF)
    outs = [((rows, width), BF), ((rows, width), F32)]
    scratch = []
    if fold:
        sem = pltpu.SemaphoreType.DMA((3, 3, PARTS))
        outs += [((heads, GROUP, length), F32)] + [((piece, width), F32)] * 3
        scratch += [pltpu.VMEM(*band), pltpu.VMEM(*mix), pltpu.VMEM((6, 16, width), F32)]
        scratch += [pltpu.VMEM((3, 7, piece, width), BF), sem, sem, pltpu.VMEM((heads, 7, GROUP, wide), BF), sem, sem]
        scratch += [pltpu.VMEM((5, 16, width), F32), pltpu.SemaphoreType.DMA((5,)), pltpu.SemaphoreType.DMA((5,))]
    else:
        outs += [band, mix]
    outs += [((16, width), F32)]
    one, flat = pltpu.VMEM((4 * rows, cols), BF), pltpu.VMEM((cols, 4 * rows), BF)
    total = pltpu.VMEM((cols, 4 * rows), F32)
    scratch += [
        pltpu.VMEM((2 * length, length), BF), pltpu.VMEM((4 * rows, 128), F32), pltpu.VMEM((4 * rows, width), BF), one,
        flat, flat, total, total, pltpu.VMEM((BLOCK, strip), F32), one, one,
        pltpu.VMEM((rows, width), BF),
        pltpu.SemaphoreType.DMA((1 + heads,)), pltpu.SemaphoreType.DMA, pltpu.SemaphoreType.DMA,
    ] + moves() + halves(rows, width)
    return call(
        partial(back_kernel, fold), "back", 4, outs, scratch,
        proj, ctx, q, k, v, lse, ids, qkv, patches, gmid, gain, *rest, gattn, rows_one, table, far=3,
    )


def scatter_dp(x):
    return lax.psum_scatter(x, "dp", scatter_dimension=0, tiled=True).astype(F32)


def in_order(packed):
    _, rows, cols = packed.shape
    return packed.reshape(2, 2, 2, rows, cols).transpose(2, 1, 0, 3, 4).reshape(SLOTS * rows, cols)


def reduce_table(band, length, n_dp):
    groups, heads, _, wide = band.shape
    shard = length // n_dp
    send = band.reshape(groups, heads, GROUP // shard, shard, wide).swapaxes(1, 2)
    part = scatter_dp(send.reshape(n_dp * heads * shard, wide)).reshape(heads, shard, wide)
    first = band_window(lax.axis_index("dp") * shard // GROUP, length)[0]
    return lax.dynamic_update_slice(jnp.zeros((heads, shard, length), F32), part, (0, 0, first))


def local(
    patches, segment_ids, fill_counts, attn_gain, attn_shift, qkv_weight, qv_bias, rel_table, proj_weight,
    proj_bias, attn_scale, mlp_gain, mlp_shift, up_weight, up_bias, down_weight, down_bias, mlp_scale, cotangent,
):
    n_dp = lax.axis_size("dp")
    seqs, length = segment_ids.shape
    cols = qkv_weight.shape[2]
    places = jnp.arange(length, dtype=jnp.int32)[None]
    ids = jnp.where(places < fill_counts[:, None], segment_ids, -1 - places).astype(F32)
    fold = n_dp == SLOTS and length == SLOTS * GROUP
    rows_one, grad_rows, queries, keys, values, context, lse = front(
        patches, attn_gain, attn_shift, qkv_weight, qv_bias, cotangent, mlp_scale, ids, rel_table
    )
    attn_out, middle, normed_two = project(context, proj_weight, proj_bias, patches, attn_scale, mlp_gain, mlp_shift)
    grad_middle, grad_attn, cross, here, up_local, down_local, sums_two = mlp(
        normed_two, grad_rows, up_weight, up_bias, down_weight, middle, attn_out, cotangent, mlp_gain, attn_scale
    )
    layer_out, patch_grad, *more, sums = back(
        fold, length, grad_attn, rows_one, rel_table, proj_weight, context, queries, keys, values, lse, ids, qkv_weight,
        patches, grad_middle, attn_gain[None], cotangent, middle, cross, here, down_bias[None], mlp_scale[None],
        up_local, down_local, sums_two,
    )
    if fold:
        table_grad, up_grad, down_grad, mixed = more
    else:
        band, mixed = more
        order = [4 * (d % 2) + 2 * (d // 2 % 2) + d // 4 for d in range(SLOTS)]
        table_grad = reduce_table(jnp.stack([band[:, slot] for slot in order]), length, n_dp)
        up_grad, down_grad, mixed = [scatter_dp(in_order(piece)) for piece in (up_local, down_local, mixed)]
        sums = jnp.concatenate([lax.psum(sums[:8], ("dp", "mp")), lax.psum(sums[8:], "dp")])
    qkv_grad = mixed[:, : 3 * cols].reshape(-1, 3, cols).swapaxes(0, 1)
    return (
        layer_out, patch_grad, sums[0], sums[1], qkv_grad, sums[9:11, :cols], table_grad, mixed[:, 3 * cols :].T,
        sums[2], sums[3], sums[4], sums[5], up_grad, sums[8], down_grad.T, sums[6], sums[7],
    )


def solution(mesh):
    rows, split = P(("dp", "mp"), None), P("mp", None)
    placed = (
        rows, P("dp", None), P("dp"), P(), P(), P(None, None, "mp"), P(None, "mp"), P("mp", None, None), split,
        P(), P(), P(), P(), P(None, "mp"), P("mp"), split, P(), P(), rows,
    )
    given = (
        rows, rows, P(), P(), P(None, "dp", "mp"), P(None, "mp"), P("mp", "dp", None), P("mp", "dp"), P(), P(),
        P(), P(), P("dp", "mp"), P("mp"), P("mp", "dp"), P(), P(),
    )
    return jax.shard_map(local, mesh=mesh, in_specs=placed, out_specs=given, check_vma=False)
```

```python
from functools import partial

import jax
import jax.numpy as jnp
from jax import lax
from jax.experimental import pallas as pl
from jax.experimental.pallas import tpu as pltpu
from jax.sharding import PartitionSpec as P

HEAD_DIM = 64
BLOCK = 256
GROUP = 128
ATTN_GAIN, ATTN_SHIFT, PROJ_BIAS, ATTN_SCALE, MLP_GAIN, MLP_SHIFT, UP_BIAS, DOWN_BIAS, MLP_SCALE = range(9)
CHUNKS = 4
SLOTS = 8
PARTS = 2
EARLY = 15
MIX_ORDER = (1, 2, 0)
PAGE_MOST = 256
BF = jnp.bfloat16
F32 = jnp.float32
MESH = pl.DeviceIdType.MESH
VMEM_MOST = 61 * 1024 * 1024
NT = (((1,), (1,)), ((), ()))
TN = (((0,), (0,)), ((), ()))


def vmem():
    return pl.BlockSpec(memory_space=pltpu.VMEM)


def dot(a, b):
    return jnp.dot(a, b, preferred_element_type=F32)


def dot_nt(a, b):
    return lax.dot_general(a, b, NT, preferred_element_type=F32)


def dot_tn(a, b):
    return lax.dot_general(a, b, TN, preferred_element_type=F32)


def norm_rows(rows, gain, shift):
    centre = rows - jnp.mean(rows, axis=-1, keepdims=True)
    inv_std = lax.rsqrt(jnp.mean(centre * centre, axis=-1, keepdims=True) + 1e-06)
    normed = centre * inv_std
    return (normed * gain + shift, normed, inv_std)


def norm_back(grad_out, normed, inv_std, gain):
    scaled = grad_out * gain
    inner = (
        scaled
        - jnp.mean(scaled, axis=-1, keepdims=True)
        - normed * jnp.mean(scaled * normed, axis=-1, keepdims=True)
    )
    return (inv_std * inner, jnp.sum(grad_out * normed, axis=0), jnp.sum(grad_out, axis=0))


def window(index, length):
    width = min(length, BLOCK + 2 * PAGE_MOST)
    start = jnp.clip(index * BLOCK - PAGE_MOST, 0, length - width)
    return pl.multiple_of(start, 128), width


def band_window(group, length):
    wide = min(length, GROUP + 2 * PAGE_MOST)
    start = jnp.clip(group * GROUP - PAGE_MOST, 0, length - wide)
    return pl.multiple_of(start, 128), wide


def head_lanes(head, cols):
    return lax.broadcasted_iota(jnp.int32, (1, cols), 1) // HEAD_DIM == head


def id_columns(ids_ref, cols_ref, seqs, length):
    for s in range(seqs):
        wide = jnp.broadcast_to(ids_ref[s : s + 1, :], (128, length))
        cols_ref[s * length : (s + 1) * length, :] = wide.T


def loop(count, body):
    lax.fori_loop(0, count, lambda i, _: (body(i), 0)[1], 0)


def neighbours():
    me = lax.axis_index("mp")
    partner = me + 1 - 2 * lax.rem(me, 2)
    return me, partner, lax.rem(me + 2, 4), lax.rem(partner + 2, 4)


def greet(peers):
    barrier = pltpu.get_barrier_semaphore()
    for peer in peers:
        pl.semaphore_signal(barrier, inc=1, device_id=peer, device_id_type=MESH)
    pl.semaphore_wait(barrier, len(peers))


def greet_mp():
    _, partner, cross, _ = neighbours()
    greet(({"mp": partner}, {"mp": cross}))


class Gather:
    def __init__(self, buffer, send, recv):
        self.buffer, self.send, self.recv = buffer, send, recv
        self.size = buffer.shape[0] // 4 // CHUNKS
        self.me, self.partner, self.cross, self.diag = neighbours()

    def rows(self, block, chunk):
        return pl.ds(pl.multiple_of((block * CHUNKS + chunk) * self.size, self.size), self.size)

    def copy(self, kind, block, chunk):
        part = self.buffer.at[self.rows(block, chunk), :]
        return pltpu.make_async_remote_copy(
            src_ref=part, dst_ref=part, send_sem=self.send.at[kind, chunk], recv_sem=self.recv.at[kind, chunk],
            device_id={"mp": self.cross if kind == 0 else self.partner}, device_id_type=MESH,
        )

    def send_own(self, chunk):
        self.copy(0, self.me, chunk).start()
        self.copy(1, self.me, chunk).start()

    def wait_partner(self, chunk):
        self.copy(1, self.partner, chunk).wait_recv()

    def relay(self, chunk):
        self.copy(0, self.cross, chunk).wait_recv()
        self.copy(2, self.cross, chunk).start()

    def wait_diag(self, chunk):
        self.copy(2, self.diag, chunk).wait_recv()

    def drain(self, chunk):
        self.copy(0, self.me, chunk).wait_send()
        self.copy(1, self.me, chunk).wait_send()
        self.copy(2, self.cross, chunk).wait_send()


class Scatter:
    def __init__(self, out, inn, send, recv):
        self.out, self.inn, self.send, self.recv = out, inn, send, recv
        self.size = out.shape[1] // CHUNKS
        self.me, self.partner, self.cross, self.diag = neighbours()

    def rows(self, chunk):
        return pl.ds(pl.multiple_of(chunk * self.size, self.size), self.size)

    def copy(self, kind, chunk):
        return pltpu.make_async_remote_copy(
            src_ref=self.out.at[kind, self.rows(chunk), :], dst_ref=self.inn.at[kind, self.rows(chunk), :],
            send_sem=self.send.at[kind, chunk], recv_sem=self.recv.at[kind, chunk],
            device_id={"mp": self.cross if kind == 1 else self.partner}, device_id_type=MESH,
        )

    def put(self, kind, chunk, value):
        self.out[kind, self.rows(chunk), :] = value.astype(BF)
        self.copy(kind, chunk).start()

    def take(self, kind, chunk):
        self.copy(kind, chunk).wait_recv()
        return self.inn[kind, self.rows(chunk), :].astype(F32)

    def drain(self, chunk, kinds=(0, 1, 2)):
        for kind in kinds:
            self.copy(kind, chunk).wait_send()


def slot_of(place):
    return 4 * lax.rem(place, 2) + 2 * lax.rem(place // 2, 2) + place // 4


def half_of(ref, i):
    size = ref.shape[1] // 2
    return pl.ds(pl.multiple_of(i * size, size), size)


def pack(ref, half, value, at=0, order=(0, 1, 2)):
    size = ref.shape[1]
    for j in range(SLOTS // 2):
        bits = (j % 2, j // 2, half)
        slot = 4 * bits[order[0]] + 2 * bits[order[1]] + bits[order[2]]
        ref[slot, :, at : at + value.shape[1]] = value[j * size : (j + 1) * size].astype(BF)


def moves():
    return [pltpu.SemaphoreType.DMA((3, CHUNKS)), pltpu.SemaphoreType.DMA((3, CHUNKS))]


def halves(rows, cols):
    return [pltpu.VMEM((3, rows, cols), BF), pltpu.VMEM((3, rows, cols), BF)] + moves()


class Moves:
    def __init__(self, sem, pairs):
        self.copies = [pltpu.make_async_copy(src, dst, sem.at[i]) for i, (src, dst) in enumerate(pairs)]

    def start(self, *which):
        for i in which:
            self.copies[i].start()

    def wait(self, *which):
        for i in which:
            self.copies[i].wait()


def row(ref, number):
    return ref[number : number + 1, :]


def like(*arrays):
    return [pltpu.VMEM(a.shape, a.dtype) for a in arrays]


def call(kernel, name, number, outs, scratch, *args, far=0, far_out=0):
    anywhere = pl.BlockSpec(memory_space=pl.ANY)
    return pl.pallas_call(
        kernel,
        out_shape=tuple(jax.ShapeDtypeStruct(shape, dtype) for shape, dtype in outs),
        in_specs=[vmem()] * (len(args) - far) + [anywhere] * far,
        out_specs=tuple([vmem()] * (len(outs) - far_out) + [anywhere] * far_out),
        scratch_shapes=scratch,
        compiler_params=pltpu.CompilerParams(
            vmem_limit_bytes=VMEM_MOST, collective_id=number, has_side_effects=True
        ),
        name=name,
    )(*args)


def attend_block(q_ref, k_ref, v_ref, table_ref, ids_ref, cols_ref, ctx_ref, lse_ref, seq, index):
    cols = q_ref.shape[1]
    length = ids_ref.shape[1]
    base = seq * length
    start, width = window(index, length)
    here = pl.ds(pl.multiple_of(index * BLOCK, BLOCK), BLOCK)
    rows = pl.ds(pl.multiple_of(base + index * BLOCK, BLOCK), BLOCK)
    keys_at = pl.ds(pl.multiple_of(base + start, 128), width)
    query = q_ref[rows, :]
    keys = k_ref[keys_at, :]
    values = v_ref[keys_at, :]
    same = cols_ref[rows, 0:1] == ids_ref[pl.ds(seq, 1), pl.ds(start, width)]
    context = jnp.zeros((BLOCK, cols), F32)
    sums = jnp.zeros((BLOCK, 128), F32)
    lane = lax.broadcasted_iota(jnp.int32, (1, 128), 1)
    for head in range(cols // HEAD_DIM):
        mine = head_lanes(head, cols)
        scores = dot_nt(jnp.where(mine, query, 0), keys)
        scores = jnp.where(same, scores + table_ref[head, here, pl.ds(start, width)].astype(F32), -1e30)
        peak = jnp.max(scores, axis=-1, keepdims=True)
        expo = jnp.exp(scores - peak)
        total = jnp.sum(expo, axis=-1, keepdims=True)
        part = dot(expo.astype(BF), values) * (1.0 / total)
        context = jnp.where(mine, part, context)
        sums = jnp.where(lane == head, peak + jnp.log(total), sums)
    ctx_ref[rows, :] = context.astype(BF)
    lse_ref[rows, :] = sums


def front_kernel(
    x_ref, par_ref, w_ref, bias_ref, cot_ref, ids_ref, table_hbm,
    ctx_ref, lse_ref, rows_hbm, grad_hbm, q_hbm, k_hbm, v_hbm,
    table_ref, cols_ref, rows_ref, grad_ref, q_ref, k_ref, v_ref, load, send, recv, gsend, grecv,
):
    net = Gather(rows_ref, send, recv)
    top = Gather(grad_ref, gsend, grecv)
    seqs, length = ids_ref.shape
    moves = Moves(
        load,
        ((table_hbm, table_ref), (rows_ref, rows_hbm), (grad_ref, grad_hbm), (q_ref, q_hbm), (k_ref, k_hbm), (v_ref, v_hbm)),
    )
    moves.start(0)
    greet_mp()

    def own(chunk):
        part = x_ref[pl.ds(pl.multiple_of(chunk * net.size, net.size), net.size), :].astype(F32)
        rows_ref[net.rows(net.me, chunk), :] = norm_rows(part, row(par_ref, ATTN_GAIN), row(par_ref, ATTN_SHIFT))[0].astype(BF)
        net.send_own(chunk)

    loop(CHUNKS, own)

    def top_own(chunk):
        part = cot_ref[pl.ds(pl.multiple_of(chunk * net.size, net.size), net.size), :].astype(F32)
        grad_ref[net.rows(net.me, chunk), :] = (part * row(par_ref, MLP_SCALE)).astype(BF)

    loop(CHUNKS, top_own)
    id_columns(ids_ref, cols_ref, seqs, length)
    tall = 2 * net.size

    def project(block):
        def part(i):
            at = pl.ds(pl.multiple_of(block * CHUNKS * net.size + i * tall, tall), tall)
            rows = rows_ref[at, :]
            query = dot_nt(rows, w_ref[0]) + bias_ref[0:1, :].astype(F32)
            q_ref[at, :] = (query.astype(BF).astype(F32) * 0.125).astype(BF)
            k_ref[at, :] = dot_nt(rows, w_ref[1]).astype(BF)
            v_ref[at, :] = (dot_nt(rows, w_ref[2]) + bias_ref[1:2, :].astype(F32)).astype(BF)

        loop(CHUNKS // 2, part)

    def attend(seq, index):
        attend_block(q_ref, k_ref, v_ref, table_ref, ids_ref, cols_ref, ctx_ref, lse_ref, seq, index)

    project(net.me)
    loop(CHUNKS, net.wait_partner)
    project(net.partner)
    moves.wait(0)
    mine = net.me // 2
    steps = length // BLOCK

    def near(i):
        attend(mine, i)
        net.relay(i)
        top.send_own(i)

    loop(steps, near)
    project(net.cross)
    loop(CHUNKS, net.wait_diag)
    project(net.diag)
    moves.start(1, 3, 4, 5)

    def far(i):
        attend(1 - mine, i)
        top.relay(i)
        net.drain(i)

    loop(steps, far)
    for wait in (top.wait_partner, top.wait_diag):
        loop(CHUNKS, wait)
    moves.start(2)
    loop(CHUNKS, top.drain)
    moves.wait(1, 2, 3, 4, 5)


def front(patches, params, weight, bias, cotangent, ids, table):
    rows, width = patches.shape
    cols = weight.shape[1]
    one, wide = ((4 * rows, cols), BF), ((4 * rows, width), BF)
    return call(
        front_kernel, "front", 1, [one, ((4 * rows, 128), F32), wide, wide, one, one, one],
        [pltpu.VMEM(table.shape, BF), pltpu.VMEM((4 * rows, 128), F32)]
        + [pltpu.VMEM(*shape) for shape in (wide, wide, one, one, one)]
        + [pltpu.SemaphoreType.DMA((6,))] + moves() + moves(),
        patches, params, weight, bias, cotangent, ids, table, far=1, far_out=5,
    )


def project_kernel(
    ctx_ref, w_ref, x_ref, par_ref, attn_ref, mid_ref, norm_ref, out, inn, send, recv
):
    net = Scatter(out, inn, send, recv)
    greet_mp()

    def share(block, chunk):
        at = pl.ds(pl.multiple_of((block * CHUNKS + chunk) * net.size, net.size), net.size)
        return dot(ctx_ref[at, :], w_ref[...])

    loop(CHUNKS, lambda c: net.put(0, c, share(net.diag, c)))
    loop(CHUNKS, lambda c: net.put(1, c, share(net.cross, c) + net.take(0, c)))
    loop(CHUNKS, lambda c: net.put(2, c, share(net.partner, c)))

    def own(chunk):
        attn_ref[net.rows(chunk), :] = share(net.me, chunk) + net.take(2, chunk) + row(par_ref, PROJ_BIAS)

    loop(CHUNKS, own)

    def last(chunk):
        at = net.rows(chunk)
        attn = attn_ref[at, :] + net.take(1, chunk)
        middle = x_ref[at, :].astype(F32) + row(par_ref, ATTN_SCALE) * attn
        attn_ref[at, :] = attn
        mid_ref[at, :] = middle
        norm_ref[at, :] = norm_rows(middle, row(par_ref, MLP_GAIN), row(par_ref, MLP_SHIFT))[0].astype(BF)

    loop(CHUNKS, last)
    loop(CHUNKS, net.drain)


def project(context, weight, patches, params):
    rows, width = patches.shape
    return call(
        project_kernel, "project", 2, [((rows, width), F32), ((rows, width), F32), ((rows, width), BF)],
        halves(rows, width), context, weight, patches, params,
    )


def gelu_both(u):
    inner = 0.7978845608028654 * (u + 0.044715 * (u * u * u))
    t = jnp.tanh(inner)
    half = 0.5 * (1.0 + t)
    slope = half + (0.5 * u) * (1.0 - t * t) * (0.7978845608028654 * (1.0 + 0.134145 * (u * u)))
    return u * half, slope


def mlp_kernel(
    norm_ref, par_ref, up_hbm, down_hbm, grad_hbm, mid_hbm, attn_hbm, cot_hbm,
    gmid_ref, gattn_ref, sums_ref, cross_hbm, here_hbm, upg_hbm, downg_hbm,
    up_ref, down_ref, grad_ref, mid_ref, attn_ref, cot_ref, cross_ref, here_ref, upg_ref, downg_ref, load,
    rows_ref, hid_ref, pre_ref, own_ref, far_ref, mfar_ref, gsend, grecv, out, inn, send, recv,
    mout, minn, msend, mrecv,
):
    gat = Gather(rows_ref, gsend, grecv)
    net = Scatter(out, inn, send, recv)
    top = Scatter(mout, minn, msend, mrecv)
    size = gat.size
    moves = Moves(
        load,
        (
            (up_hbm, up_ref), (down_hbm, down_ref), (grad_hbm, grad_ref), (mid_hbm, mid_ref), (attn_hbm, attn_ref),
            (cot_hbm, cot_ref), (cross_ref, cross_hbm), (here_ref, here_hbm), (upg_ref, upg_hbm), (downg_ref, downg_hbm),
        ),
    )
    moves.start(0, 1, 2, 3, 4, 5)
    greet_mp()
    sums_ref[...] = jnp.zeros_like(sums_ref)

    def own(chunk):
        rows_ref[gat.rows(gat.me, chunk), :] = norm_ref[net.rows(chunk), :]
        gat.send_own(chunk)

    loop(CHUNKS, own)

    moves.wait(0, 1, 2)

    def two(first, second, chunk):
        at, by = gat.rows(first, chunk), gat.rows(second, chunk)
        both = lambda ref: jnp.concatenate([ref[at, :], ref[by, :]], axis=0)
        value, slope = gelu_both(dot(both(rows_ref), up_ref[...]) + row(par_ref, UP_BIAS))
        hidden = value.astype(BF)
        hid_ref[at, :], hid_ref[by, :] = hidden[:size], hidden[size:]
        grad_pre = (dot_nt(both(grad_ref), down_ref[...]) * slope).astype(BF)
        pre_ref[at, :], pre_ref[by, :] = grad_pre[:size], grad_pre[size:]
        sums_ref[0:1, :] += jnp.sum(grad_pre.astype(F32), axis=0, keepdims=True)
        back = dot_nt(grad_pre, up_ref[...])
        part = dot(hidden, down_ref[...])
        return back[:size], back[size:], part[:size], part[size:]

    def near(chunk):
        gat.wait_partner(chunk)
        theirs, mine, share, kept = two(gat.partner, gat.me, chunk)
        net.put(2, chunk, theirs)
        top.put(2, chunk, share)
        own_ref[net.rows(chunk), :] = mine
        here_ref[net.rows(chunk), :] = kept

    loop(CHUNKS, near)

    def across(chunk):
        net.put(1, chunk, far_ref[net.rows(chunk), :] + net.take(0, chunk))

    def far(chunk):
        gat.relay(chunk)
        gat.wait_diag(chunk)
        theirs, mine, share, kept = two(gat.diag, gat.cross, chunk)
        net.put(0, chunk, theirs)
        top.put(0, chunk, share)
        far_ref[net.rows(chunk), :] = mine
        mfar_ref[net.rows(chunk), :] = kept

        @pl.when(chunk > 0)
        def _():
            across(chunk - 1)

    loop(CHUNKS, far)
    across(CHUNKS - 1)

    def weights(i):
        pack(upg_ref, i, dot_tn(rows_ref[:, half_of(rows_ref, i)], pre_ref[...]))
        pack(downg_ref, i, dot_tn(grad_ref[:, half_of(grad_ref, i)], hid_ref[...]))

    loop(2, weights)

    def outs(chunk):
        at = net.rows(chunk)
        here_ref[at, :] += top.take(2, chunk)
        cross_ref[at, :] = (mfar_ref[at, :] + top.take(0, chunk)).astype(BF)

    loop(CHUNKS, outs)
    moves.start(6, 7, 8, 9)
    moves.wait(3, 4, 5)

    def last(chunk):
        at = net.rows(chunk)
        grad = own_ref[at, :] + net.take(2, chunk) + net.take(1, chunk)
        normed, inv = norm_rows(mid_ref[at, :], 1.0, 0.0)[1:]
        back, gain_sum, shift_sum = norm_back(grad, normed, inv, row(par_ref, MLP_GAIN))
        middle = cot_ref[at, :].astype(F32) + back
        gattn = (middle * row(par_ref, ATTN_SCALE)).astype(BF)
        gmid_ref[at, :] = middle
        gattn_ref[at, :] = gattn
        sums_ref[1:2, :] += gain_sum[None]
        sums_ref[2:3, :] += shift_sum[None]
        sums_ref[3:4, :] += jnp.sum(middle * attn_ref[at, :], axis=0, keepdims=True)
        sums_ref[4:5, :] += jnp.sum(gattn.astype(F32), axis=0, keepdims=True)

    loop(CHUNKS, last)
    loop(CHUNKS, gat.drain)
    loop(CHUNKS, net.drain)
    loop(CHUNKS, lambda chunk: top.drain(chunk, (0, 2)))
    moves.wait(6, 7, 8, 9)


def mlp(normed, params, up, down, grad_rows, middle, attn, cotangent):
    rows, width = normed.shape
    ff = up.shape[1]
    one = pltpu.VMEM((rows, width), F32)
    packed = ((SLOTS, width // SLOTS, ff), BF)
    late = [((rows, width), BF), ((rows, width), F32), packed, packed]
    return call(
        mlp_kernel, "mlp", 3,
        [((rows, width), F32), ((rows, width), BF), ((8, width), F32)] + late,
        like(up, down, grad_rows, middle, attn, cotangent) + [pltpu.VMEM(*shape) for shape in late]
        + [pltpu.SemaphoreType.DMA((10,))]
        + [pltpu.VMEM((4 * rows, width), BF), pltpu.VMEM((4 * rows, ff), BF), pltpu.VMEM((4 * rows, ff), BF), one, one, one]
        + moves() + halves(rows, width) + halves(rows, width),
        normed, params, up, down, grad_rows, middle, attn, cotangent, far=6, far_out=4,
    )


class Fold:
    def __init__(self, src, inn, send, recv, order=(0, 1, 2)):
        self.src, self.inn, self.send, self.recv = src, inn, send, recv
        self.size = src.shape[1] // PARTS
        place = lax.axis_index("dp")
        bits = (lax.rem(place, 2), lax.rem(place // 2, 2), place // 4)
        a, b, c = [bits[i] for i in order]
        self.peers = [place + (1 << i) - (2 << i) * bits[i] for i in order]
        self.theirs = (4 * (1 - a), 2 * (1 - b), 4 + 1 - c)
        self.mine = (4 * a, 2 * b, 4 + c)

    def copy(self, stage, part):
        count, offset = (4, 2, 1)[stage], (0, 4, 6)[stage]
        rows = pl.ds(part * self.size, self.size)
        src = self.src if stage == 0 else self.inn
        return pltpu.make_async_remote_copy(
            src_ref=src.at[pl.ds(self.theirs[stage], count), rows, :],
            dst_ref=self.inn.at[pl.ds(offset, count), rows, :],
            send_sem=self.send.at[stage, part], recv_sem=self.recv.at[stage, part],
            device_id={"dp": self.peers[stage]}, device_id_type=MESH,
        )

    def start(self):
        for part in range(PARTS):
            self.copy(0, part).start()

    def advance(self, stage):
        count, offset = (4, 2)[stage], (0, 4)[stage]
        src = self.src if stage == 0 else self.inn
        for part in range(PARTS):
            rows = pl.ds(part * self.size, self.size)
            self.copy(stage, part).wait_recv()
            for i in range(count):
                self.inn[offset + i, rows, :] = self.inn[offset + i, rows, :] + src[self.mine[stage] + i, rows, :]
            self.copy(stage + 1, part).start()

    def finish(self, put):
        for part in range(PARTS):
            rows = pl.ds(part * self.size, self.size)
            self.copy(2, part).wait_recv()
            put(rows, self.inn[self.mine[2], rows, :].astype(F32) + self.inn[6, rows, :].astype(F32))

    def drain(self):
        for stage in range(3):
            for part in range(PARTS):
                self.copy(stage, part).wait_send()


class Total:
    def __init__(self, acc, inn, send, recv):
        self.acc, self.inn, self.send, self.recv = acc, inn, send, recv
        place = lax.axis_index("dp")
        x, lo, hi = lax.rem(place, 2), lax.rem(place // 2, 2), place // 4
        _, partner, cross, _ = neighbours()
        self.peers = (
            {"dp": place + 1 - 2 * x}, {"dp": place + 2 - 4 * lo}, {"dp": place + 4 - 8 * hi}, {"mp": partner}, {"mp": cross},
        )

    def copy(self, stage):
        return pltpu.make_async_remote_copy(
            src_ref=self.acc.at[stage], dst_ref=self.inn.at[stage], send_sem=self.send.at[stage],
            recv_sem=self.recv.at[stage], device_id=self.peers[stage], device_id_type=MESH,
        )

    def start(self, stage):
        self.copy(stage).start()

    def finish(self, stage):
        self.copy(stage).wait_recv()
        self.acc[stage + 1] = self.acc[stage] + self.inn[stage]

    def drain(self):
        for stage in range(5):
            self.copy(stage).wait_send()


def back_kernel(
    fold,
    pw_ref, ids_ref, par_ref, two_ref, rows_hbm, table_hbm, *refs,
):
    early, refs = refs[:EARLY], refs[EARLY:]
    if fold:
        layer_ref, grad_ref, tab_ref, upo_ref, downo_ref, mixo_ref, sums_ref, *refs = refs
        band_ref, mix_ref, acc_ref, *refs = refs
        winn, wsend, wrecv, tinn, tsend, trecv, ainn, asend, arecv, *refs = refs
    else:
        layer_ref, grad_ref, band_ref, mix_ref, sums_ref, *refs = refs
        acc_ref = None
    held, refs = refs[: EARLY - 1], refs[EARLY - 1 :]
    upg_ref, downg_ref, q_ref, k_ref, v_ref, lse_ref, cross_ref, ctx_ref, w_ref, here_ref, mid_ref, cot_ref, x_ref, gmid_ref = held
    (
        table_ref, cols_ref, rowsg_ref, g_ref, qt_ref, gt_ref, dkt_ref, dvt_ref, strip_ref, dq_ref, dv_ref,
        far_ref, load, hold, fsend, frecv, gsend, grecv, out, inn, send, recv,
    ) = refs
    dk_ref = g_ref
    own_ref = grad_ref
    gat = Gather(rowsg_ref, gsend, grecv)
    net = Scatter(out, inn, send, recv)
    seqs, length = ids_ref.shape
    rows_all, cols = q_ref.shape
    blocks = length // BLOCK
    heads = cols // HEAD_DIM
    small_ref = acc_ref.at[0] if fold else sums_ref
    me, partner, cross, _ = neighbours()
    whole = CHUNKS * gat.size
    mine_at = pl.ds(pl.multiple_of(me * whole, whole), whole)
    moves = Moves(hold, [(early[0], rowsg_ref.at[mine_at, :])] + list(zip(early[1:], held)))
    moves.start(*range(7))

    def fetch(head):
        at = pl.ds(pl.multiple_of(lax.rem(head, 2) * length, length), length)
        return pltpu.make_async_copy(table_hbm.at[head], table_ref.at[at, :], load.at[1 + head])

    fetch(0).start()
    fetch(1).start()
    moves.start(*range(7, EARLY))
    far = pltpu.make_async_remote_copy(
        src_ref=cross_ref, dst_ref=far_ref, send_sem=fsend, recv_sem=frecv, device_id={"mp": cross}, device_id_type=MESH
    )
    if fold:
        up = Fold(upg_ref, winn.at[0], wsend.at[0], wrecv.at[0])
        down = Fold(downg_ref, winn.at[1], wsend.at[1], wrecv.at[1])
        mix = Fold(mix_ref, winn.at[2], wsend.at[2], wrecv.at[2], MIX_ORDER)
        tab = lambda head: Fold(band_ref.at[head], tinn.at[head], tsend.at[head], trecv.at[head])
        small = Total(acc_ref, ainn, asend, arecv)
        greet(({"mp": partner}, {"mp": cross}) + tuple({"dp": peer} for peer in up.peers))
    else:
        greet_mp()

    moves.wait(0)
    loop(CHUNKS, gat.send_own)
    moves.wait(1, 2)
    if fold:
        up.start()
        down.start()
    id_columns(ids_ref, cols_ref, seqs, length)

    def block(number):
        at = pl.ds(pl.multiple_of(number * whole, whole), whole)
        g_ref[at, :] = dot_nt(rowsg_ref[at, :], pw_ref[...]).astype(BF)

    def tall(i):
        return pl.ds(pl.multiple_of(i * BLOCK, BLOCK), BLOCK)

    def flip_q(i):
        qt_ref[:, tall(i)] = q_ref[tall(i), :].T

    def flip_g(i):
        gt_ref[:, tall(i)] = g_ref[tall(i), :].T

    per = rows_all // BLOCK // seqs
    near_seq = gat.me // 2
    block(gat.me)
    dkt_ref[...] = jnp.zeros_like(dkt_ref)
    dvt_ref[...] = jnp.zeros_like(dvt_ref)
    dq_ref[...] = jnp.zeros_like(dq_ref)
    small_ref[...] = jnp.zeros_like(small_ref)
    if fold:
        tab_ref[...] = jnp.zeros_like(tab_ref)
    moves.wait(3, 4, 5, 6)
    loop(rows_all // BLOCK, flip_q)
    loop(CHUNKS, gat.wait_partner)
    block(gat.partner)
    loop(per, lambda i: flip_g(near_seq * per + i))
    lane = lax.broadcasted_iota(jnp.int32, (1, 128), 1)

    def step(head, index, seq, first):
        start, width = window(index, length)
        mine = head_lanes(head, cols)
        feats = pl.ds(pl.multiple_of(head * HEAD_DIM, HEAD_DIM), HEAD_DIM)
        rows = tall(seq * blocks + index)
        keys_at = pl.ds(pl.multiple_of(seq * length + start, 128), width)
        keys = k_ref[keys_at, :]
        same = cols_ref[rows, 0:1] == ids_ref[pl.ds(seq, 1), pl.ds(start, width)]
        sums = jnp.sum(jnp.where(lane == head, lse_ref[rows, :], 0.0), axis=-1, keepdims=True)
        bias = table_ref[tall(lax.rem(head, 2) * blocks + index), pl.ds(start, width)].astype(F32)
        scores = dot_nt(jnp.where(mine, q_ref[rows, :], 0), keys) + bias
        probs = jnp.where(same, jnp.exp(scores - sums), 0.0)
        grad_probs = dot_nt(jnp.where(mine, g_ref[rows, :], 0), v_ref[keys_at, :])
        centre = jnp.sum(grad_probs * probs, axis=-1, keepdims=True)
        grad_scores = (probs * (grad_probs - centre)).astype(BF)
        strip_ref[:, 0:width] = grad_scores
        dvt_ref[feats, keys_at] += dot(gt_ref[feats, rows], probs.astype(BF))
        dkt_ref[feats, keys_at] += dot(qt_ref[feats, rows], grad_scores)
        grad_q = (dot(grad_scores, keys) * 0.125).astype(BF)
        dq_ref[rows, :] = jnp.where(mine, grad_q, dq_ref[rows, :])
        for part in range(BLOCK // GROUP):
            group = index * (BLOCK // GROUP) + part
            begin, wide = band_window(group, length)
            offset = pl.multiple_of(begin - start, 128)
            value = strip_ref[part * GROUP : (part + 1) * GROUP, pl.ds(offset, wide)]
            slot = slot_of(group)
            if not first:
                value = (value.astype(F32) + band_ref[head, slot, :, :].astype(F32)).astype(BF)
            band_ref[head, slot, :, :] = value

    def one_head(head, seq, first):
        fetch(head).wait()

        def inner(index):
            step(head, index, seq, first)
            if first:
                i = head * blocks + index

                @pl.when(lax.rem(i, heads) == heads - 1)
                def _():
                    gat.relay(i // heads)

        loop(blocks, inner)

        @pl.when(head + 2 < heads)
        def _():
            fetch(head + 2).start()

    def near_head(head):
        one_head(head, near_seq, True)

    def far_head(head):
        one_head(head, 1 - near_seq, False)
        if fold:
            tab(head).start()

            @pl.when(head == 0)
            def _():
                down.advance(0)
                up.advance(1)

            @pl.when(head == 1)
            def _():
                down.advance(1)

            @pl.when(head == 2)
            def _():
                tab(0).advance(0)

    loop(heads, near_head)
    fetch(0).start()
    fetch(1).start()
    block(gat.cross)
    loop(CHUNKS, gat.wait_diag)
    block(gat.diag)
    moves.wait(7)
    far.start()
    loop(per, lambda i: flip_g((1 - near_seq) * per + i))
    if fold:
        up.advance(0)
    loop(heads, far_head)
    moves.wait(*range(8, EARLY))
    rows_ref = table_ref.at[:, 0 : rowsg_ref.shape[1]]
    again = pltpu.make_async_copy(rows_hbm, rows_ref, load.at[0])
    again.start()

    def unflip(i):
        dk_ref[tall(i), :] = dkt_ref[:, tall(i)].T.astype(BF)
        dv_ref[tall(i), :] = dvt_ref[:, tall(i)].T.astype(BF)

    loop(rows_all // BLOCK, unflip)

    again.wait()

    order = MIX_ORDER if fold else (0, 1, 2)

    def weights(i):
        rows = table_ref[:, half_of(rowsg_ref, i)]
        for number, ref in enumerate((dq_ref, dk_ref, dv_ref)):
            pack(mix_ref, i, dot_tn(rows, ref[...]), number * cols, order)
        pack(mix_ref, i, dot_tn(rowsg_ref[:, half_of(rowsg_ref, i)], ctx_ref[...]), 3 * cols, order)

    loop(2, weights)

    def put_table(head):
        def put(rows, value):
            first = band_window(lax.axis_index("dp"), length)[0]
            tab_ref[head, rows, pl.ds(first, value.shape[1])] = value
        return put

    def put_to(ref):
        def put(rows, value):
            ref[rows, :] = value
        return put

    if fold:
        mix.start()

    def share(number, chunk):
        at = gat.rows(number, chunk)
        return dot(dq_ref[at, :], w_ref[0]) + dot(dk_ref[at, :], w_ref[1]) + dot(dv_ref[at, :], w_ref[2])

    loop(CHUNKS, lambda c: net.put(0, c, share(net.diag, c)))
    loop(CHUNKS, lambda c: net.put(1, c, share(net.cross, c) + net.take(0, c)))
    if fold:
        up.finish(put_to(upo_ref))
        down.finish(put_to(downo_ref))
        tab(0).advance(1)
        tab(1).advance(0)
    loop(CHUNKS, lambda c: net.put(2, c, share(net.partner, c)))

    def keep(chunk):
        own_ref[net.rows(chunk), :] = share(net.me, chunk) + net.take(2, chunk)

    loop(CHUNKS, keep)
    far.wait_recv()

    def layer(chunk):
        at = net.rows(chunk)
        mlp_out = here_ref[at, :] + far_ref[at, :].astype(F32) + row(par_ref, DOWN_BIAS)
        layer_ref[at, :] = (mid_ref[at, :] + row(par_ref, MLP_SCALE) * mlp_out).astype(BF)
        top = cot_ref[at, :].astype(F32)
        small_ref[7:8, :] += jnp.sum(top * mlp_out, axis=0, keepdims=True)
        low = (top * row(par_ref, MLP_SCALE)).astype(BF).astype(F32)
        small_ref[6:7, :] += jnp.sum(low, axis=0, keepdims=True)

    loop(CHUNKS, layer)
    for put, source in ((2, 4), (3, 3), (4, 1), (5, 2), (8, 0)):
        small_ref[put : put + 1, :] = two_ref[source : source + 1, :]
    small_ref[9:10, 0:cols] = jnp.sum(dq_ref[...].astype(F32), axis=0, keepdims=True)
    small_ref[10:11, 0:cols] = jnp.sum(dv_ref[...].astype(F32), axis=0, keepdims=True)
    if fold:
        tab(2).advance(0)
        tab(1).advance(1)
        tab(0).finish(put_table(0))

    def last(chunk):
        at = net.rows(chunk)
        grad = own_ref[at, :] + net.take(1, chunk)
        normed, inv = norm_rows(x_ref[at, :].astype(F32), 1.0, 0.0)[1:]
        back, gain_sum, shift_sum = norm_back(grad, normed, inv, row(par_ref, ATTN_GAIN))
        grad_ref[at, :] = gmid_ref[at, :] + back
        small_ref[0:1, :] += gain_sum[None]
        small_ref[1:2, :] += shift_sum[None]

    loop(CHUNKS, last)
    if fold:
        small.start(0)
        mix.advance(0)
        small.finish(0)
        small.start(1)
        tab(2).advance(1)
        tab(1).finish(put_table(1))
        small.finish(1)
        small.start(2)
        mix.advance(1)
        small.finish(2)
        small.start(3)
        tab(2).finish(put_table(2))
        small.finish(3)
        small.start(4)
        mix.finish(put_to(mixo_ref))
        small.finish(4)
        sums_ref[0:8, :] = acc_ref[5, 0:8, :]
        sums_ref[8:16, :] = acc_ref[3, 8:16, :]
        for piece in (up, down, mix, tab(0), tab(1), tab(2), small):
            piece.drain()
    far.wait_send()
    loop(CHUNKS, gat.drain)
    loop(CHUNKS, net.drain)


def back(fold, length, proj, ids, params, two, rows_one, table, *early):
    rows, width = early[0].shape
    cols = proj.shape[0]
    heads = cols // HEAD_DIM
    piece, wide = width // SLOTS, band_window(0, length)[1]
    strip = min(length, BLOCK + 2 * PAGE_MOST)
    band, mix = ((heads, SLOTS, GROUP, wide), BF), ((SLOTS, piece, width), BF)
    outs = [((rows, width), BF), ((rows, width), F32)]
    scratch = []
    if fold:
        sem = pltpu.SemaphoreType.DMA((3, 3, PARTS))
        outs += [((heads, GROUP, length), F32)] + [((piece, width), F32)] * 3
        scratch += [pltpu.VMEM(*band), pltpu.VMEM(*mix), pltpu.VMEM((6, 16, width), F32)]
        scratch += [pltpu.VMEM((3, 7, piece, width), BF), sem, sem, pltpu.VMEM((heads, 7, GROUP, wide), BF), sem, sem]
        scratch += [pltpu.VMEM((5, 16, width), F32), pltpu.SemaphoreType.DMA((5,)), pltpu.SemaphoreType.DMA((5,))]
    else:
        outs += [band, mix]
    outs += [((16, width), F32)]
    one, flat = pltpu.VMEM((4 * rows, cols), BF), pltpu.VMEM((cols, 4 * rows), BF)
    total = pltpu.VMEM((cols, 4 * rows), F32)
    scratch += like(*early[1:]) + [
        pltpu.VMEM((2 * length, length), BF), pltpu.VMEM((4 * rows, 128), F32), pltpu.VMEM((4 * rows, width), BF), one,
        flat, flat, total, total, pltpu.VMEM((BLOCK, strip), BF), one, one, pltpu.VMEM((rows, width), BF),
        pltpu.SemaphoreType.DMA((1 + heads,)), pltpu.SemaphoreType.DMA((EARLY,)),
        pltpu.SemaphoreType.DMA, pltpu.SemaphoreType.DMA,
    ] + moves() + halves(rows, width)
    return call(
        partial(back_kernel, fold), "back", 4, outs, scratch, proj, ids, params, two, rows_one, table, *early, far=2 + EARLY
    )


def scatter_dp(x):
    return lax.psum_scatter(x, "dp", scatter_dimension=0, tiled=True).astype(F32)


def in_order(packed):
    _, rows, cols = packed.shape
    return packed.reshape(2, 2, 2, rows, cols).transpose(2, 1, 0, 3, 4).reshape(SLOTS * rows, cols)


def reduce_table(band, length, n_dp):
    groups, heads, _, wide = band.shape
    shard = length // n_dp
    send = band.reshape(groups, heads, GROUP // shard, shard, wide).swapaxes(1, 2)
    part = scatter_dp(send.reshape(n_dp * heads * shard, wide)).reshape(heads, shard, wide)
    first = band_window(lax.axis_index("dp") * shard // GROUP, length)[0]
    return lax.dynamic_update_slice(jnp.zeros((heads, shard, length), F32), part, (0, 0, first))


def local(
    patches, segment_ids, fill_counts, attn_gain, attn_shift, qkv_weight, qv_bias, rel_table, proj_weight,
    proj_bias, attn_scale, mlp_gain, mlp_shift, up_weight, up_bias, down_weight, down_bias, mlp_scale, cotangent,
):
    n_dp = lax.axis_size("dp")
    seqs, length = segment_ids.shape
    cols = qkv_weight.shape[2]
    places = jnp.arange(length, dtype=jnp.int32)[None]
    ids = jnp.where(places < fill_counts[:, None], segment_ids, -1 - places).astype(F32)
    fold = n_dp == SLOTS and length == SLOTS * GROUP
    vectors = (attn_gain, attn_shift, proj_bias, attn_scale, mlp_gain, mlp_shift, up_bias, down_bias, mlp_scale)
    params = jnp.concatenate([v.astype(F32) for v in vectors]).reshape(len(vectors), -1)
    turned = qkv_weight.swapaxes(1, 2)
    context, lse, rows_one, grad_rows, queries, keys, values = front(
        patches, params, turned, qv_bias, cotangent, ids, rel_table
    )
    attn_out, middle, normed_two = project(context, proj_weight, patches, params)
    grad_middle, grad_attn, sums_two, cross, here, up_local, down_local = mlp(
        normed_two, params, up_weight, down_weight, grad_rows, middle, attn_out, cotangent
    )
    layer_out, patch_grad, *more, sums = back(
        fold, length, proj_weight, ids, params, sums_two, rows_one, rel_table,
        grad_attn, up_local, down_local, queries, keys, values, lse, cross, context, turned, here, middle, cotangent,
        patches, grad_middle,
    )
    if fold:
        table_grad, up_grad, down_grad, mixed = more
    else:
        band, mixed = more
        order = [4 * (d % 2) + 2 * (d // 2 % 2) + d // 4 for d in range(SLOTS)]
        table_grad = reduce_table(jnp.stack([band[:, slot] for slot in order]), length, n_dp)
        up_grad, down_grad, mixed = [scatter_dp(in_order(piece)) for piece in (up_local, down_local, mixed)]
        sums = jnp.concatenate([lax.psum(sums[:8], ("dp", "mp")), lax.psum(sums[8:], "dp")])
    qkv_grad = mixed[:, : 3 * cols].reshape(-1, 3, cols).swapaxes(0, 1)
    return (
        layer_out, patch_grad, sums[0], sums[1], qkv_grad, sums[9:11, :cols], table_grad, mixed[:, 3 * cols :].T,
        sums[2], sums[3], sums[4], sums[5], up_grad, sums[8], down_grad.T, sums[6], sums[7],
    )


def solution(mesh):
    rows, split = P(("dp", "mp"), None), P("mp", None)
    placed = (
        rows, P("dp", None), P("dp"), P(), P(), P(None, None, "mp"), P(None, "mp"), P("mp", None, None), split,
        P(), P(), P(), P(), P(None, "mp"), P("mp"), split, P(), P(), rows,
    )
    given = (
        rows, rows, P(), P(), P(None, "dp", "mp"), P(None, "mp"), P("mp", "dp", None), P("mp", "dp"), P(), P(),
        P(), P(), P("dp", "mp"), P("mp"), P("mp", "dp"), P(), P(),
    )
    return jax.shard_map(local, mesh=mesh, in_specs=placed, out_specs=given, check_vma=False)
```

```python
from functools import partial

import jax
import jax.numpy as jnp
from jax import lax
from jax.experimental import pallas as pl
from jax.experimental.pallas import tpu as pltpu
from jax.sharding import PartitionSpec as P

HEAD_DIM = 64
BLOCK = 256
GROUP = 128

ATTN_GAIN, ATTN_SHIFT, PROJ_BIAS, ATTN_SCALE, MLP_GAIN, MLP_SHIFT, UP_BIAS, DOWN_BIAS, MLP_SCALE = range(9)
CHUNKS = 4
SLOTS = 8
PARTS = 2
EARLY = 15
MIX_ORDER = (0, 1, 2)
PAGE_MOST = 256
TILES = 2 * PAGE_MOST // GROUP
BF = jnp.bfloat16
F32 = jnp.float32
MESH = pl.DeviceIdType.MESH
VMEM_MOST = 61 * 1024 * 1024
NT = (((1,), (1,)), ((), ()))
TN = (((0,), (0,)), ((), ()))


def vmem():
    return pl.BlockSpec(memory_space=pltpu.VMEM)


def dot(a, b):
    return jnp.dot(a, b, preferred_element_type=F32)


def dot_nt(a, b):
    return lax.dot_general(a, b, NT, preferred_element_type=F32)


def dot_tn(a, b):
    return lax.dot_general(a, b, TN, preferred_element_type=F32)


def norm_rows(rows, gain, shift):
    centre = rows - jnp.mean(rows, axis=-1, keepdims=True)
    inv_std = lax.rsqrt(jnp.mean(centre * centre, axis=-1, keepdims=True) + 1e-06)
    normed = centre * inv_std
    return (normed * gain + shift, normed, inv_std)


def norm_back(grad_out, normed, inv_std, gain):
    scaled = grad_out * gain
    inner = (
        scaled
        - jnp.mean(scaled, axis=-1, keepdims=True)
        - normed * jnp.mean(scaled * normed, axis=-1, keepdims=True)
    )
    return (inv_std * inner, jnp.sum(grad_out * normed, axis=0), jnp.sum(grad_out, axis=0))


def window(index, length):
    width = min(length, BLOCK + 2 * PAGE_MOST)
    start = jnp.clip(index * BLOCK - PAGE_MOST, 0, length - width)
    return pl.multiple_of(start, 128), width


def edge(first_row, rows):
    place = lax.broadcasted_iota(jnp.int32, (rows, GROUP), 0) + first_row
    column = lax.broadcasted_iota(jnp.int32, (rows, GROUP), 1)
    return column > place, column < place


def head_lanes(head, cols):
    return lax.broadcasted_iota(jnp.int32, (1, cols), 1) // HEAD_DIM == head


def id_columns(ids_ref, cols_ref, seqs, length):
    for s in range(seqs):
        wide = jnp.broadcast_to(ids_ref[s : s + 1, :], (128, length))
        cols_ref[s * length : (s + 1) * length, :] = wide.T


def loop(count, body):
    lax.fori_loop(0, count, lambda i, _: (body(i), 0)[1], 0)


def neighbours():
    me = lax.axis_index("mp")
    partner = me + 1 - 2 * lax.rem(me, 2)
    return me, partner, lax.rem(me + 2, 4), lax.rem(partner + 2, 4)


def greet(peers):
    barrier = pltpu.get_barrier_semaphore()
    for peer in peers:
        pl.semaphore_signal(barrier, inc=1, device_id=peer, device_id_type=MESH)
    pl.semaphore_wait(barrier, len(peers))


def greet_mp():
    _, partner, cross, _ = neighbours()
    greet(({"mp": partner}, {"mp": cross}))


class Gather:
    def __init__(self, buffer, send, recv):
        self.buffer, self.send, self.recv = buffer, send, recv
        self.size = buffer.shape[0] // 4 // CHUNKS
        self.me, self.partner, self.cross, self.diag = neighbours()

    def rows(self, block, chunk):
        return pl.ds(pl.multiple_of((block * CHUNKS + chunk) * self.size, self.size), self.size)

    def copy(self, kind, block, chunk):
        part = self.buffer.at[self.rows(block, chunk), :]
        return pltpu.make_async_remote_copy(
            src_ref=part, dst_ref=part, send_sem=self.send.at[kind, chunk], recv_sem=self.recv.at[kind, chunk],
            device_id={"mp": self.cross if kind == 0 else self.partner}, device_id_type=MESH,
        )

    def send_own(self, chunk):
        self.copy(0, self.me, chunk).start()
        self.copy(1, self.me, chunk).start()

    def wait_partner(self, chunk):
        self.copy(1, self.partner, chunk).wait_recv()

    def relay(self, chunk):
        self.copy(0, self.cross, chunk).wait_recv()
        self.copy(2, self.cross, chunk).start()

    def wait_diag(self, chunk):
        self.copy(2, self.diag, chunk).wait_recv()

    def drain(self, chunk):
        self.copy(0, self.me, chunk).wait_send()
        self.copy(1, self.me, chunk).wait_send()
        self.copy(2, self.cross, chunk).wait_send()


class Scatter:
    def __init__(self, out, inn, send, recv):
        self.out, self.inn, self.send, self.recv = out, inn, send, recv
        self.size = out.shape[1] // CHUNKS
        self.me, self.partner, self.cross, self.diag = neighbours()

    def rows(self, chunk):
        return pl.ds(pl.multiple_of(chunk * self.size, self.size), self.size)

    def copy(self, kind, chunk):
        return pltpu.make_async_remote_copy(
            src_ref=self.out.at[kind, self.rows(chunk), :], dst_ref=self.inn.at[kind, self.rows(chunk), :],
            send_sem=self.send.at[kind, chunk], recv_sem=self.recv.at[kind, chunk],
            device_id={"mp": self.cross if kind == 1 else self.partner}, device_id_type=MESH,
        )

    def put(self, kind, chunk, value):
        self.out[kind, self.rows(chunk), :] = value.astype(BF)
        self.copy(kind, chunk).start()

    def take(self, kind, chunk):
        self.copy(kind, chunk).wait_recv()
        return self.inn[kind, self.rows(chunk), :].astype(F32)

    def drain(self, chunk, kinds=(0, 1, 2)):
        for kind in kinds:
            self.copy(kind, chunk).wait_send()


def slot_of(place):
    return 4 * lax.rem(place, 2) + 2 * lax.rem(place // 2, 2) + place // 4


def half_of(ref, i):
    size = ref.shape[1] // 2
    return pl.ds(pl.multiple_of(i * size, size), size)


def pack(ref, half, value, at=0, order=(0, 1, 2)):
    size = ref.shape[1]
    for j in range(SLOTS // 2):
        bits = (j % 2, j // 2, half)
        slot = 4 * bits[order[0]] + 2 * bits[order[1]] + bits[order[2]]
        ref[slot, :, at : at + value.shape[1]] = value[j * size : (j + 1) * size].astype(BF)


def moves():
    return [pltpu.SemaphoreType.DMA((3, CHUNKS)), pltpu.SemaphoreType.DMA((3, CHUNKS))]


def halves(rows, cols):
    return [pltpu.VMEM((3, rows, cols), BF), pltpu.VMEM((3, rows, cols), BF)] + moves()


class Moves:
    def __init__(self, sem, pairs):
        self.copies = [pltpu.make_async_copy(src, dst, sem.at[i]) for i, (src, dst) in enumerate(pairs)]

    def start(self, *which):
        for i in which:
            self.copies[i].start()

    def wait(self, *which):
        for i in which:
            self.copies[i].wait()


def row(vectors, number):
    return vectors[number][...].astype(F32).reshape(1, -1)


def some(vectors, *numbers):
    return {number: vectors[number] for number in numbers}


def like(*arrays):
    return [pltpu.VMEM(a.shape, a.dtype) for a in arrays]


def call(kernel, name, number, outs, scratch, *args, far=0, far_out=0):
    anywhere = pl.BlockSpec(memory_space=pl.ANY)
    return pl.pallas_call(
        kernel,
        out_shape=tuple(jax.ShapeDtypeStruct(shape, dtype) for shape, dtype in outs),
        in_specs=[jax.tree.map(lambda _: vmem(), arg) for arg in args[: len(args) - far]] + [anywhere] * far,
        out_specs=tuple([vmem()] * (len(outs) - far_out) + [anywhere] * far_out),
        scratch_shapes=scratch,
        compiler_params=pltpu.CompilerParams(
            vmem_limit_bytes=VMEM_MOST, collective_id=number, has_side_effects=True
        ),
        name=name,
    )(*args)


def attend_block(q_ref, k_ref, v_ref, table_ref, ids_ref, cols_ref, ctx_ref, lse_ref, seq, index):
    cols = q_ref.shape[1]
    length = ids_ref.shape[1]
    base = seq * length
    start, width = window(index, length)
    here = pl.ds(pl.multiple_of(index * BLOCK, BLOCK), BLOCK)
    rows = pl.ds(pl.multiple_of(base + index * BLOCK, BLOCK), BLOCK)
    keys_at = pl.ds(pl.multiple_of(base + start, 128), width)
    query = q_ref[rows, :]
    keys = k_ref[keys_at, :]
    values = v_ref[keys_at, :]
    same = cols_ref[rows, 0:1] == ids_ref[pl.ds(seq, 1), pl.ds(start, width)]
    context = jnp.zeros((BLOCK, cols), F32)
    sums = jnp.zeros((BLOCK, 128), F32)
    lane = lax.broadcasted_iota(jnp.int32, (1, 128), 1)
    for head in range(cols // HEAD_DIM):
        mine = head_lanes(head, cols)
        scores = dot_nt(jnp.where(mine, query, 0), keys)
        scores = jnp.where(same, scores + table_ref[head, here, pl.ds(start, width)].astype(F32), -1e30)
        peak = jnp.max(scores, axis=-1, keepdims=True)
        expo = jnp.exp(scores - peak)
        total = jnp.sum(expo, axis=-1, keepdims=True)
        part = dot(expo.astype(BF), values) * (1.0 / total)
        context = jnp.where(mine, part, context)
        sums = jnp.where(lane == head, peak + jnp.log(total), sums)
    ctx_ref[rows, :] = context.astype(BF)
    lse_ref[rows, :] = sums


def front_kernel(
    x_ref, par_ref, w_ref, bias_ref, cot_ref, ids_ref, table_hbm,
    ctx_ref, lse_ref, rows_hbm, grad_hbm, q_hbm, k_hbm, v_hbm,
    table_ref, cols_ref, rows_ref, grad_ref, q_ref, k_ref, v_ref, load, send, recv, gsend, grecv,
):
    net = Gather(rows_ref, send, recv)
    top = Gather(grad_ref, gsend, grecv)
    seqs, length = ids_ref.shape
    moves = Moves(
        load,
        ((table_hbm, table_ref), (rows_ref, rows_hbm), (grad_ref, grad_hbm), (q_ref, q_hbm), (k_ref, k_hbm), (v_ref, v_hbm)),
    )
    moves.start(0)
    greet_mp()

    def own(chunk):
        part = x_ref[pl.ds(pl.multiple_of(chunk * net.size, net.size), net.size), :].astype(F32)
        rows_ref[net.rows(net.me, chunk), :] = norm_rows(part, row(par_ref, ATTN_GAIN), row(par_ref, ATTN_SHIFT))[0].astype(BF)
        net.send_own(chunk)

    loop(CHUNKS, own)

    def top_own(chunk):
        part = cot_ref[pl.ds(pl.multiple_of(chunk * net.size, net.size), net.size), :].astype(F32)
        grad_ref[net.rows(net.me, chunk), :] = (part * row(par_ref, MLP_SCALE)).astype(BF)

    loop(CHUNKS, top_own)
    id_columns(ids_ref, cols_ref, seqs, length)
    tall = 2 * net.size

    def project(block):
        def part(i):
            at = pl.ds(pl.multiple_of(block * CHUNKS * net.size + i * tall, tall), tall)
            rows = rows_ref[at, :]
            query = dot_nt(rows, w_ref[0]) + bias_ref[0:1, :].astype(F32)
            q_ref[at, :] = (query.astype(BF).astype(F32) * 0.125).astype(BF)
            k_ref[at, :] = dot_nt(rows, w_ref[1]).astype(BF)
            v_ref[at, :] = (dot_nt(rows, w_ref[2]) + bias_ref[1:2, :].astype(F32)).astype(BF)

        loop(CHUNKS // 2, part)

    def attend(seq, index):
        attend_block(q_ref, k_ref, v_ref, table_ref, ids_ref, cols_ref, ctx_ref, lse_ref, seq, index)

    project(net.me)
    loop(CHUNKS, net.wait_partner)
    project(net.partner)
    moves.wait(0)
    mine = net.me // 2
    steps = length // BLOCK

    def near(i):
        attend(mine, i)
        net.relay(i)
        top.send_own(i)

    loop(steps, near)
    project(net.cross)
    loop(CHUNKS, net.wait_diag)
    project(net.diag)
    moves.start(1, 3, 4, 5)

    def far(i):
        attend(1 - mine, i)
        top.relay(i)
        net.drain(i)

    loop(steps, far)
    for wait in (top.wait_partner, top.wait_diag):
        loop(CHUNKS, wait)
    moves.start(2)
    loop(CHUNKS, top.drain)
    moves.wait(1, 2, 3, 4, 5)


def front(patches, params, weight, bias, cotangent, ids, table):
    rows, width = patches.shape
    cols = weight.shape[1]
    one, wide = ((4 * rows, cols), BF), ((4 * rows, width), BF)
    return call(
        front_kernel, "front", 1, [one, ((4 * rows, 128), F32), wide, wide, one, one, one],
        [pltpu.VMEM(table.shape, BF), pltpu.VMEM((4 * rows, 128), F32)]
        + [pltpu.VMEM(*shape) for shape in (wide, wide, one, one, one)]
        + [pltpu.SemaphoreType.DMA((6,))] + moves() + moves(),
        patches, some(params, ATTN_GAIN, ATTN_SHIFT, MLP_SCALE), weight, bias, cotangent, ids, table, far=1, far_out=5,
    )


def project_kernel(
    ctx_ref, w_ref, x_ref, par_ref, attn_ref, mid_ref, norm_ref, out, inn, send, recv
):
    net = Scatter(out, inn, send, recv)
    greet_mp()

    def share(block, chunk):
        at = pl.ds(pl.multiple_of((block * CHUNKS + chunk) * net.size, net.size), net.size)
        return dot(ctx_ref[at, :], w_ref[...])

    loop(CHUNKS, lambda c: net.put(0, c, share(net.diag, c)))
    loop(CHUNKS, lambda c: net.put(1, c, share(net.cross, c) + net.take(0, c)))
    loop(CHUNKS, lambda c: net.put(2, c, share(net.partner, c)))

    def own(chunk):
        attn_ref[net.rows(chunk), :] = share(net.me, chunk) + net.take(2, chunk) + row(par_ref, PROJ_BIAS)

    loop(CHUNKS, own)

    def last(chunk):
        at = net.rows(chunk)
        attn = attn_ref[at, :] + net.take(1, chunk)
        middle = x_ref[at, :].astype(F32) + row(par_ref, ATTN_SCALE) * attn
        attn_ref[at, :] = attn
        mid_ref[at, :] = middle
        norm_ref[at, :] = norm_rows(middle, row(par_ref, MLP_GAIN), row(par_ref, MLP_SHIFT))[0].astype(BF)

    loop(CHUNKS, last)
    loop(CHUNKS, net.drain)


def project(context, weight, patches, params):
    rows, width = patches.shape
    return call(
        project_kernel, "project", 2, [((rows, width), F32), ((rows, width), F32), ((rows, width), BF)],
        halves(rows, width), context, weight, patches, some(params, PROJ_BIAS, ATTN_SCALE, MLP_GAIN, MLP_SHIFT),
    )


def gelu_both(u):
    inner = 0.7978845608028654 * (u + 0.044715 * (u * u * u))
    t = jnp.tanh(inner)
    half = 0.5 * (1.0 + t)
    slope = half + (0.5 * u) * (1.0 - t * t) * (0.7978845608028654 * (1.0 + 0.134145 * (u * u)))
    return u * half, slope


def mlp_kernel(
    norm_ref, par_ref, up_hbm, down_hbm, grad_hbm, mid_hbm, attn_hbm, cot_hbm,
    gmid_ref, gattn_ref, sums_ref, cross_hbm, here_hbm, upg_hbm, downg_hbm,
    up_ref, down_ref, grad_ref, mid_ref, attn_ref, cot_ref, cross_ref, here_ref, upg_ref, downg_ref, load,
    rows_ref, hid_ref, pre_ref, own_ref, far_ref, mfar_ref, gsend, grecv, out, inn, send, recv,
    mout, minn, msend, mrecv,
):
    gat = Gather(rows_ref, gsend, grecv)
    net = Scatter(out, inn, send, recv)
    top = Scatter(mout, minn, msend, mrecv)
    size = gat.size
    moves = Moves(
        load,
        (
            (up_hbm, up_ref), (down_hbm, down_ref), (grad_hbm, grad_ref), (mid_hbm, mid_ref), (attn_hbm, attn_ref),
            (cot_hbm, cot_ref), (cross_ref, cross_hbm), (here_ref, here_hbm), (upg_ref, upg_hbm), (downg_ref, downg_hbm),
        ),
    )
    moves.start(0, 1, 2, 3, 4, 5)
    greet_mp()
    sums_ref[...] = jnp.zeros_like(sums_ref)

    def own(chunk):
        rows_ref[gat.rows(gat.me, chunk), :] = norm_ref[net.rows(chunk), :]
        gat.send_own(chunk)

    loop(CHUNKS, own)

    moves.wait(0, 1, 2)

    def two(first, second, chunk):
        at, by = gat.rows(first, chunk), gat.rows(second, chunk)
        both = lambda ref: jnp.concatenate([ref[at, :], ref[by, :]], axis=0)
        value, slope = gelu_both(dot(both(rows_ref), up_ref[...]) + row(par_ref, UP_BIAS))
        hidden = value.astype(BF)
        hid_ref[at, :], hid_ref[by, :] = hidden[:size], hidden[size:]
        grad_pre = (dot_nt(both(grad_ref), down_ref[...]) * slope).astype(BF)
        pre_ref[at, :], pre_ref[by, :] = grad_pre[:size], grad_pre[size:]
        sums_ref[0:1, :] += jnp.sum(grad_pre.astype(F32), axis=0, keepdims=True)
        back = dot_nt(grad_pre, up_ref[...])
        part = dot(hidden, down_ref[...])
        return back[:size], back[size:], part[:size], part[size:]

    def near(chunk):
        gat.wait_partner(chunk)
        theirs, mine, share, kept = two(gat.partner, gat.me, chunk)
        net.put(2, chunk, theirs)
        top.put(2, chunk, share)
        own_ref[net.rows(chunk), :] = mine
        here_ref[net.rows(chunk), :] = kept

    loop(CHUNKS, near)

    def across(chunk):
        net.put(1, chunk, far_ref[net.rows(chunk), :] + net.take(0, chunk))

    def far(chunk):
        gat.relay(chunk)
        gat.wait_diag(chunk)
        theirs, mine, share, kept = two(gat.diag, gat.cross, chunk)
        net.put(0, chunk, theirs)
        top.put(0, chunk, share)
        far_ref[net.rows(chunk), :] = mine
        mfar_ref[net.rows(chunk), :] = kept

        @pl.when(chunk > 0)
        def _():
            across(chunk - 1)

    loop(CHUNKS, far)
    across(CHUNKS - 1)

    def weights(i):
        pack(upg_ref, i, dot_tn(rows_ref[:, half_of(rows_ref, i)], pre_ref[...]))
        pack(downg_ref, i, dot_tn(grad_ref[:, half_of(grad_ref, i)], hid_ref[...]))

    loop(2, weights)

    def outs(chunk):
        at = net.rows(chunk)
        here_ref[at, :] += top.take(2, chunk)
        cross_ref[at, :] = (mfar_ref[at, :] + top.take(0, chunk)).astype(BF)

    loop(CHUNKS, outs)
    moves.start(6, 7, 8, 9)
    moves.wait(3, 4, 5)

    def last(chunk):
        at = net.rows(chunk)
        grad = own_ref[at, :] + net.take(2, chunk) + net.take(1, chunk)
        normed, inv = norm_rows(mid_ref[at, :], 1.0, 0.0)[1:]
        back, gain_sum, shift_sum = norm_back(grad, normed, inv, row(par_ref, MLP_GAIN))
        middle = cot_ref[at, :].astype(F32) + back
        gattn = (middle * row(par_ref, ATTN_SCALE)).astype(BF)
        gmid_ref[at, :] = middle
        gattn_ref[at, :] = gattn
        sums_ref[1:2, :] += gain_sum[None]
        sums_ref[2:3, :] += shift_sum[None]
        sums_ref[3:4, :] += jnp.sum(middle * attn_ref[at, :], axis=0, keepdims=True)
        sums_ref[4:5, :] += jnp.sum(gattn.astype(F32), axis=0, keepdims=True)

    loop(CHUNKS, last)
    loop(CHUNKS, gat.drain)
    loop(CHUNKS, net.drain)
    loop(CHUNKS, lambda chunk: top.drain(chunk, (0, 2)))
    moves.wait(6, 7, 8, 9)


def mlp(normed, params, up, down, grad_rows, middle, attn, cotangent):
    rows, width = normed.shape
    ff = up.shape[1]
    one = pltpu.VMEM((rows, width), F32)
    packed = ((SLOTS, width // SLOTS, ff), BF)
    late = [((rows, width), BF), ((rows, width), F32), packed, packed]
    return call(
        mlp_kernel, "mlp", 3,
        [((rows, width), F32), ((rows, width), BF), ((8, width), F32)] + late,
        like(up, down, grad_rows, middle, attn, cotangent) + [pltpu.VMEM(*shape) for shape in late]
        + [pltpu.SemaphoreType.DMA((10,))]
        + [pltpu.VMEM((4 * rows, width), BF), pltpu.VMEM((4 * rows, ff), BF), pltpu.VMEM((4 * rows, ff), BF), one, one, one]
        + moves() + halves(rows, width) + halves(rows, width),
        normed, some(params, UP_BIAS, MLP_GAIN, ATTN_SCALE), up, down, grad_rows, middle, attn, cotangent, far=6, far_out=4,
    )


class Fold:
    def __init__(self, src, inn, send, recv, order=(0, 1, 2)):
        self.src, self.inn, self.send, self.recv = src, inn, send, recv
        self.size = src.shape[1] // PARTS
        place = lax.axis_index("dp")
        bits = (lax.rem(place, 2), lax.rem(place // 2, 2), place // 4)
        a, b, c = [bits[i] for i in order]
        self.peers = [place + (1 << i) - (2 << i) * bits[i] for i in order]
        self.theirs = (4 * (1 - a), 2 * (1 - b), 4 + 1 - c)
        self.mine = (4 * a, 2 * b, 4 + c)

    def copy(self, stage, part):
        count, offset = (4, 2, 1)[stage], (0, 4, 6)[stage]
        rows = pl.ds(part * self.size, self.size)
        src = self.src if stage == 0 else self.inn
        return pltpu.make_async_remote_copy(
            src_ref=src.at[pl.ds(self.theirs[stage], count), rows, :],
            dst_ref=self.inn.at[pl.ds(offset, count), rows, :],
            send_sem=self.send.at[stage, part], recv_sem=self.recv.at[stage, part],
            device_id={"dp": self.peers[stage]}, device_id_type=MESH,
        )

    def start(self):
        for part in range(PARTS):
            self.copy(0, part).start()

    def advance(self, stage):
        count, offset = (4, 2)[stage], (0, 4)[stage]
        src = self.src if stage == 0 else self.inn
        for part in range(PARTS):
            rows = pl.ds(part * self.size, self.size)
            self.copy(stage, part).wait_recv()
            for i in range(count):
                self.inn[offset + i, rows, :] = self.inn[offset + i, rows, :] + src[self.mine[stage] + i, rows, :]
            self.copy(stage + 1, part).start()

    def finish(self, put):
        for part in range(PARTS):
            rows = pl.ds(part * self.size, self.size)
            self.copy(2, part).wait_recv()
            put(rows, self.inn[self.mine[2], rows, :].astype(F32) + self.inn[6, rows, :].astype(F32))

    def drain(self):
        for stage in range(3):
            for part in range(PARTS):
                self.copy(stage, part).wait_send()


class Total:
    def __init__(self, acc, inn, send, recv):
        self.acc, self.inn, self.send, self.recv = acc, inn, send, recv
        place = lax.axis_index("dp")
        x, lo, hi = lax.rem(place, 2), lax.rem(place // 2, 2), place // 4
        _, partner, cross, _ = neighbours()
        self.peers = (
            {"mp": partner}, {"mp": cross}, {"dp": place + 1 - 2 * x}, {"dp": place + 2 - 4 * lo}, {"dp": place + 4 - 8 * hi},
        )

    def copy(self, stage):
        return pltpu.make_async_remote_copy(
            src_ref=self.acc.at[stage], dst_ref=self.inn.at[stage], send_sem=self.send.at[stage],
            recv_sem=self.recv.at[stage], device_id=self.peers[stage], device_id_type=MESH,
        )

    def start(self, stage):
        self.copy(stage).start()

    def finish(self, stage):
        self.copy(stage).wait_recv()
        self.acc[stage + 1] = self.acc[stage] + self.inn[stage]
        if stage == 1:
            self.acc[2, 8:16, :] = self.acc[0, 8:16, :]

    def drain(self):
        for stage in range(5):
            self.copy(stage).wait_send()


def back_kernel(
    fold,
    pw_ref, ids_ref, par_ref, two_ref, rows_hbm, table_hbm, *refs,
):
    early, refs = refs[:EARLY], refs[EARLY:]
    if fold:
        layer_ref, grad_ref, tab_ref, upo_ref, downo_ref, mixo_ref, sums_ref, *refs = refs
        band_ref, mix_ref, acc_ref, *refs = refs
        winn, wsend, wrecv, tinn, tsend, trecv, ainn, asend, arecv, *refs = refs
    else:
        layer_ref, grad_ref, band_ref, mix_ref, sums_ref, *refs = refs
        acc_ref = None
    held, refs = refs[: EARLY - 1], refs[EARLY - 1 :]
    upg_ref, downg_ref, q_ref, k_ref, v_ref, lse_ref, cross_ref, ctx_ref, w_ref, here_ref, mid_ref, cot_ref, x_ref, gmid_ref = held
    (
        table_ref, cols_ref, rowsg_ref, g_ref, qt_ref, gt_ref, dkt_ref, dvt_ref, strip_ref, dq_ref, dv_ref,
        far_ref, load, hold, fsend, frecv, gsend, grecv, out, inn, send, recv,
    ) = refs
    dk_ref = g_ref
    own_ref = grad_ref
    gat = Gather(rowsg_ref, gsend, grecv)
    net = Scatter(out, inn, send, recv)
    seqs, length = ids_ref.shape
    rows_all, cols = q_ref.shape
    blocks = length // BLOCK
    heads = cols // HEAD_DIM
    small_ref = acc_ref.at[0] if fold else sums_ref
    me, partner, cross, _ = neighbours()
    whole = CHUNKS * gat.size
    mine_at = pl.ds(pl.multiple_of(me * whole, whole), whole)
    moves = Moves(hold, [(early[0], rowsg_ref.at[mine_at, :])] + list(zip(early[1:], held)))
    moves.start(*range(7))

    def fetch(head):
        at = pl.ds(pl.multiple_of(lax.rem(head, 2) * length, length), length)
        return pltpu.make_async_copy(table_hbm.at[head], table_ref.at[at, :], load.at[1 + head])

    fetch(0).start()
    fetch(1).start()
    moves.start(*range(7, EARLY))
    far = pltpu.make_async_remote_copy(
        src_ref=cross_ref, dst_ref=far_ref, send_sem=fsend, recv_sem=frecv, device_id={"mp": cross}, device_id_type=MESH
    )
    if fold:
        up = Fold(upg_ref, winn.at[0], wsend.at[0], wrecv.at[0])
        down = Fold(downg_ref, winn.at[1], wsend.at[1], wrecv.at[1])
        mix = Fold(mix_ref, winn.at[2], wsend.at[2], wrecv.at[2], MIX_ORDER)
        tab = lambda head: Fold(band_ref.at[head], tinn.at[head], tsend.at[head], trecv.at[head])
        small = Total(acc_ref, ainn, asend, arecv)
        greet(({"mp": partner}, {"mp": cross}) + tuple({"dp": peer} for peer in up.peers))
    else:
        greet_mp()

    moves.wait(0)
    loop(CHUNKS, gat.send_own)
    moves.wait(1, 2)
    if fold:
        up.start()
        down.start()
    id_columns(ids_ref, cols_ref, seqs, length)

    def block(number):
        at = pl.ds(pl.multiple_of(number * whole, whole), whole)
        g_ref[at, :] = dot_nt(rowsg_ref[at, :], pw_ref[...]).astype(BF)

    def tall(i):
        return pl.ds(pl.multiple_of(i * BLOCK, BLOCK), BLOCK)

    def flip_q(i):
        qt_ref[:, tall(i)] = q_ref[tall(i), :].T

    def flip_g(i):
        gt_ref[:, tall(i)] = g_ref[tall(i), :].T

    per = rows_all // BLOCK // seqs
    near_seq = gat.me // 2
    block(gat.me)
    dkt_ref[...] = jnp.zeros_like(dkt_ref)
    dvt_ref[...] = jnp.zeros_like(dvt_ref)
    dq_ref[...] = jnp.zeros_like(dq_ref)
    small_ref[...] = jnp.zeros_like(small_ref)
    if fold:
        tab_ref[...] = jnp.zeros_like(tab_ref)
    moves.wait(3, 4, 5, 6)
    loop(rows_all // BLOCK, flip_q)
    loop(CHUNKS, gat.wait_partner)
    block(gat.partner)
    loop(per, lambda i: flip_g(near_seq * per + i))
    lane = lax.broadcasted_iota(jnp.int32, (1, 128), 1)

    def step(head, index, seq, first):
        start, width = window(index, length)
        mine = head_lanes(head, cols)
        feats = pl.ds(pl.multiple_of(head * HEAD_DIM, HEAD_DIM), HEAD_DIM)
        rows = tall(seq * blocks + index)
        keys_at = pl.ds(pl.multiple_of(seq * length + start, 128), width)
        keys = k_ref[keys_at, :]
        same = cols_ref[rows, 0:1] == ids_ref[pl.ds(seq, 1), pl.ds(start, width)]
        sums = jnp.sum(jnp.where(lane == head, lse_ref[rows, :], 0.0), axis=-1, keepdims=True)
        bias = table_ref[tall(lax.rem(head, 2) * blocks + index), pl.ds(start, width)].astype(F32)
        scores = dot_nt(jnp.where(mine, q_ref[rows, :], 0), keys) + bias
        probs = jnp.where(same, jnp.exp(scores - sums), 0.0)
        grad_probs = dot_nt(jnp.where(mine, g_ref[rows, :], 0), v_ref[keys_at, :])
        centre = jnp.sum(grad_probs * probs, axis=-1, keepdims=True)
        grad_scores = (probs * (grad_probs - centre)).astype(BF)
        strip_ref[:, 0:width] = grad_scores
        dvt_ref[feats, keys_at] += dot(gt_ref[feats, rows], probs.astype(BF))
        dkt_ref[feats, keys_at] += dot(qt_ref[feats, rows], grad_scores)
        grad_q = (dot(grad_scores, keys) * 0.125).astype(BF)
        dq_ref[rows, :] = jnp.where(mine, grad_q, dq_ref[rows, :])
        for part in range(BLOCK // GROUP):
            group = index * (BLOCK // GROUP) + part
            tiles = []
            for t in range(TILES + 1):
                block = group - TILES // 2 + t
                there = (block >= 0) & (block < length // GROUP)
                offset = jnp.clip(block * GROUP - start, 0, width - GROUP)
                tile = strip_ref[part * GROUP : (part + 1) * GROUP, pl.ds(pl.multiple_of(offset, GROUP), GROUP)]
                tiles.append(jnp.where(there, tile, 0))
            tiles[0] += tiles.pop()
            value = jnp.concatenate(tiles, axis=1)
            slot = slot_of(group)
            if not first:
                value = (value.astype(F32) + band_ref[head, slot, :, :].astype(F32)).astype(BF)
            band_ref[head, slot, :, :] = value

    def one_head(head, seq, first):
        fetch(head).wait()

        def inner(index):
            step(head, index, seq, first)
            if first:
                i = head * blocks + index

                @pl.when(lax.rem(i, heads) == heads - 1)
                def _():
                    gat.relay(i // heads)

        loop(blocks, inner)

        @pl.when(head + 2 < heads)
        def _():
            fetch(head + 2).start()

    def near_head(head):
        one_head(head, near_seq, True)

    def far_head(head):
        one_head(head, 1 - near_seq, False)
        if fold:
            tab(head).start()

            @pl.when(head == 0)
            def _():
                down.advance(0)
                up.advance(1)

            @pl.when(head == 1)
            def _():
                down.advance(1)

    loop(heads, near_head)
    fetch(0).start()
    fetch(1).start()
    block(gat.cross)
    loop(CHUNKS, gat.wait_diag)
    block(gat.diag)
    moves.wait(7)
    far.start()
    loop(per, lambda i: flip_g((1 - near_seq) * per + i))
    if fold:
        up.advance(0)
    loop(heads, far_head)
    moves.wait(*range(8, EARLY))
    rows_ref = table_ref.at[:, 0 : rowsg_ref.shape[1]]
    again = pltpu.make_async_copy(rows_hbm, rows_ref, load.at[0])
    again.start()

    def unflip(i):
        dk_ref[tall(i), :] = dkt_ref[:, tall(i)].T.astype(BF)
        dv_ref[tall(i), :] = dvt_ref[:, tall(i)].T.astype(BF)

    loop(rows_all // BLOCK, unflip)

    again.wait()

    order = MIX_ORDER if fold else (0, 1, 2)

    def weights(i):
        rows = table_ref[:, half_of(rowsg_ref, i)]
        for number, ref in enumerate((dq_ref, dk_ref, dv_ref)):
            pack(mix_ref, i, dot_tn(rows, ref[...]), number * cols, order)
        pack(mix_ref, i, dot_tn(rowsg_ref[:, half_of(rowsg_ref, i)], ctx_ref[...]), 3 * cols, order)

    loop(2, weights)

    def put_table(head):
        def put(rows, value):
            group = lax.axis_index("dp")
            left, right = edge(rows.start, rows.size)
            for t in range(TILES + 1):
                tile = value[:, t % TILES * GROUP : (t % TILES + 1) * GROUP]
                if t % TILES == 0:
                    tile = jnp.where(right if t else left, tile, 0.0)
                block = group - TILES // 2 + t

                @pl.when((block >= 0) & (block < length // GROUP))
                def _():
                    tab_ref[head, rows, pl.ds(pl.multiple_of(block * GROUP, GROUP), GROUP)] = tile
        return put

    def put_to(ref):
        def put(rows, value):
            ref[rows, :] = value
        return put

    if fold:
        mix.start()

    def share(number, chunk):
        at = gat.rows(number, chunk)
        return dot(dq_ref[at, :], w_ref[0]) + dot(dk_ref[at, :], w_ref[1]) + dot(dv_ref[at, :], w_ref[2])

    loop(CHUNKS, lambda c: net.put(0, c, share(net.diag, c)))
    loop(CHUNKS, lambda c: net.put(1, c, share(net.cross, c) + net.take(0, c)))
    loop(CHUNKS, lambda c: net.put(2, c, share(net.partner, c)))

    def keep(chunk):
        own_ref[net.rows(chunk), :] = share(net.me, chunk) + net.take(2, chunk)

    loop(CHUNKS, keep)
    if fold:
        tab(0).advance(0)
        up.finish(put_to(upo_ref))
        down.finish(put_to(downo_ref))
    far.wait_recv()

    def layer(chunk):
        at = net.rows(chunk)
        mlp_out = here_ref[at, :] + far_ref[at, :].astype(F32) + row(par_ref, DOWN_BIAS)
        layer_ref[at, :] = (mid_ref[at, :] + row(par_ref, MLP_SCALE) * mlp_out).astype(BF)
        top = cot_ref[at, :].astype(F32)
        small_ref[7:8, :] += jnp.sum(top * mlp_out, axis=0, keepdims=True)
        low = (top * row(par_ref, MLP_SCALE)).astype(BF).astype(F32)
        small_ref[6:7, :] += jnp.sum(low, axis=0, keepdims=True)

    loop(CHUNKS, layer)
    for put, source in ((2, 4), (3, 3), (4, 1), (5, 2), (8, 0)):
        small_ref[put : put + 1, :] = two_ref[source : source + 1, :]
    small_ref[9:10, 0:cols] = jnp.sum(dq_ref[...].astype(F32), axis=0, keepdims=True)
    small_ref[10:11, 0:cols] = jnp.sum(dv_ref[...].astype(F32), axis=0, keepdims=True)
    if fold:
        tab(0).advance(1)
        tab(1).advance(0)

    def last(chunk):
        at = net.rows(chunk)
        grad = own_ref[at, :] + net.take(1, chunk)
        normed, inv = norm_rows(x_ref[at, :].astype(F32), 1.0, 0.0)[1:]
        back, gain_sum, shift_sum = norm_back(grad, normed, inv, row(par_ref, ATTN_GAIN))
        grad_ref[at, :] = gmid_ref[at, :] + back
        small_ref[0:1, :] += gain_sum[None]
        small_ref[1:2, :] += shift_sum[None]

    loop(CHUNKS, last)
    if fold:
        small.start(0)
        tab(0).finish(put_table(0))
        tab(1).advance(1)
        small.finish(0)
        small.start(1)
        tab(2).advance(0)
        small.finish(1)
        small.start(2)
        tab(1).finish(put_table(1))
        small.finish(2)
        small.start(3)
        tab(2).advance(1)
        mix.advance(0)
        small.finish(3)
        small.start(4)
        mix.advance(1)
        mix.finish(put_to(mixo_ref))
        tab(2).finish(put_table(2))
        small.finish(4)
        sums_ref[...] = acc_ref[5]
        for piece in (up, down, mix, tab(0), tab(1), tab(2), small):
            piece.drain()
    far.wait_send()
    loop(CHUNKS, gat.drain)
    loop(CHUNKS, net.drain)


def back(fold, length, proj, ids, params, two, rows_one, table, *early):
    rows, width = early[0].shape
    cols = proj.shape[0]
    heads = cols // HEAD_DIM
    piece, wide = width // SLOTS, TILES * GROUP
    strip = min(length, BLOCK + 2 * PAGE_MOST)
    band, mix = ((heads, SLOTS, GROUP, wide), BF), ((SLOTS, piece, width), BF)
    outs = [((rows, width), BF), ((rows, width), F32)]
    scratch = []
    if fold:
        sem = pltpu.SemaphoreType.DMA((3, 3, PARTS))
        outs += [((heads, GROUP, length), F32)] + [((piece, width), F32)] * 3
        scratch += [pltpu.VMEM(*band), pltpu.VMEM(*mix), pltpu.VMEM((6, 16, width), F32)]
        scratch += [pltpu.VMEM((3, 7, piece, width), BF), sem, sem, pltpu.VMEM((heads, 7, GROUP, wide), BF), sem, sem]
        scratch += [pltpu.VMEM((5, 16, width), F32), pltpu.SemaphoreType.DMA((5,)), pltpu.SemaphoreType.DMA((5,))]
    else:
        outs += [band, mix]
    outs += [((16, width), F32)]
    one, flat = pltpu.VMEM((4 * rows, cols), BF), pltpu.VMEM((cols, 4 * rows), BF)
    total = pltpu.VMEM((cols, 4 * rows), F32)
    scratch += like(*early[1:]) + [
        pltpu.VMEM((2 * length, length), BF), pltpu.VMEM((4 * rows, 128), F32), pltpu.VMEM((4 * rows, width), BF), one,
        flat, flat, total, total, pltpu.VMEM((BLOCK, strip), BF), one, one, pltpu.VMEM((rows, width), BF),
        pltpu.SemaphoreType.DMA((1 + heads,)), pltpu.SemaphoreType.DMA((EARLY,)),
        pltpu.SemaphoreType.DMA, pltpu.SemaphoreType.DMA,
    ] + moves() + halves(rows, width)
    params = some(params, DOWN_BIAS, MLP_SCALE, ATTN_GAIN)
    return call(
        partial(back_kernel, fold), "back", 4, outs, scratch, proj, ids, params, two, rows_one, table, *early, far=2 + EARLY
    )


def scatter_dp(x):
    return lax.psum_scatter(x, "dp", scatter_dimension=0, tiled=True).astype(F32)


def in_order(packed):
    _, rows, cols = packed.shape
    return packed.reshape(2, 2, 2, rows, cols).transpose(2, 1, 0, 3, 4).reshape(SLOTS * rows, cols)


def reduce_table(band, length, n_dp):
    groups, heads, _, wide = band.shape
    shard = length // n_dp
    send = band.reshape(groups, heads, GROUP // shard, shard, wide).swapaxes(1, 2)
    part = scatter_dp(send.reshape(n_dp * heads * shard, wide)).reshape(heads, shard, wide)
    place = lax.axis_index("dp") * shard
    return unfold(part, place // GROUP, place % GROUP, length)


def unfold(part, group, first_row, length):
    heads, shard, _ = part.shape
    left, right = edge(first_row, shard)
    end = part[:, :, :GROUP]
    band = jnp.concatenate([jnp.where(left, end, 0.0), part[:, :, GROUP:], jnp.where(right, end, 0.0)], axis=2)
    full = jnp.zeros((heads, shard, length + 2 * PAGE_MOST), F32)
    full = lax.dynamic_update_slice(full, band, (0, 0, group * GROUP))
    return full[:, :, PAGE_MOST : PAGE_MOST + length]


def local(
    patches, segment_ids, fill_counts, attn_gain, attn_shift, qkv_weight, qv_bias, rel_table, proj_weight,
    proj_bias, attn_scale, mlp_gain, mlp_shift, up_weight, up_bias, down_weight, down_bias, mlp_scale, cotangent,
):
    n_dp = lax.axis_size("dp")
    seqs, length = segment_ids.shape
    cols = qkv_weight.shape[2]
    places = jnp.arange(length, dtype=jnp.int32)[None]
    ids = jnp.where(places < fill_counts[:, None], segment_ids, -1 - places).astype(F32)
    fold = n_dp == SLOTS and length == SLOTS * GROUP
    vectors = (attn_gain, attn_shift, proj_bias, attn_scale, mlp_gain, mlp_shift, up_bias, down_bias, mlp_scale)
    params = dict(enumerate(vectors))
    turned = qkv_weight.swapaxes(1, 2)
    context, lse, rows_one, grad_rows, queries, keys, values = front(
        patches, params, turned, qv_bias, cotangent, ids, rel_table
    )
    attn_out, middle, normed_two = project(context, proj_weight, patches, params)
    grad_middle, grad_attn, sums_two, cross, here, up_local, down_local = mlp(
        normed_two, params, up_weight, down_weight, grad_rows, middle, attn_out, cotangent
    )
    layer_out, patch_grad, *more, sums = back(
        fold, length, proj_weight, ids, params, sums_two, rows_one, rel_table,
        grad_attn, up_local, down_local, queries, keys, values, lse, cross, context, turned, here, middle, cotangent,
        patches, grad_middle,
    )
    if fold:
        table_grad, up_grad, down_grad, mixed = more
    else:
        band, mixed = more
        order = [4 * (d % 2) + 2 * (d // 2 % 2) + d // 4 for d in range(SLOTS)]
        table_grad = reduce_table(jnp.stack([band[:, slot] for slot in order]), length, n_dp)
        up_grad, down_grad, mixed = [scatter_dp(in_order(piece)) for piece in (up_local, down_local, mixed)]
        sums = jnp.concatenate([lax.psum(sums[:8], ("dp", "mp")), lax.psum(sums[8:], "dp")])
    qkv_grad = mixed[:, : 3 * cols].reshape(-1, 3, cols).swapaxes(0, 1)
    return (
        layer_out, patch_grad, sums[0], sums[1], qkv_grad, sums[9:11, :cols], table_grad, mixed[:, 3 * cols :].T,
        sums[2], sums[3], sums[4], sums[5], up_grad, sums[8], down_grad.T, sums[6], sums[7],
    )


def solution(mesh):
    rows, split = P(("dp", "mp"), None), P("mp", None)
    placed = (
        rows, P("dp", None), P("dp"), P(), P(), P(None, None, "mp"), P(None, "mp"), P("mp", None, None), split,
        P(), P(), P(), P(), P(None, "mp"), P("mp"), split, P(), P(), rows,
    )
    given = (
        rows, rows, P(), P(), P(None, "dp", "mp"), P(None, "mp"), P("mp", "dp", None), P("mp", "dp"), P(), P(),
        P(), P(), P("dp", "mp"), P("mp"), P("mp", "dp"), P(), P(),
    )
    return jax.shard_map(local, mesh=mesh, in_specs=placed, out_specs=given, check_vma=False)
```

```python
from functools import partial

import jax
import jax.numpy as jnp
from jax import lax
from jax.experimental import pallas as pl
from jax.experimental.pallas import tpu as pltpu
from jax.sharding import PartitionSpec as P

HEAD_DIM = 64
BLOCK = 256
GROUP = 128

ATTN_GAIN, ATTN_SHIFT, PROJ_BIAS, ATTN_SCALE, MLP_GAIN, MLP_SHIFT, UP_BIAS, DOWN_BIAS, MLP_SCALE = range(9)
CHUNKS = 4
SLOTS = 8
PARTS = 2
EARLY = 15
MIX_ORDER = (0, 1, 2)
PAGE_MOST = 256
TILES = 2 * PAGE_MOST // GROUP
BF = jnp.bfloat16
F32 = jnp.float32
MESH = pl.DeviceIdType.MESH
VMEM_MOST = 61 * 1024 * 1024
NT = (((1,), (1,)), ((), ()))
TN = (((0,), (0,)), ((), ()))


def vmem():
    return pl.BlockSpec(memory_space=pltpu.VMEM)


def dot(a, b):
    return jnp.dot(a, b, preferred_element_type=F32)


def dot_nt(a, b):
    return lax.dot_general(a, b, NT, preferred_element_type=F32)


def dot_tn(a, b):
    return lax.dot_general(a, b, TN, preferred_element_type=F32)


def norm_rows(rows, gain, shift):
    centre = rows - jnp.mean(rows, axis=-1, keepdims=True)
    inv_std = lax.rsqrt(jnp.mean(centre * centre, axis=-1, keepdims=True) + 1e-06)
    normed = centre * inv_std
    return (normed * gain + shift, normed, inv_std)


def norm_back(grad_out, normed, inv_std, gain):
    scaled = grad_out * gain
    inner = (
        scaled
        - jnp.mean(scaled, axis=-1, keepdims=True)
        - normed * jnp.mean(scaled * normed, axis=-1, keepdims=True)
    )
    return (inv_std * inner, jnp.sum(grad_out * normed, axis=0), jnp.sum(grad_out, axis=0))


def window(index, length):
    width = min(length, BLOCK + 2 * PAGE_MOST)
    start = jnp.clip(index * BLOCK - PAGE_MOST, 0, length - width)
    return pl.multiple_of(start, 128), width


def edge(first_row, rows):
    place = lax.broadcasted_iota(jnp.int32, (rows, GROUP), 0) + first_row
    column = lax.broadcasted_iota(jnp.int32, (rows, GROUP), 1)
    return column > place, column < place


def head_lanes(head, cols):
    return lax.broadcasted_iota(jnp.int32, (1, cols), 1) // HEAD_DIM == head


def id_columns(ids_ref, cols_ref, seqs, length):
    for s in range(seqs):
        wide = jnp.broadcast_to(ids_ref[s : s + 1, :], (128, length))
        cols_ref[s * length : (s + 1) * length, :] = wide.T


def loop(count, body):
    lax.fori_loop(0, count, lambda i, _: (body(i), 0)[1], 0)


def neighbours():
    me = lax.axis_index("mp")
    partner = me + 1 - 2 * lax.rem(me, 2)
    return me, partner, lax.rem(me + 2, 4), lax.rem(partner + 2, 4)


def greet(peers):
    barrier = pltpu.get_barrier_semaphore()
    for peer in peers:
        pl.semaphore_signal(barrier, inc=1, device_id=peer, device_id_type=MESH)
    pl.semaphore_wait(barrier, len(peers))


def greet_mp():
    _, partner, cross, _ = neighbours()
    greet(({"mp": partner}, {"mp": cross}))


class Gather:
    def __init__(self, buffer, send, recv):
        self.buffer, self.send, self.recv = buffer, send, recv
        self.size = buffer.shape[0] // 4 // CHUNKS
        self.me, self.partner, self.cross, self.diag = neighbours()

    def rows(self, block, chunk):
        return pl.ds(pl.multiple_of((block * CHUNKS + chunk) * self.size, self.size), self.size)

    def copy(self, kind, block, chunk):
        part = self.buffer.at[self.rows(block, chunk), :]
        return pltpu.make_async_remote_copy(
            src_ref=part, dst_ref=part, send_sem=self.send.at[kind, chunk], recv_sem=self.recv.at[kind, chunk],
            device_id={"mp": self.cross if kind == 0 else self.partner}, device_id_type=MESH,
        )

    def send_own(self, chunk):
        self.copy(0, self.me, chunk).start()
        self.copy(1, self.me, chunk).start()

    def wait_partner(self, chunk):
        self.copy(1, self.partner, chunk).wait_recv()

    def relay(self, chunk):
        self.copy(0, self.cross, chunk).wait_recv()
        self.copy(2, self.cross, chunk).start()

    def wait_diag(self, chunk):
        self.copy(2, self.diag, chunk).wait_recv()

    def drain(self, chunk):
        self.copy(0, self.me, chunk).wait_send()
        self.copy(1, self.me, chunk).wait_send()
        self.copy(2, self.cross, chunk).wait_send()


class Scatter:
    def __init__(self, out, inn, send, recv):
        self.out, self.inn, self.send, self.recv = out, inn, send, recv
        self.size = out.shape[1] // CHUNKS
        self.me, self.partner, self.cross, self.diag = neighbours()

    def rows(self, chunk):
        return pl.ds(pl.multiple_of(chunk * self.size, self.size), self.size)

    def copy(self, kind, chunk):
        return pltpu.make_async_remote_copy(
            src_ref=self.out.at[kind, self.rows(chunk), :], dst_ref=self.inn.at[kind, self.rows(chunk), :],
            send_sem=self.send.at[kind, chunk], recv_sem=self.recv.at[kind, chunk],
            device_id={"mp": self.cross if kind == 1 else self.partner}, device_id_type=MESH,
        )

    def put(self, kind, chunk, value):
        self.out[kind, self.rows(chunk), :] = value.astype(BF)
        self.copy(kind, chunk).start()

    def take(self, kind, chunk):
        self.copy(kind, chunk).wait_recv()
        return self.inn[kind, self.rows(chunk), :].astype(F32)

    def drain(self, chunk, kinds=(0, 1, 2)):
        for kind in kinds:
            self.copy(kind, chunk).wait_send()


def slot_of(place):
    return 4 * lax.rem(place, 2) + 2 * lax.rem(place // 2, 2) + place // 4


def half_of(ref, i):
    size = ref.shape[1] // 2
    return pl.ds(pl.multiple_of(i * size, size), size)


def pack(ref, half, value, at=0, order=(0, 1, 2)):
    size = ref.shape[1]
    for j in range(SLOTS // 2):
        bits = (j % 2, j // 2, half)
        slot = 4 * bits[order[0]] + 2 * bits[order[1]] + bits[order[2]]
        ref[slot, :, at : at + value.shape[1]] = value[j * size : (j + 1) * size].astype(BF)


def moves():
    return [pltpu.SemaphoreType.DMA((3, CHUNKS)), pltpu.SemaphoreType.DMA((3, CHUNKS))]


def halves(rows, cols):
    return [pltpu.VMEM((3, rows, cols), BF), pltpu.VMEM((3, rows, cols), BF)] + moves()


class Moves:
    def __init__(self, sem, pairs):
        self.copies = [pltpu.make_async_copy(src, dst, sem.at[i]) for i, (src, dst) in enumerate(pairs)]

    def start(self, *which):
        for i in which:
            self.copies[i].start()

    def wait(self, *which):
        for i in which:
            self.copies[i].wait()


def row(vectors, number):
    return vectors[number][...].astype(F32).reshape(1, -1)


def some(vectors, *numbers):
    return {number: vectors[number] for number in numbers}


def like(*arrays):
    return [pltpu.VMEM(a.shape, a.dtype) for a in arrays]


def call(kernel, name, number, outs, scratch, *args, far=0, far_out=0):
    anywhere = pl.BlockSpec(memory_space=pl.ANY)
    return pl.pallas_call(
        kernel,
        out_shape=tuple(jax.ShapeDtypeStruct(shape, dtype) for shape, dtype in outs),
        in_specs=[jax.tree.map(lambda _: vmem(), arg) for arg in args[: len(args) - far]] + [anywhere] * far,
        out_specs=tuple([vmem()] * (len(outs) - far_out) + [anywhere] * far_out),
        scratch_shapes=scratch,
        compiler_params=pltpu.CompilerParams(
            vmem_limit_bytes=VMEM_MOST, collective_id=number, has_side_effects=True
        ),
        name=name,
    )(*args)


def attend_block(q_ref, k_ref, v_ref, table_ref, ids_ref, cols_ref, ctx_ref, lse_ref, seq, index):
    cols = q_ref.shape[1]
    length = ids_ref.shape[1]
    base = seq * length
    start, width = window(index, length)
    here = pl.ds(pl.multiple_of(index * BLOCK, BLOCK), BLOCK)
    rows = pl.ds(pl.multiple_of(base + index * BLOCK, BLOCK), BLOCK)
    keys_at = pl.ds(pl.multiple_of(base + start, 128), width)
    query = q_ref[rows, :]
    keys = k_ref[keys_at, :]
    values = v_ref[keys_at, :]
    same = cols_ref[rows, 0:1] == ids_ref[pl.ds(seq, 1), pl.ds(start, width)]
    context = jnp.zeros((BLOCK, cols), F32)
    sums = jnp.zeros((BLOCK, 128), F32)
    lane = lax.broadcasted_iota(jnp.int32, (1, 128), 1)
    for head in range(cols // HEAD_DIM):
        mine = head_lanes(head, cols)
        scores = dot_nt(jnp.where(mine, query, 0), keys)
        scores = jnp.where(same, scores + table_ref[head, here, pl.ds(start, width)].astype(F32), -1e30)
        peak = jnp.max(scores, axis=-1, keepdims=True)
        expo = jnp.exp(scores - peak)
        total = jnp.sum(expo, axis=-1, keepdims=True)
        part = dot(expo.astype(BF), values) * (1.0 / total)
        context = jnp.where(mine, part, context)
        sums = jnp.where(lane == head, peak + jnp.log(total), sums)
    ctx_ref[rows, :] = context.astype(BF)
    lse_ref[rows, :] = sums


def front_kernel(
    x_ref, par_ref, w_ref, bias_ref, cot_ref, ids_ref, pw_ref, table_hbm,
    ctx_ref, lse_ref, attn_ref, mid_ref, norm_ref, rows_hbm, grad_hbm, q_hbm, k_hbm, v_hbm,
    table_ref, cols_ref, rows_ref, grad_ref, q_ref, k_ref, v_ref, load, send, recv, gsend, grecv,
    out, inn, ssend, srecv,
):
    net = Gather(rows_ref, send, recv)
    top = Gather(grad_ref, gsend, grecv)
    red = Scatter(out, inn, ssend, srecv)
    seqs, length = ids_ref.shape
    moves = Moves(
        load,
        ((table_hbm, table_ref), (rows_ref, rows_hbm), (grad_ref, grad_hbm), (q_ref, q_hbm), (k_ref, k_hbm), (v_ref, v_hbm)),
    )
    moves.start(0)
    greet_mp()

    def own(chunk):
        part = x_ref[pl.ds(pl.multiple_of(chunk * net.size, net.size), net.size), :].astype(F32)
        rows_ref[net.rows(net.me, chunk), :] = norm_rows(part, row(par_ref, ATTN_GAIN), row(par_ref, ATTN_SHIFT))[0].astype(BF)
        net.send_own(chunk)

    loop(CHUNKS, own)

    def top_own(chunk):
        part = cot_ref[pl.ds(pl.multiple_of(chunk * net.size, net.size), net.size), :].astype(F32)
        grad_ref[net.rows(net.me, chunk), :] = (part * row(par_ref, MLP_SCALE)).astype(BF)

    loop(CHUNKS, top_own)
    id_columns(ids_ref, cols_ref, seqs, length)
    tall = 2 * net.size

    def project(block):
        def part(i):
            at = pl.ds(pl.multiple_of(block * CHUNKS * net.size + i * tall, tall), tall)
            rows = rows_ref[at, :]
            query = dot_nt(rows, w_ref[0]) + bias_ref[0:1, :].astype(F32)
            q_ref[at, :] = (query.astype(BF).astype(F32) * 0.125).astype(BF)
            k_ref[at, :] = dot_nt(rows, w_ref[1]).astype(BF)
            v_ref[at, :] = (dot_nt(rows, w_ref[2]) + bias_ref[1:2, :].astype(F32)).astype(BF)

        loop(CHUNKS // 2, part)

    def attend(seq, index):
        attend_block(q_ref, k_ref, v_ref, table_ref, ids_ref, cols_ref, ctx_ref, lse_ref, seq, index)

    project(net.me)
    loop(CHUNKS, net.wait_partner)
    project(net.partner)
    moves.wait(0)
    mine = net.me // 2
    steps = length // BLOCK

    def near(i):
        attend(mine, i)
        net.relay(i)
        top.send_own(i)

    loop(steps, near)
    project(net.cross)
    loop(CHUNKS, net.wait_diag)
    project(net.diag)
    moves.start(1, 3, 4, 5)

    def far(i):
        attend(1 - mine, i)
        top.relay(i)
        net.drain(i)

    loop(steps, far)

    def share(block, chunk):
        return dot(ctx_ref[net.rows(block, chunk), :], pw_ref[...])

    loop(CHUNKS, lambda c: red.put(0, c, share(red.diag, c)))
    loop(CHUNKS, lambda c: red.put(1, c, share(red.cross, c) + red.take(0, c)))
    loop(CHUNKS, lambda c: red.put(2, c, share(red.partner, c)))

    def keep(chunk):
        attn_ref[red.rows(chunk), :] = share(red.me, chunk) + red.take(2, chunk) + row(par_ref, PROJ_BIAS)

    loop(CHUNKS, keep)
    for wait in (top.wait_partner, top.wait_diag):
        loop(CHUNKS, wait)
    moves.start(2)

    def last(chunk):
        at = red.rows(chunk)
        attn = attn_ref[at, :] + red.take(1, chunk)
        middle = x_ref[at, :].astype(F32) + row(par_ref, ATTN_SCALE) * attn
        attn_ref[at, :] = attn
        mid_ref[at, :] = middle
        norm_ref[at, :] = norm_rows(middle, row(par_ref, MLP_GAIN), row(par_ref, MLP_SHIFT))[0].astype(BF)

    loop(CHUNKS, last)
    loop(CHUNKS, top.drain)
    loop(CHUNKS, red.drain)
    moves.wait(1, 2, 3, 4, 5)


def front(patches, params, weight, bias, cotangent, ids, proj, table):
    rows, width = patches.shape
    cols = weight.shape[1]
    one, wide = ((4 * rows, cols), BF), ((4 * rows, width), BF)
    own = ((rows, width), F32)
    params = some(params, ATTN_GAIN, ATTN_SHIFT, MLP_SCALE, PROJ_BIAS, ATTN_SCALE, MLP_GAIN, MLP_SHIFT)
    return call(
        front_kernel, "front", 1,
        [one, ((4 * rows, 128), F32), own, own, ((rows, width), BF), wide, wide, one, one, one],
        [pltpu.VMEM(table.shape, BF), pltpu.VMEM((4 * rows, 128), F32)]
        + [pltpu.VMEM(*shape) for shape in (wide, wide, one, one, one)]
        + [pltpu.SemaphoreType.DMA((6,))] + moves() + moves() + halves(rows, width),
        patches, params, weight, bias, cotangent, ids, proj, table, far=1, far_out=5,
    )


def gelu_both(u):
    inner = 0.7978845608028654 * (u + 0.044715 * (u * u * u))
    t = jnp.tanh(inner)
    half = 0.5 * (1.0 + t)
    slope = half + (0.5 * u) * (1.0 - t * t) * (0.7978845608028654 * (1.0 + 0.134145 * (u * u)))
    return u * half, slope


def mlp_kernel(
    norm_ref, par_ref, up_hbm, down_hbm, grad_hbm, mid_hbm, attn_hbm, cot_hbm,
    gmid_ref, gattn_ref, sums_ref, cross_hbm, here_hbm, upg_hbm, downg_hbm,
    up_ref, down_ref, grad_ref, mid_ref, attn_ref, cot_ref, cross_ref, here_ref, upg_ref, downg_ref, load,
    rows_ref, hid_ref, pre_ref, own_ref, far_ref, mfar_ref, gsend, grecv, out, inn, send, recv,
    mout, minn, msend, mrecv,
):
    gat = Gather(rows_ref, gsend, grecv)
    net = Scatter(out, inn, send, recv)
    top = Scatter(mout, minn, msend, mrecv)
    size = gat.size
    moves = Moves(
        load,
        (
            (up_hbm, up_ref), (down_hbm, down_ref), (grad_hbm, grad_ref), (mid_hbm, mid_ref), (attn_hbm, attn_ref),
            (cot_hbm, cot_ref), (cross_ref, cross_hbm), (here_ref, here_hbm), (upg_ref, upg_hbm), (downg_ref, downg_hbm),
        ),
    )
    moves.start(0, 1, 2, 3, 4, 5)
    greet_mp()
    sums_ref[...] = jnp.zeros_like(sums_ref)

    def own(chunk):
        rows_ref[gat.rows(gat.me, chunk), :] = norm_ref[net.rows(chunk), :]
        gat.send_own(chunk)

    loop(CHUNKS, own)

    moves.wait(0, 1, 2)

    def two(first, second, chunk):
        at, by = gat.rows(first, chunk), gat.rows(second, chunk)
        both = lambda ref: jnp.concatenate([ref[at, :], ref[by, :]], axis=0)
        value, slope = gelu_both(dot(both(rows_ref), up_ref[...]) + row(par_ref, UP_BIAS))
        hidden = value.astype(BF)
        hid_ref[at, :], hid_ref[by, :] = hidden[:size], hidden[size:]
        grad_pre = (dot_nt(both(grad_ref), down_ref[...]) * slope).astype(BF)
        pre_ref[at, :], pre_ref[by, :] = grad_pre[:size], grad_pre[size:]
        sums_ref[0:1, :] += jnp.sum(grad_pre.astype(F32), axis=0, keepdims=True)
        back = dot_nt(grad_pre, up_ref[...])
        part = dot(hidden, down_ref[...])
        return back[:size], back[size:], part[:size], part[size:]

    def near(chunk):
        gat.wait_partner(chunk)
        theirs, mine, share, kept = two(gat.partner, gat.me, chunk)
        net.put(2, chunk, theirs)
        top.put(2, chunk, share)
        own_ref[net.rows(chunk), :] = mine
        here_ref[net.rows(chunk), :] = kept

    loop(CHUNKS, near)

    def across(chunk):
        net.put(1, chunk, far_ref[net.rows(chunk), :] + net.take(0, chunk))

    def far(chunk):
        gat.relay(chunk)
        gat.wait_diag(chunk)
        theirs, mine, share, kept = two(gat.diag, gat.cross, chunk)
        net.put(0, chunk, theirs)
        top.put(0, chunk, share)
        far_ref[net.rows(chunk), :] = mine
        mfar_ref[net.rows(chunk), :] = kept

        @pl.when(chunk > 0)
        def _():
            across(chunk - 1)

    loop(CHUNKS, far)
    across(CHUNKS - 1)

    def weights(i):
        pack(upg_ref, i, dot_tn(rows_ref[:, half_of(rows_ref, i)], pre_ref[...]))
        pack(downg_ref, i, dot_tn(grad_ref[:, half_of(grad_ref, i)], hid_ref[...]))

    loop(2, weights)

    def outs(chunk):
        at = net.rows(chunk)
        here_ref[at, :] += top.take(2, chunk)
        cross_ref[at, :] = (mfar_ref[at, :] + top.take(0, chunk)).astype(BF)

    loop(CHUNKS, outs)
    moves.start(6, 7, 8, 9)
    moves.wait(3, 4, 5)

    def last(chunk):
        at = net.rows(chunk)
        grad = own_ref[at, :] + net.take(2, chunk) + net.take(1, chunk)
        normed, inv = norm_rows(mid_ref[at, :], 1.0, 0.0)[1:]
        back, gain_sum, shift_sum = norm_back(grad, normed, inv, row(par_ref, MLP_GAIN))
        middle = cot_ref[at, :].astype(F32) + back
        gattn = (middle * row(par_ref, ATTN_SCALE)).astype(BF)
        gmid_ref[at, :] = middle
        gattn_ref[at, :] = gattn
        sums_ref[1:2, :] += gain_sum[None]
        sums_ref[2:3, :] += shift_sum[None]
        sums_ref[3:4, :] += jnp.sum(middle * attn_ref[at, :], axis=0, keepdims=True)
        sums_ref[4:5, :] += jnp.sum(gattn.astype(F32), axis=0, keepdims=True)

    loop(CHUNKS, last)
    loop(CHUNKS, gat.drain)
    loop(CHUNKS, net.drain)
    loop(CHUNKS, lambda chunk: top.drain(chunk, (0, 2)))
    moves.wait(6, 7, 8, 9)


def mlp(normed, params, up, down, grad_rows, middle, attn, cotangent):
    rows, width = normed.shape
    ff = up.shape[1]
    one = pltpu.VMEM((rows, width), F32)
    packed = ((SLOTS, width // SLOTS, ff), BF)
    late = [((rows, width), BF), ((rows, width), F32), packed, packed]
    return call(
        mlp_kernel, "mlp", 3,
        [((rows, width), F32), ((rows, width), BF), ((8, width), F32)] + late,
        like(up, down, grad_rows, middle, attn, cotangent) + [pltpu.VMEM(*shape) for shape in late]
        + [pltpu.SemaphoreType.DMA((10,))]
        + [pltpu.VMEM((4 * rows, width), BF), pltpu.VMEM((4 * rows, ff), BF), pltpu.VMEM((4 * rows, ff), BF), one, one, one]
        + moves() + halves(rows, width) + halves(rows, width),
        normed, some(params, UP_BIAS, MLP_GAIN, ATTN_SCALE), up, down, grad_rows, middle, attn, cotangent, far=6, far_out=4,
    )


class Fold:
    def __init__(self, src, inn, send, recv, order=(0, 1, 2)):
        self.src, self.inn, self.send, self.recv = src, inn, send, recv
        self.size = src.shape[1] // PARTS
        place = lax.axis_index("dp")
        bits = (lax.rem(place, 2), lax.rem(place // 2, 2), place // 4)
        a, b, c = [bits[i] for i in order]
        self.peers = [place + (1 << i) - (2 << i) * bits[i] for i in order]
        self.theirs = (4 * (1 - a), 2 * (1 - b), 4 + 1 - c)
        self.mine = (4 * a, 2 * b, 4 + c)

    def copy(self, stage, part):
        count, offset = (4, 2, 1)[stage], (0, 4, 6)[stage]
        rows = pl.ds(part * self.size, self.size)
        src = self.src if stage == 0 else self.inn
        return pltpu.make_async_remote_copy(
            src_ref=src.at[pl.ds(self.theirs[stage], count), rows, :],
            dst_ref=self.inn.at[pl.ds(offset, count), rows, :],
            send_sem=self.send.at[stage, part], recv_sem=self.recv.at[stage, part],
            device_id={"dp": self.peers[stage]}, device_id_type=MESH,
        )

    def start(self):
        for part in range(PARTS):
            self.copy(0, part).start()

    def advance(self, stage):
        count, offset = (4, 2)[stage], (0, 4)[stage]
        src = self.src if stage == 0 else self.inn
        for part in range(PARTS):
            rows = pl.ds(part * self.size, self.size)
            self.copy(stage, part).wait_recv()
            for i in range(count):
                self.inn[offset + i, rows, :] = self.inn[offset + i, rows, :] + src[self.mine[stage] + i, rows, :]
            self.copy(stage + 1, part).start()

    def finish(self, put):
        for part in range(PARTS):
            rows = pl.ds(part * self.size, self.size)
            self.copy(2, part).wait_recv()
            put(rows, self.inn[self.mine[2], rows, :].astype(F32) + self.inn[6, rows, :].astype(F32))

    def drain(self):
        for stage in range(3):
            for part in range(PARTS):
                self.copy(stage, part).wait_send()


class Total:
    def __init__(self, acc, inn, send, recv):
        self.acc, self.inn, self.send, self.recv = acc, inn, send, recv
        place = lax.axis_index("dp")
        x, lo, hi = lax.rem(place, 2), lax.rem(place // 2, 2), place // 4
        _, partner, cross, _ = neighbours()
        self.peers = (
            {"mp": partner}, {"mp": cross}, {"dp": place + 1 - 2 * x}, {"dp": place + 2 - 4 * lo}, {"dp": place + 4 - 8 * hi},
        )

    def copy(self, stage):
        return pltpu.make_async_remote_copy(
            src_ref=self.acc.at[stage], dst_ref=self.inn.at[stage], send_sem=self.send.at[stage],
            recv_sem=self.recv.at[stage], device_id=self.peers[stage], device_id_type=MESH,
        )

    def start(self, stage):
        self.copy(stage).start()

    def finish(self, stage):
        self.copy(stage).wait_recv()
        self.acc[stage + 1] = self.acc[stage] + self.inn[stage]
        if stage == 1:
            self.acc[2, 8:16, :] = self.acc[0, 8:16, :]

    def drain(self):
        for stage in range(5):
            self.copy(stage).wait_send()


def back_kernel(
    fold,
    pw_ref, ids_ref, par_ref, two_ref, rows_hbm, table_hbm, *refs,
):
    early, refs = refs[:EARLY], refs[EARLY:]
    if fold:
        layer_ref, grad_ref, tab_ref, upo_ref, downo_ref, mixo_ref, sums_ref, *refs = refs
        band_ref, mix_ref, acc_ref, *refs = refs
        winn, wsend, wrecv, tinn, tsend, trecv, ainn, asend, arecv, *refs = refs
    else:
        layer_ref, grad_ref, band_ref, mix_ref, sums_ref, *refs = refs
        acc_ref = None
    held, refs = refs[: EARLY - 1], refs[EARLY - 1 :]
    upg_ref, downg_ref, q_ref, k_ref, v_ref, lse_ref, cross_ref, ctx_ref, w_ref, here_ref, mid_ref, cot_ref, x_ref, gmid_ref = held
    (
        table_ref, cols_ref, rowsg_ref, g_ref, qt_ref, gt_ref, dkt_ref, dvt_ref, strip_ref, dq_ref, dv_ref,
        far_ref, load, hold, fsend, frecv, gsend, grecv, out, inn, send, recv,
    ) = refs
    dk_ref = g_ref
    own_ref = grad_ref
    gat = Gather(rowsg_ref, gsend, grecv)
    net = Scatter(out, inn, send, recv)
    seqs, length = ids_ref.shape
    rows_all, cols = q_ref.shape
    blocks = length // BLOCK
    heads = cols // HEAD_DIM
    small_ref = acc_ref.at[0] if fold else sums_ref
    me, partner, cross, _ = neighbours()
    whole = CHUNKS * gat.size
    mine_at = pl.ds(pl.multiple_of(me * whole, whole), whole)
    moves = Moves(hold, [(early[0], rowsg_ref.at[mine_at, :])] + list(zip(early[1:], held)))
    moves.start(*range(7))

    def fetch(head):
        at = pl.ds(pl.multiple_of(lax.rem(head, 2) * length, length), length)
        return pltpu.make_async_copy(table_hbm.at[head], table_ref.at[at, :], load.at[1 + head])

    fetch(0).start()
    fetch(1).start()
    moves.start(*range(7, EARLY))
    far = pltpu.make_async_remote_copy(
        src_ref=cross_ref, dst_ref=far_ref, send_sem=fsend, recv_sem=frecv, device_id={"mp": cross}, device_id_type=MESH
    )
    if fold:
        up = Fold(upg_ref, winn.at[0], wsend.at[0], wrecv.at[0])
        down = Fold(downg_ref, winn.at[1], wsend.at[1], wrecv.at[1])
        mix = Fold(mix_ref, winn.at[2], wsend.at[2], wrecv.at[2], MIX_ORDER)
        tab = lambda head: Fold(band_ref.at[head], tinn.at[head], tsend.at[head], trecv.at[head])
        small = Total(acc_ref, ainn, asend, arecv)
        greet(({"mp": partner}, {"mp": cross}) + tuple({"dp": peer} for peer in up.peers))
    else:
        greet_mp()

    moves.wait(0)
    loop(CHUNKS, gat.send_own)
    moves.wait(1, 2)
    if fold:
        up.start()
        down.start()
    id_columns(ids_ref, cols_ref, seqs, length)

    def block(number):
        at = pl.ds(pl.multiple_of(number * whole, whole), whole)
        g_ref[at, :] = dot_nt(rowsg_ref[at, :], pw_ref[...]).astype(BF)

    def tall(i):
        return pl.ds(pl.multiple_of(i * BLOCK, BLOCK), BLOCK)

    def flip_q(i):
        qt_ref[:, tall(i)] = q_ref[tall(i), :].T

    def flip_g(i):
        gt_ref[:, tall(i)] = g_ref[tall(i), :].T

    per = rows_all // BLOCK // seqs
    near_seq = gat.me // 2
    block(gat.me)
    dkt_ref[...] = jnp.zeros_like(dkt_ref)
    dvt_ref[...] = jnp.zeros_like(dvt_ref)
    dq_ref[...] = jnp.zeros_like(dq_ref)
    small_ref[...] = jnp.zeros_like(small_ref)
    if fold:
        tab_ref[...] = jnp.zeros_like(tab_ref)
    moves.wait(3, 4, 5, 6)
    loop(rows_all // BLOCK, flip_q)
    loop(CHUNKS, gat.wait_partner)
    block(gat.partner)
    loop(per, lambda i: flip_g(near_seq * per + i))
    lane = lax.broadcasted_iota(jnp.int32, (1, 128), 1)

    def step(head, index, seq, first):
        start, width = window(index, length)
        mine = head_lanes(head, cols)
        feats = pl.ds(pl.multiple_of(head * HEAD_DIM, HEAD_DIM), HEAD_DIM)
        rows = tall(seq * blocks + index)
        keys_at = pl.ds(pl.multiple_of(seq * length + start, 128), width)
        keys = k_ref[keys_at, :]
        same = cols_ref[rows, 0:1] == ids_ref[pl.ds(seq, 1), pl.ds(start, width)]
        sums = jnp.sum(jnp.where(lane == head, lse_ref[rows, :], 0.0), axis=-1, keepdims=True)
        bias = table_ref[tall(lax.rem(head, 2) * blocks + index), pl.ds(start, width)].astype(F32)
        scores = dot_nt(jnp.where(mine, q_ref[rows, :], 0), keys) + bias
        probs = jnp.where(same, jnp.exp(scores - sums), 0.0)
        grad_probs = dot_nt(jnp.where(mine, g_ref[rows, :], 0), v_ref[keys_at, :])
        centre = jnp.sum(grad_probs * probs, axis=-1, keepdims=True)
        grad_scores = (probs * (grad_probs - centre)).astype(BF)
        strip_ref[:, 0:width] = grad_scores
        dvt_ref[feats, keys_at] += dot(gt_ref[feats, rows], probs.astype(BF))
        dkt_ref[feats, keys_at] += dot(qt_ref[feats, rows], grad_scores)
        grad_q = (dot(grad_scores, keys) * 0.125).astype(BF)
        dq_ref[rows, :] = jnp.where(mine, grad_q, dq_ref[rows, :])
        for part in range(BLOCK // GROUP):
            group = index * (BLOCK // GROUP) + part
            tiles = []
            for t in range(TILES + 1):
                block = group - TILES // 2 + t
                there = (block >= 0) & (block < length // GROUP)
                offset = jnp.clip(block * GROUP - start, 0, width - GROUP)
                tile = strip_ref[part * GROUP : (part + 1) * GROUP, pl.ds(pl.multiple_of(offset, GROUP), GROUP)]
                tiles.append(jnp.where(there, tile, 0))
            tiles[0] += tiles.pop()
            value = jnp.concatenate(tiles, axis=1)
            slot = slot_of(group)
            if not first:
                value = (value.astype(F32) + band_ref[head, slot, :, :].astype(F32)).astype(BF)
            band_ref[head, slot, :, :] = value

    def one_head(head, seq, first):
        fetch(head).wait()

        def inner(index):
            step(head, index, seq, first)
            if first:
                i = head * blocks + index

                @pl.when(lax.rem(i, heads) == heads - 1)
                def _():
                    gat.relay(i // heads)

        loop(blocks, inner)

        @pl.when(head + 2 < heads)
        def _():
            fetch(head + 2).start()

    def near_head(head):
        one_head(head, near_seq, True)

    def far_head(head):
        one_head(head, 1 - near_seq, False)
        if fold:
            tab(head).start()

            @pl.when(head == 0)
            def _():
                down.advance(0)
                up.advance(1)

            @pl.when(head == 1)
            def _():
                down.advance(1)

    loop(heads, near_head)
    fetch(0).start()
    fetch(1).start()
    block(gat.cross)
    loop(CHUNKS, gat.wait_diag)
    block(gat.diag)
    moves.wait(7)
    far.start()
    loop(per, lambda i: flip_g((1 - near_seq) * per + i))
    if fold:
        up.advance(0)
    loop(heads, far_head)
    moves.wait(*range(8, EARLY))
    rows_ref = table_ref.at[:, 0 : rowsg_ref.shape[1]]
    again = pltpu.make_async_copy(rows_hbm, rows_ref, load.at[0])
    again.start()

    def unflip(i):
        dk_ref[tall(i), :] = dkt_ref[:, tall(i)].T.astype(BF)
        dv_ref[tall(i), :] = dvt_ref[:, tall(i)].T.astype(BF)

    loop(rows_all // BLOCK, unflip)

    again.wait()

    order = MIX_ORDER if fold else (0, 1, 2)

    def weights(i):
        rows = table_ref[:, half_of(rowsg_ref, i)]
        for number, ref in enumerate((dq_ref, dk_ref, dv_ref)):
            pack(mix_ref, i, dot_tn(rows, ref[...]), number * cols, order)
        pack(mix_ref, i, dot_tn(rowsg_ref[:, half_of(rowsg_ref, i)], ctx_ref[...]), 3 * cols, order)

    loop(2, weights)

    def put_table(head):
        def put(rows, value):
            group = lax.axis_index("dp")
            left, right = edge(rows.start, rows.size)
            for t in range(TILES + 1):
                tile = value[:, t % TILES * GROUP : (t % TILES + 1) * GROUP]
                if t % TILES == 0:
                    tile = jnp.where(right if t else left, tile, 0.0)
                block = group - TILES // 2 + t

                @pl.when((block >= 0) & (block < length // GROUP))
                def _():
                    tab_ref[head, rows, pl.ds(pl.multiple_of(block * GROUP, GROUP), GROUP)] = tile
        return put

    def put_to(ref):
        def put(rows, value):
            ref[rows, :] = value
        return put

    if fold:
        mix.start()

    def share(number, chunk):
        at = gat.rows(number, chunk)
        return dot(dq_ref[at, :], w_ref[0]) + dot(dk_ref[at, :], w_ref[1]) + dot(dv_ref[at, :], w_ref[2])

    loop(CHUNKS, lambda c: net.put(0, c, share(net.diag, c)))
    loop(CHUNKS, lambda c: net.put(1, c, share(net.cross, c) + net.take(0, c)))
    loop(CHUNKS, lambda c: net.put(2, c, share(net.partner, c)))

    def keep(chunk):
        own_ref[net.rows(chunk), :] = share(net.me, chunk) + net.take(2, chunk)

    loop(CHUNKS, keep)
    if fold:
        tab(0).advance(0)
        up.finish(put_to(upo_ref))
        down.finish(put_to(downo_ref))
    far.wait_recv()

    def layer(chunk):
        at = net.rows(chunk)
        mlp_out = here_ref[at, :] + far_ref[at, :].astype(F32) + row(par_ref, DOWN_BIAS)
        layer_ref[at, :] = (mid_ref[at, :] + row(par_ref, MLP_SCALE) * mlp_out).astype(BF)
        top = cot_ref[at, :].astype(F32)
        small_ref[7:8, :] += jnp.sum(top * mlp_out, axis=0, keepdims=True)
        low = (top * row(par_ref, MLP_SCALE)).astype(BF).astype(F32)
        small_ref[6:7, :] += jnp.sum(low, axis=0, keepdims=True)

    loop(CHUNKS, layer)
    for put, source in ((2, 4), (3, 3), (4, 1), (5, 2), (8, 0)):
        small_ref[put : put + 1, :] = two_ref[source : source + 1, :]
    small_ref[9:10, 0:cols] = jnp.sum(dq_ref[...].astype(F32), axis=0, keepdims=True)
    small_ref[10:11, 0:cols] = jnp.sum(dv_ref[...].astype(F32), axis=0, keepdims=True)
    if fold:
        tab(0).advance(1)
        tab(1).advance(0)

    def last(chunk):
        at = net.rows(chunk)
        grad = own_ref[at, :] + net.take(1, chunk)
        normed, inv = norm_rows(x_ref[at, :].astype(F32), 1.0, 0.0)[1:]
        back, gain_sum, shift_sum = norm_back(grad, normed, inv, row(par_ref, ATTN_GAIN))
        grad_ref[at, :] = gmid_ref[at, :] + back
        small_ref[0:1, :] += gain_sum[None]
        small_ref[1:2, :] += shift_sum[None]

    loop(CHUNKS, last)
    if fold:
        small.start(0)
        tab(0).finish(put_table(0))
        tab(1).advance(1)
        small.finish(0)
        small.start(1)
        tab(2).advance(0)
        small.finish(1)
        small.start(2)
        tab(1).finish(put_table(1))
        small.finish(2)
        small.start(3)
        tab(2).advance(1)
        mix.advance(0)
        small.finish(3)
        small.start(4)
        mix.advance(1)
        mix.finish(put_to(mixo_ref))
        tab(2).finish(put_table(2))
        small.finish(4)
        sums_ref[...] = acc_ref[5]
        for piece in (up, down, mix, tab(0), tab(1), tab(2), small):
            piece.drain()
    far.wait_send()
    loop(CHUNKS, gat.drain)
    loop(CHUNKS, net.drain)


def back(fold, length, proj, ids, params, two, rows_one, table, *early):
    rows, width = early[0].shape
    cols = proj.shape[0]
    heads = cols // HEAD_DIM
    piece, wide = width // SLOTS, TILES * GROUP
    strip = min(length, BLOCK + 2 * PAGE_MOST)
    band, mix = ((heads, SLOTS, GROUP, wide), BF), ((SLOTS, piece, width), BF)
    outs = [((rows, width), BF), ((rows, width), F32)]
    scratch = []
    if fold:
        sem = pltpu.SemaphoreType.DMA((3, 3, PARTS))
        outs += [((heads, GROUP, length), F32)] + [((piece, width), F32)] * 3
        scratch += [pltpu.VMEM(*band), pltpu.VMEM(*mix), pltpu.VMEM((6, 16, width), F32)]
        scratch += [pltpu.VMEM((3, 7, piece, width), BF), sem, sem, pltpu.VMEM((heads, 7, GROUP, wide), BF), sem, sem]
        scratch += [pltpu.VMEM((5, 16, width), F32), pltpu.SemaphoreType.DMA((5,)), pltpu.SemaphoreType.DMA((5,))]
    else:
        outs += [band, mix]
    outs += [((16, width), F32)]
    one, flat = pltpu.VMEM((4 * rows, cols), BF), pltpu.VMEM((cols, 4 * rows), BF)
    total = pltpu.VMEM((cols, 4 * rows), F32)
    scratch += like(*early[1:]) + [
        pltpu.VMEM((2 * length, length), BF), pltpu.VMEM((4 * rows, 128), F32), pltpu.VMEM((4 * rows, width), BF), one,
        flat, flat, total, total, pltpu.VMEM((BLOCK, strip), BF), one, one, pltpu.VMEM((rows, width), BF),
        pltpu.SemaphoreType.DMA((1 + heads,)), pltpu.SemaphoreType.DMA((EARLY,)),
        pltpu.SemaphoreType.DMA, pltpu.SemaphoreType.DMA,
    ] + moves() + halves(rows, width)
    params = some(params, DOWN_BIAS, MLP_SCALE, ATTN_GAIN)
    return call(
        partial(back_kernel, fold), "back", 4, outs, scratch, proj, ids, params, two, rows_one, table, *early, far=2 + EARLY
    )


def finish_kernel(mix_ref, sums_ref, *refs):
    late, refs = refs[:5], refs[5:]
    (qkv_ref, proj_ref, qv_ref), refs = refs[:3], refs[3:]
    vectors, refs = refs[:9], refs[9:]
    done, held, sem, back_sem = refs[:5], refs[5:10], refs[10], refs[11]
    inward = Moves(sem, zip(late, held))
    outward = Moves(back_sem, zip(held, done))
    inward.start(*range(5))
    cols = qkv_ref.shape[2]
    for number in range(3):
        qkv_ref[number] = mix_ref[:, number * cols : (number + 1) * cols]
    proj_ref[...] = mix_ref[:, 3 * cols :].T
    qv_ref[...] = sums_ref[9:11, 0:cols]
    for number in range(9):
        vectors[number][...] = sums_ref[number : number + 1, :].reshape(-1)
    for number in range(5):
        inward.wait(number)
        outward.start(number)
    outward.wait(*range(5))


def finish(mixed, sums, cols, *late):
    piece, width = mixed.shape
    anywhere = pl.BlockSpec(memory_space=pl.ANY)
    shapes = [(3, piece, cols), (width - 3 * cols, piece), (2, cols)] + [(width,)] * 9
    return pl.pallas_call(
        finish_kernel,
        out_shape=tuple(jax.ShapeDtypeStruct(shape, F32) for shape in shapes)
        + tuple(jax.ShapeDtypeStruct(a.shape, a.dtype) for a in late),
        in_specs=[vmem()] * 2 + [anywhere] * 5,
        out_specs=tuple([vmem()] * len(shapes) + [anywhere] * 5),
        scratch_shapes=like(*late) + [pltpu.SemaphoreType.DMA((5,)), pltpu.SemaphoreType.DMA((5,))],
        compiler_params=pltpu.CompilerParams(vmem_limit_bytes=VMEM_MOST),
        name="finish",
    )(mixed, sums, *late)


def scatter_dp(x):
    return lax.psum_scatter(x, "dp", scatter_dimension=0, tiled=True).astype(F32)


def in_order(packed):
    _, rows, cols = packed.shape
    return packed.reshape(2, 2, 2, rows, cols).transpose(2, 1, 0, 3, 4).reshape(SLOTS * rows, cols)


def reduce_table(band, length, n_dp):
    groups, heads, _, wide = band.shape
    shard = length // n_dp
    send = band.reshape(groups, heads, GROUP // shard, shard, wide).swapaxes(1, 2)
    part = scatter_dp(send.reshape(n_dp * heads * shard, wide)).reshape(heads, shard, wide)
    place = lax.axis_index("dp") * shard
    return unfold(part, place // GROUP, place % GROUP, length)


def unfold(part, group, first_row, length):
    heads, shard, _ = part.shape
    left, right = edge(first_row, shard)
    end = part[:, :, :GROUP]
    band = jnp.concatenate([jnp.where(left, end, 0.0), part[:, :, GROUP:], jnp.where(right, end, 0.0)], axis=2)
    full = jnp.zeros((heads, shard, length + 2 * PAGE_MOST), F32)
    full = lax.dynamic_update_slice(full, band, (0, 0, group * GROUP))
    return full[:, :, PAGE_MOST : PAGE_MOST + length]


def local(
    patches, segment_ids, fill_counts, attn_gain, attn_shift, qkv_weight, qv_bias, rel_table, proj_weight,
    proj_bias, attn_scale, mlp_gain, mlp_shift, up_weight, up_bias, down_weight, down_bias, mlp_scale, cotangent,
):
    n_dp = lax.axis_size("dp")
    seqs, length = segment_ids.shape
    cols = qkv_weight.shape[2]
    places = jnp.arange(length, dtype=jnp.int32)[None]
    ids = jnp.where(places < fill_counts[:, None], segment_ids, -1 - places).astype(F32)
    fold = n_dp == SLOTS and length == SLOTS * GROUP
    vectors = (attn_gain, attn_shift, proj_bias, attn_scale, mlp_gain, mlp_shift, up_bias, down_bias, mlp_scale)
    params = dict(enumerate(vectors))
    turned = qkv_weight.swapaxes(1, 2)
    context, lse, attn_out, middle, normed_two, rows_one, grad_rows, queries, keys, values = front(
        patches, params, turned, qv_bias, cotangent, ids, proj_weight, rel_table
    )
    grad_middle, grad_attn, sums_two, cross, here, up_local, down_local = mlp(
        normed_two, params, up_weight, down_weight, grad_rows, middle, attn_out, cotangent
    )
    layer_out, patch_grad, *more, sums = back(
        fold, length, proj_weight, ids, params, sums_two, rows_one, rel_table,
        grad_attn, up_local, down_local, queries, keys, values, lse, cross, context, turned, here, middle, cotangent,
        patches, grad_middle,
    )
    if fold:
        table_grad, up_grad, down_grad, mixed = more
        qkv_grad, proj_grad, qv_grad, *vectors, layer_out, patch_grad, table_grad, up_grad, down_grad = finish(
            mixed, sums, cols, layer_out, patch_grad, table_grad, up_grad, down_grad
        )
    else:
        band, mixed = more
        order = [4 * (d % 2) + 2 * (d // 2 % 2) + d // 4 for d in range(SLOTS)]
        table_grad = reduce_table(jnp.stack([band[:, slot] for slot in order]), length, n_dp)
        up_grad, down_grad, mixed = [scatter_dp(in_order(piece)) for piece in (up_local, down_local, mixed)]
        sums = jnp.concatenate([lax.psum(sums[:8], ("dp", "mp")), lax.psum(sums[8:], "dp")])
        qkv_grad = mixed[:, : 3 * cols].reshape(-1, 3, cols).swapaxes(0, 1)
        proj_grad, qv_grad, vectors = mixed[:, 3 * cols :].T, sums[9:11, :cols], sums[:9]
    return (
        layer_out, patch_grad, vectors[0], vectors[1], qkv_grad, qv_grad, table_grad, proj_grad,
        vectors[2], vectors[3], vectors[4], vectors[5], up_grad, vectors[8], down_grad.T, vectors[6], vectors[7],
    )


def solution(mesh):
    rows, split = P(("dp", "mp"), None), P("mp", None)
    placed = (
        rows, P("dp", None), P("dp"), P(), P(), P(None, None, "mp"), P(None, "mp"), P("mp", None, None), split,
        P(), P(), P(), P(), P(None, "mp"), P("mp"), split, P(), P(), rows,
    )
    given = (
        rows, rows, P(), P(), P(None, "dp", "mp"), P(None, "mp"), P("mp", "dp", None), P("mp", "dp"), P(), P(),
        P(), P(), P("dp", "mp"), P("mp"), P("mp", "dp"), P(), P(),
    )
    return jax.shard_map(local, mesh=mesh, in_specs=placed, out_specs=given, check_vma=False)
```
